32 devices in a mesh: groups: 2 (over y), expert: 8 (over z, core), tensor: 2 (over x).
Axes of the slice: x: 2, y: 2, z: 4, core: 2. Of those that a mesh axis runs over, the one named last changes fastest.
Arguments:
- hidden_in: bfloat16 [128, 2880], P(('groups', 'expert')), parts along dimension 0, may hold values from -6 to 6
- queries: bfloat16 [128, 32, 64], P(('groups', 'expert'), 'tensor'), parts along dimension 0, may hold values from -8 to 8
- new_keys: bfloat16 [128, 8, 64], P(('groups', 'expert'), 'tensor'), parts along dimension 0, may hold values from -4 to 4
- new_values: bfloat16 [128, 8, 64], P(('groups', 'expert'), 'tensor'), parts along dimension 0, may hold values from -4 to 4
- cache_keys: bfloat16 [128, 8, 64, 256], P(('groups', 'expert'), 'tensor'), parts along dimension 0, may hold values from -8 to 8
- cache_values: bfloat16 [128, 8, 64, 256], P(('groups', 'expert'), 'tensor'), parts along dimension 0, may hold values from -4 to 4
- cache_lengths: int32 [128], P(('groups', 'expert')), parts along dimension 0, may hold values from 2 to 256, as said below
- out_weight: bfloat16 [2048, 2880], P('tensor'), may hold values from -0.125 to 0.125
- norm_gain: float32 [2880], replicated, may hold values from 0.1 to 1.9
- expert_ids: int32 [128, 4], P(('groups', 'expert')), parts along dimension 0, may hold values from 0 to 7, all different within a row; in each aligned block of 8 rows (0 to 7, 8 to 15, ...) at most 4 rows name the same one
- route_probs: float32 [128, 4], P(('groups', 'expert')), parts along dimension 0, may hold values from 0.05 to 1
- route_order: int32 [128, 4], P(('groups', 'expert')), parts along dimension 0, may hold values from 0 to 3, each once within a row
- gate_weight: bfloat16 [8, 2880, 1440], P('expert', None, 'tensor'), may hold values from -0.109375 to 0.109375
- up_weight: bfloat16 [8, 2880, 1440], P('expert', None, 'tensor'), may hold values from -0.109375 to 0.109375
- down_weight: bfloat16 [8, 1440, 2880], P('expert', 'tensor'), may hold values from -0.15625 to 0.15625
Outputs:
- layer_out: bfloat16 [128, 2880], P(('groups', 'expert'), 'tensor'), parts along dimension 0
The draws below stay inside these ranges and needn't reach their ends.
There are 2 independent parts, one for each index of `groups`. The reference program is written for one: setup_inputs(seed, part) draws one part's arguments, and reference() takes and returns one part's arrays. A program takes and returns all parts, laid end to end along the dimension named above; an argument that names none is the same for every part. Nothing has to cross between parts.
Inputs may be any that keep to these rules, and one draw needn't show every extreme that they name: `cache_lengths`: some sequence fills all 256 slots. `expert_ids`: each row names 4 different experts; among the 8 rows of one device no expert is named by more than 4 rows, a bound that some block reaches. `route_order`: each row is a permutation of 0 to 3.
All inputs are finite; a program needn't handle non-finite values.
Results may differ from the reference program's by a relative error of at most 0.007.
Values may be sent and summed in bfloat16 or wider, within the bound.
No kernel may reach another device: no remote copies, remote signals or barrier semaphores. Data moves between devices by JAX's collectives and lax.ppermute only.
A program may use at most 64 MiB of HBM per device.

```python
import math
from functools import partial
import jax
import jax.numpy as jnp
import numpy as np
from jax import lax

D = 2880
FF = 1440
HEADS = 32
KVH = 8
HD = 64
TOP = 4
SEQ_DEV = 8
CACHE = 256
SEQS = 64
EXPERTS = 8
CAP = 4


def draw_queries(key, part):
    noise_key = jax.random.fold_in(key, 3)
    values = jnp.clip(jax.random.normal(noise_key, (SEQS, HEADS, HD), jnp.float32), -4.0, 4.0)
    return values.astype(jnp.bfloat16)


def draw_cache_keys(key, part):
    noise_key = jax.random.fold_in(key, 5)
    values = jnp.clip(jax.random.normal(noise_key, (SEQS, KVH, HD, CACHE), jnp.float32), -4.0, 4.0)
    return values.astype(jnp.bfloat16)


def draw_cache_lengths(key, part):
    length_key, pick_key = jax.random.split(jax.random.fold_in(key, 11))
    drawn_lengths = jax.random.randint(length_key, (SEQS,), 2, CACHE + 1)
    chosen = jax.random.randint(pick_key, (), 0, SEQS)
    return jnp.where(jnp.arange(SEQS) == chosen, CACHE, drawn_lengths).astype(jnp.int32)


def block_scale(own_key, shape, pieces, smallest, largest):
    level = 1.0
    for dim, shards_of in pieces:
        heights = jax.random.uniform(jax.random.fold_in(jax.random.fold_in(own_key, 6), dim), (shards_of,), jnp.float32, smallest / len(pieces), largest / len(pieces))
        level = level * jnp.repeat(jnp.exp(heights), shape[dim] // shards_of).reshape((-1,) + (1,) * (len(shape) - 1 - dim))
    return level


def routed_block(key, own, number, rows, number_of, top, most, slope):
    sequence = jax.random.permutation(key, number_of)
    packed, ordinary = shares(number_of, rows * top, most, slope, True), shares(number_of, rows * top, most, slope, False)
    places = jnp.arange(number_of)

    def named(lengths, offset_by):
        used = int((lengths > 0).sum())
        fixed = max(1, used // 4)
        passed = fixed + (places - fixed + offset_by * (used - fixed)) % max(1, number_of - fixed)
        return jnp.zeros((number_of,), jnp.int32).at[sequence[jnp.where(places < fixed, places, passed)]].set(jnp.asarray(lengths, jnp.int32))

    lengths = jnp.where(number % 4 == 0, named(packed, number // 4), named(ordinary, number - number // 4 - 1))
    mixed = jax.random.permutation(jax.random.fold_in(own, 3), number_of)
    source_of, receiver = mixed[0:number_of // 2 * 2:2], mixed[1:number_of // 2 * 2:2]
    slack = jnp.minimum(lengths[source_of] - 1, most - lengths[receiver]) // 2
    slack = jnp.where((source_of == sequence[0]) | (receiver == sequence[0]) | (lengths[receiver] == 0), 0, jnp.maximum(slack, 0))
    passed = jax.random.randint(jax.random.fold_in(own, 4), (number_of // 2,), 0, 1 << 20) % (slack + 1)
    lengths = lengths.at[source_of].add(-passed).at[receiver].add(passed)
    items = jnp.searchsorted(jnp.cumsum(lengths), jnp.arange(rows * top), side="right").astype(jnp.int32)
    listing = items.reshape(top, rows).T
    listing = listing[jax.random.permutation(jax.random.fold_in(own, 1), rows)]
    offset_by = jax.random.randint(jax.random.fold_in(own, 2), (rows, 1), 0, top)
    return jnp.take_along_axis(listing, (jnp.arange(top)[None, :] + offset_by) % top, axis=1)


def shares(amount, total, most, lean, full):
    weights = [(1 << 20) // math.isqrt(rank ** lean) + 1 for rank in range(1, amount + 1)]
    largest = most if full else min(most, max(-(-total // amount), total * weights[0] // sum(weights)))
    least = 1 if total - largest >= amount - 1 else 0
    counts, rest = [largest] + [least] * (amount - 1), total - largest - least * (amount - 1)
    while rest > 0:
        candidates = [i for i in range(1, amount) if counts[i] < largest] or [i for i in range(1, amount) if counts[i] < most]
        mass, remaining = sum([weights[i] for i in candidates]), rest
        for i in candidates:
            more = min(most - counts[i], max(1, remaining * weights[i] // mass), rest)
            counts[i] = counts[i] + more
            rest = rest - more
    return np.array(counts)


def gaussian(own_key, dims, spread, limit, shards=(), kind=jnp.bfloat16):
    result = jax.random.normal(own_key, dims, jnp.float32) * spread
    if len(shards) > 0:
        result = block_scale(own_key, dims, shards, -0.22, 0.18) * result
    return jnp.clip(result, min=-limit, max=limit).astype(kind)


def setup_inputs(seed: int = 0, part: int = 0) -> dict:
    keys = jax.random.split(jax.random.key(seed), 16)
    part_splits = jax.random.split(jax.random.fold_in(keys[15], part), 16)
    hidden_in = gaussian(part_splits[0], (SEQS, D), 1.0, 6.0, ((0, 8),))
    queries = draw_queries(jax.random.fold_in(jax.random.fold_in(keys[15], part), 71), part)
    new_keys = gaussian(part_splits[2], (SEQS, KVH, HD), 1.0, 4.0, ((0, 8), (1, 2)))
    new_values = gaussian(part_splits[3], (SEQS, KVH, HD), 1.0, 4.0, ((0, 8), (1, 2)))
    cache_keys = draw_cache_keys(jax.random.fold_in(jax.random.fold_in(keys[15], part), 71), part)
    cache_values = gaussian(part_splits[5], (SEQS, KVH, HD, CACHE), 1.0, 4.0, ((0, 8), (1, 2)))
    cache_lengths = draw_cache_lengths(jax.random.fold_in(jax.random.fold_in(keys[15], part), 71), part)
    out_weight = gaussian(keys[7], (HEADS * HD, D), (HEADS * HD) ** -0.5, 0.125, ((0, 2),))
    norm_gain = jnp.clip(1.0 + 0.18 * jax.random.normal(keys[8], (D,), jnp.float32), 0.1, 1.9)
    expert_ids_keys = jax.random.split(jax.random.fold_in(part_splits[9], 1), SEQS // SEQ_DEV)
    expert_ids_turns = jax.random.permutation(jax.random.fold_in(part_splits[9], 3), SEQS // SEQ_DEV)
    expert_ids = jax.vmap(lambda own, number: routed_block(jax.random.fold_in(part_splits[9], 2), own, number, SEQ_DEV, EXPERTS, TOP, CAP, 2))(expert_ids_keys, expert_ids_turns).reshape((SEQS, TOP))
    route_probs = jnp.clip(jnp.exp(math.log(1.0) - 2.9957323 * jax.random.uniform(part_splits[10], (SEQS, TOP), jnp.float32) ** block_scale(part_splits[10], (SEQS, TOP), ((0, 8),), -0.2, 0.2)), 0.05, 1.0)
    route_order = jax.vmap(lambda own: jax.random.permutation(own, TOP))(jax.random.split(part_splits[11], SEQS)).reshape((SEQS, TOP)).astype(jnp.int32)
    gate_weight = gaussian(keys[12], (EXPERTS, D, FF), D ** -0.5, 0.109375, ((0, 8), (2, 2)))
    up_weight = gaussian(keys[13], (EXPERTS, D, FF), D ** -0.5, 0.109375, ((0, 8), (2, 2)))
    down_weight = gaussian(keys[14], (EXPERTS, FF, D), FF ** -0.5, 0.15625, ((0, 8), (1, 2)))
    return dict(hidden_in=hidden_in, queries=queries, new_keys=new_keys, new_values=new_values, cache_keys=cache_keys, cache_values=cache_values, cache_lengths=cache_lengths, out_weight=out_weight, norm_gain=norm_gain, expert_ids=expert_ids, route_probs=route_probs, route_order=route_order, gate_weight=gate_weight, up_weight=up_weight, down_weight=down_weight)


EPSILON = 1e-05
GLU_SLOPE = 1.702

def attend(queries, new_keys, new_values, cache_keys, cache_values, cache_lengths):
    sequence_count, head_count, head_dim = queries.shape
    kv_heads = new_keys.shape[1]
    group_size = head_count // kv_heads
    scaling = 1.0 / head_dim ** 0.5
    query_rows = queries.astype(jnp.float32).reshape(sequence_count, kv_heads, group_size, head_dim)
    scores = jnp.einsum('sgqd,sgdc->sgqc', query_rows, cache_keys.astype(jnp.float32)) * scaling
    own_score = jnp.einsum('sgqd,sgd->sgq', query_rows, new_keys.astype(jnp.float32)) * scaling
    positions = jnp.arange(cache_keys.shape[3], dtype=jnp.int32)
    visible = positions[None, :] < cache_lengths[:, None]
    scores = jnp.where(visible[:, None, None, :], scores, -1e+30)
    highest = jnp.maximum(lax.optimization_barrier(jnp.max(scores, axis=3)), own_score)
    cache_exp = jnp.exp(scores - highest[..., None])
    own_exp = jnp.exp(own_score - highest)
    totals = lax.optimization_barrier(jnp.sum(cache_exp, axis=3)) + own_exp
    cache_prob = (cache_exp / totals[..., None]).astype(jnp.bfloat16)
    own_prob = (own_exp / totals).astype(jnp.bfloat16)
    attended = jnp.einsum('sgqc,sgdc->sgqd', cache_prob.astype(jnp.float32), cache_values.astype(jnp.float32))
    attended = attended + own_prob.astype(jnp.float32)[..., None] * new_values.astype(jnp.float32)[:, :, None, :]
    return attended.astype(jnp.bfloat16).reshape(sequence_count, head_count * head_dim)

def apply_norm(residual, norm_gain):
    mean_square = lax.optimization_barrier(jnp.mean(residual * residual, axis=1, keepdims=True))
    return (residual * lax.rsqrt(mean_square + EPSILON) * norm_gain).astype(jnp.bfloat16)

def route_tables(expert_ids, route_probs, route_order, experts, capacity):
    tokens, top_count = expert_ids.shape
    flat_ids = expert_ids.reshape(tokens * top_count)
    expert_mark = (flat_ids[:, None] == jnp.arange(experts, dtype=jnp.int32)[None, :]).astype(jnp.int32)
    earlier = jnp.cumsum(expert_mark, axis=0) - expert_mark
    position = lax.optimization_barrier(jnp.sum(earlier * expert_mark, axis=1))
    slot_code = flat_ids * capacity + position
    slot_table = slot_code[:, None] == jnp.arange(experts * capacity, dtype=jnp.int32)[None, :]
    slot_table = slot_table.astype(jnp.float32).reshape(tokens, top_count, experts * capacity)
    picked = jnp.zeros((tokens, top_count), jnp.float32)
    for column in range(top_count):
        picked = picked + jnp.where(route_order == column, route_probs[:, column:column + 1], 0.0)
    weights = picked / lax.optimization_barrier(jnp.sum(route_probs, axis=1, keepdims=True))
    select_experts = lax.optimization_barrier(jnp.sum(slot_table, axis=1))
    weighted_output = lax.optimization_barrier(jnp.sum(slot_table * weights[:, :, None], axis=1))
    return (select_experts, weighted_output)

def expert_block(operands):
    token_rows, gate_part, up_part, down_part = operands
    gate_sums = jnp.dot(token_rows, gate_part, preferred_element_type=jnp.float32)
    upward = jnp.dot(token_rows, up_part, preferred_element_type=jnp.float32)
    active = (gate_sums * jax.nn.sigmoid(GLU_SLOPE * gate_sums) * (upward + 1.0)).astype(jnp.bfloat16)
    return jnp.dot(active, down_part, preferred_element_type=jnp.float32)

def reference(hidden_in, queries, new_keys, new_values, cache_keys, cache_values, cache_lengths, out_weight, norm_gain, expert_ids, route_probs, route_order, gate_weight, up_weight, down_weight):
    attended = attend(queries, new_keys, new_values, cache_keys, cache_values, cache_lengths)
    attention = jnp.dot(attended, out_weight, preferred_element_type=jnp.float32)
    residual = hidden_in.astype(jnp.float32) + attention
    normed = apply_norm(residual, norm_gain)
    blocks = SEQS // SEQ_DEV
    tables = jax.vmap(partial(route_tables, experts=EXPERTS, capacity=CAP))
    select_experts, weighted_output = tables(expert_ids.reshape(blocks, SEQ_DEV, TOP), route_probs.reshape(blocks, SEQ_DEV, TOP), route_order.reshape(blocks, SEQ_DEV, TOP))
    block_row_count = normed.astype(jnp.float32).reshape(blocks, SEQ_DEV, D)
    token_rows = jnp.einsum('cgh,cga->cha', select_experts, block_row_count, precision=lax.Precision.HIGHEST).astype(jnp.bfloat16)
    token_rows = token_rows.reshape(blocks, EXPERTS, CAP, D).transpose(1, 0, 2, 3).reshape(EXPERTS, blocks * CAP, D)
    expert_output = lax.map(expert_block, (token_rows, gate_weight, up_weight, down_weight))
    expert_output = expert_output.reshape(EXPERTS, blocks, CAP, D).transpose(1, 0, 2, 3).reshape(blocks, EXPERTS * CAP, D)
    expert_mixture = jnp.einsum('nyz,nzs->nys', weighted_output, expert_output, precision=lax.Precision.HIGHEST)
    return (residual + expert_mixture.reshape(SEQS, D)).astype(jnp.bfloat16)
```

```python
import jax
import jax.numpy as jnp
from jax import lax
from jax.sharding import PartitionSpec as P

EPSILON = 1e-05
GLU_SLOPE = 1.702


def attend(queries, new_keys, new_values, cache_keys, cache_values, cache_lengths):
    sequence_count, head_count, head_dim = queries.shape
    kv_heads = new_keys.shape[1]
    group_size = head_count // kv_heads
    scaling = 1.0 / head_dim**0.5
    query_rows = queries.reshape(sequence_count, kv_heads, group_size, head_dim)
    scores = (
        jnp.einsum("sgqd,sgdc->sgqc", query_rows, cache_keys, preferred_element_type=jnp.float32)
        * scaling
    )
    own_score = (
        jnp.einsum("sgqd,sgd->sgq", query_rows, new_keys, preferred_element_type=jnp.float32)
        * scaling
    )
    positions = jnp.arange(cache_keys.shape[3], dtype=jnp.int32)
    visible = positions[None, :] < cache_lengths[:, None]
    scores = jnp.where(visible[:, None, None, :], scores, -1e30)
    highest = jnp.maximum(jnp.max(scores, axis=3), own_score)
    cache_exp = jnp.exp(scores - highest[..., None])
    own_exp = jnp.exp(own_score - highest)
    totals = jnp.sum(cache_exp, axis=3) + own_exp
    cache_prob = (cache_exp / totals[..., None]).astype(jnp.bfloat16)
    own_prob = (own_exp / totals).astype(jnp.bfloat16)
    attended = jnp.einsum(
        "sgqc,sgdc->sgqd", cache_prob, cache_values, preferred_element_type=jnp.float32
    )
    attended = (
        attended
        + own_prob.astype(jnp.float32)[..., None] * new_values.astype(jnp.float32)[:, :, None, :]
    )
    return attended.astype(jnp.bfloat16).reshape(sequence_count, head_count * head_dim)


def apply_norm(residual, norm_gain):
    mean_square = jnp.mean(residual * residual, axis=1, keepdims=True)
    return (residual * lax.rsqrt(mean_square + EPSILON) * norm_gain).astype(jnp.bfloat16)


def route_tables(expert_ids, route_probs, route_order, experts, capacity):
    tokens, top_count = expert_ids.shape
    flat_ids = expert_ids.reshape(tokens * top_count)
    expert_mark = (flat_ids[:, None] == jnp.arange(experts, dtype=jnp.int32)[None, :]).astype(
        jnp.int32
    )
    earlier = jnp.cumsum(expert_mark, axis=0) - expert_mark
    position = jnp.sum(earlier * expert_mark, axis=1)
    slot_code = flat_ids * capacity + position
    slot_table = slot_code[:, None] == jnp.arange(experts * capacity, dtype=jnp.int32)[None, :]
    slot_table = slot_table.astype(jnp.float32).reshape(tokens, top_count, experts * capacity)
    picked = jnp.zeros((tokens, top_count), jnp.float32)
    for column in range(top_count):
        picked = picked + jnp.where(route_order == column, route_probs[:, column : column + 1], 0.0)
    weights = picked / jnp.sum(route_probs, axis=1, keepdims=True)
    select_experts = jnp.sum(slot_table, axis=1)
    weighted_output = jnp.sum(slot_table * weights[:, :, None], axis=1)
    return (select_experts, weighted_output)


def sum_over(values, axis, ranks):
    step = 1
    while step < ranks:
        pairs = [(rank, rank ^ step) for rank in range(ranks)]
        values = values + lax.ppermute(values.astype(jnp.bfloat16), axis, pairs).astype(jnp.float32)
        step *= 2
    return values


def per_device(
    hidden_in,
    queries,
    new_keys,
    new_values,
    cache_keys,
    cache_values,
    cache_lengths,
    out_weight,
    norm_gain,
    expert_ids,
    route_probs,
    route_order,
    gate_weight,
    up_weight,
    down_weight,
):
    sequence_count, model_width = hidden_in.shape
    expert_ranks = lax.axis_size("expert")
    tensor_ranks = lax.axis_size("tensor")
    local_experts = gate_weight.shape[0]
    experts = local_experts * expert_ranks
    top_count = expert_ids.shape[1]
    capacity = min(sequence_count, max(2, (sequence_count * top_count + experts - 1) // experts))
    slab_width = model_width // tensor_ranks
    offset = lax.axis_index("tensor") * slab_width
    attended = attend(queries, new_keys, new_values, cache_keys, cache_values, cache_lengths)
    partial_sums = jnp.dot(attended, out_weight, preferred_element_type=jnp.float32)
    attention = sum_over(partial_sums, "tensor", tensor_ranks)
    residual = hidden_in.astype(jnp.float32) + attention
    normed = apply_norm(residual, norm_gain)
    select_experts, weighted_output = route_tables(
        expert_ids, route_probs, route_order, experts, capacity
    )
    outgoing = jnp.dot(
        select_experts.T.astype(jnp.bfloat16), normed, preferred_element_type=jnp.float32
    ).astype(jnp.bfloat16)
    outgoing = outgoing.reshape(expert_ranks, local_experts * capacity, model_width)
    arrived = lax.all_to_all(outgoing, "expert", split_axis=0, concat_axis=0, tiled=True)
    arrived = arrived.reshape(expert_ranks, local_experts, capacity, model_width)
    gate_sums = jnp.einsum(
        "secd,edf->secf", arrived, gate_weight, preferred_element_type=jnp.float32
    )
    upward = jnp.einsum("secd,edf->secf", arrived, up_weight, preferred_element_type=jnp.float32)
    active = (gate_sums * jax.nn.sigmoid(GLU_SLOPE * gate_sums) * (upward + 1.0)).astype(
        jnp.bfloat16
    )
    expert_part = jnp.einsum(
        "secf,efd->secd", active, down_weight, preferred_element_type=jnp.float32
    )
    rows = local_experts * capacity
    slabs = expert_part.astype(jnp.bfloat16).reshape(expert_ranks, rows, tensor_ranks, slab_width)
    slabs = slabs.transpose(0, 2, 1, 3).reshape(expert_ranks * tensor_ranks, rows, slab_width)
    kept = lax.dynamic_slice_in_dim(residual, offset, slab_width, 1)
    returned = lax.all_to_all(
        slabs, ("expert", "tensor"), split_axis=0, concat_axis=0, tiled=True
    )
    returned = returned.reshape(expert_ranks, tensor_ranks, rows, slab_width)
    returned = jnp.sum(returned.astype(jnp.float32), axis=1).reshape(experts * capacity, slab_width)
    blended = jnp.dot(weighted_output, returned, precision=lax.Precision.HIGHEST)
    return (kept + blended).astype(jnp.bfloat16)


def solution(mesh):
    in_specs = (
        P(("groups", "expert"), None),
        P(("groups", "expert"), "tensor", None),
        P(("groups", "expert"), "tensor", None),
        P(("groups", "expert"), "tensor", None),
        P(("groups", "expert"), "tensor", None, None),
        P(("groups", "expert"), "tensor", None, None),
        P(("groups", "expert")),
        P("tensor", None),
        P(),
        P(("groups", "expert"), None),
        P(("groups", "expert"), None),
        P(("groups", "expert"), None),
        P("expert", None, "tensor"),
        P("expert", None, "tensor"),
        P("expert", "tensor", None),
    )
    out_specs = P(("groups", "expert"), "tensor")
    return jax.shard_map(
        per_device, mesh=mesh, in_specs=in_specs, out_specs=out_specs, check_vma=False
    )
```

```python
import functools

import jax
import jax.numpy as jnp
from jax import lax
from jax.experimental import pallas as pl
from jax.experimental.pallas import tpu as pltpu
from jax.sharding import PartitionSpec as P

EPSILON = 1e-05
GLU_SLOPE = 1.702
WINDOW_FLOPS = 20_000_000_000


def attend(queries, new_keys, new_values, cache_keys, cache_values, cache_lengths):
    sequence_count, head_count, head_dim = queries.shape
    kv_heads = new_keys.shape[1]
    group_size = head_count // kv_heads
    scaling = 1.0 / head_dim**0.5
    query_rows = queries.reshape(sequence_count, kv_heads, group_size, head_dim)
    scores = (
        jnp.einsum("sgqd,sgdc->sgqc", query_rows, cache_keys, preferred_element_type=jnp.float32)
        * scaling
    )
    own_score = (
        jnp.einsum("sgqd,sgd->sgq", query_rows, new_keys, preferred_element_type=jnp.float32)
        * scaling
    )
    positions = jnp.arange(cache_keys.shape[3], dtype=jnp.int32)
    visible = positions[None, :] < cache_lengths[:, None]
    scores = jnp.where(visible[:, None, None, :], scores, -1e30)
    highest = jnp.maximum(jnp.max(scores, axis=3), own_score)
    cache_exp = jnp.exp(scores - highest[..., None])
    own_exp = jnp.exp(own_score - highest)
    totals = jnp.sum(cache_exp, axis=3) + own_exp
    cache_prob = (cache_exp / totals[..., None]).astype(jnp.bfloat16)
    own_prob = (own_exp / totals).astype(jnp.bfloat16)
    attended = jnp.einsum(
        "sgqc,sgdc->sgqd", cache_prob, cache_values, preferred_element_type=jnp.float32
    )
    attended = (
        attended
        + own_prob.astype(jnp.float32)[..., None] * new_values.astype(jnp.float32)[:, :, None, :]
    )
    return attended.astype(jnp.bfloat16).reshape(sequence_count, head_count * head_dim)


VMEM = pl.BlockSpec(memory_space=pltpu.VMEM)
LAST_DIMS = (((1,), (1,)), ((), ()))
FIRST_DIMS = (((0,), (0,)), ((), ()))
MIB = 1 << 20


def call(kernel, outs, args, flops, moved, limit):
    return pl.pallas_call(
        kernel,
        out_shape=[jax.ShapeDtypeStruct(shape, dtype) for shape, dtype in outs],
        in_specs=[VMEM] * len(args),
        out_specs=[VMEM] * len(outs),
        compiler_params=pltpu.CompilerParams(vmem_limit_bytes=limit),
        cost_estimate=pl.CostEstimate(flops=flops, bytes_accessed=moved, transcendentals=0),
    )(*args)


def route_weights(expert_ids, route_probs, route_order, experts):
    picked = jnp.zeros(expert_ids.shape, jnp.float32)
    for column in range(expert_ids.shape[1]):
        picked = picked + jnp.where(route_order == column, route_probs[:, column : column + 1], 0.0)
    weights = picked / jnp.sum(route_probs, axis=1, keepdims=True)
    named = expert_ids[:, :, None] == jnp.arange(experts, dtype=jnp.int32)[None, None, :]
    return jnp.sum(jnp.where(named, weights[:, :, None], 0.0), axis=1)


def exchange(values, axis, ranks):
    step = 1
    while True:
        pairs = [(rank, rank ^ step) for rank in range(ranks)]
        received = lax.ppermute(values.astype(jnp.bfloat16), axis, pairs)
        step *= 2
        if step >= ranks:
            return values, received
        values = values + received.astype(jnp.float32)


def norm_kernel(mine_ref, received_ref, hidden_ref, gain_ref, table_ref, residual_ref, rows_ref):
    width = hidden_ref.shape[1]
    residual = (
        hidden_ref[...].astype(jnp.float32) + mine_ref[...] + received_ref[...].astype(jnp.float32)
    )
    residual_ref[...] = residual
    mean_square = jnp.mean(residual * residual, axis=1, keepdims=True)
    normed = residual * lax.rsqrt(mean_square + EPSILON) * gain_ref[...]
    rows_ref[:, :width] = normed.astype(jnp.bfloat16)
    rows_ref[:, width:] = table_ref[...]


def expert_kernel(blocks, experts, *refs):
    row_refs = refs[:blocks]
    gate_ref, up_ref, down_ref, mine_ref, other_ref = refs[blocks:]
    local_experts, _, width = down_ref.shape
    rows = jnp.concatenate([ref[:, :width] for ref in row_refs], axis=0)
    table = jnp.concatenate([ref[:, width:] for ref in row_refs], axis=0).astype(jnp.float32)
    column = lax.broadcasted_iota(jnp.int32, table.shape, 1)
    total = None
    for local in range(local_experts):
        expert = lax.axis_index("expert") * local_experts + local
        chosen = (column == expert) | (column == expert + experts)
        weight = jnp.sum(jnp.where(chosen, table, 0.0), axis=1, keepdims=True)
        gate = lax.dot_general(
            gate_ref[local], rows, LAST_DIMS, preferred_element_type=jnp.float32
        )
        up = lax.dot_general(up_ref[local], rows, LAST_DIMS, preferred_element_type=jnp.float32)
        active = (gate * jax.nn.sigmoid(GLU_SLOPE * gate) * (up + 1.0)).astype(jnp.bfloat16)
        part = lax.dot_general(
            active, down_ref[local], FIRST_DIMS, preferred_element_type=jnp.float32
        )
        part = part * weight
        total = part if total is None else total + part
    half = mine_ref.shape[0]
    mine_ref[...] = total[:half]
    if other_ref.shape[0] == half:
        other_ref[...] = total[half:].astype(jnp.bfloat16)


def split_kernel(mine_ref, received_ref, kept_ref, *sent_refs):
    size = kept_ref.shape[0]
    kept_ref[...] = mine_ref[:size] + received_ref[:size].astype(jnp.float32)
    for number, sent_ref in enumerate(sent_refs, 1):
        block = pl.ds(number * size, size)
        total = mine_ref[block] + received_ref[block].astype(jnp.float32)
        sent_ref[...] = total.astype(jnp.bfloat16)


def gather_kernel(kept_ref, *refs):
    *received_refs, total_ref = refs
    total = kept_ref[...]
    for received_ref in received_refs:
        total = total + received_ref[...].astype(jnp.float32)
    total_ref[...] = total


def per_device(
    hidden_in,
    queries,
    new_keys,
    new_values,
    cache_keys,
    cache_values,
    cache_lengths,
    out_weight,
    norm_gain,
    expert_ids,
    route_probs,
    route_order,
    gate_weight,
    up_weight,
    down_weight,
):
    sequences, width = hidden_in.shape
    expert_ranks = lax.axis_size("expert")
    tensor_ranks = lax.axis_size("tensor")
    local_experts, hidden_units = down_weight.shape[:2]
    experts = local_experts * expert_ranks
    inner = 2
    outer = expert_ranks // inner
    slab_width = width // tensor_ranks
    offset = lax.axis_index("tensor") * slab_width
    row_width = -(-(width + 2 * experts) // 128) * 128

    def to_outer(values, step):
        pairs = [(rank, rank ^ (step * inner)) for rank in range(expert_ranks)]
        return lax.ppermute(values, "expert", pairs)

    def to_inner(values):
        return lax.ppermute(values, "expert", [(rank, rank ^ 1) for rank in range(expert_ranks)])

    attended = attend(queries, new_keys, new_values, cache_keys, cache_values, cache_lengths)
    partial_sums = jnp.dot(attended, out_weight, preferred_element_type=jnp.float32)
    mine, received = exchange(partial_sums, "tensor", tensor_ranks)

    weights = route_weights(expert_ids, route_probs, route_order, experts)
    high = weights.astype(jnp.bfloat16)
    low = (weights - high.astype(jnp.float32)).astype(jnp.bfloat16)
    spare = jnp.zeros((sequences, row_width - width - 2 * experts), jnp.bfloat16)
    table = jnp.concatenate([high, low, spare], axis=1)

    block = (sequences, width)
    residual, rows = call(
        norm_kernel,
        [(block, jnp.float32), ((sequences, row_width), jnp.bfloat16)],
        (mine, received, hidden_in, norm_gain.reshape(1, width), table),
        flops=WINDOW_FLOPS,
        moved=sequences * width * 16,
        limit=2 * MIB,
    )

    near = [rows] + [to_outer(rows, step) for step in range(1, outer)]
    far = [to_inner(piece) for piece in near]
    half = (outer * sequences, width)
    mine, other = call(
        functools.partial(expert_kernel, 2 * outer, experts),
        [(half, jnp.float32), (half, jnp.bfloat16)],
        (*near, *far, gate_weight.swapaxes(1, 2), up_weight.swapaxes(1, 2), down_weight),
        flops=12 * half[0] * width * hidden_units * local_experts,
        moved=6 * width * hidden_units * local_experts,
        limit=16 * MIB,
    )
    received = to_inner(other)
    kept, *sent = call(
        split_kernel,
        [(block, jnp.float32)] + [(block, jnp.bfloat16)] * (outer - 1),
        (mine, received),
        flops=half[0] * width,
        moved=half[0] * width * 8,
        limit=4 * MIB,
    )
    returned = [to_outer(piece, step) for step, piece in enumerate(sent, 1)]
    (mixture,) = call(
        gather_kernel,
        [(block, jnp.float32)],
        (kept, *returned),
        flops=half[0] * width,
        moved=half[0] * width * 2,
        limit=2 * MIB,
    )
    mine, received = exchange(mixture, "tensor", tensor_ranks)
    total = residual + mine + received.astype(jnp.float32)
    return lax.dynamic_slice_in_dim(total, offset, slab_width, 1).astype(jnp.bfloat16)


def solution(mesh):
    in_specs = (
        P(("groups", "expert"), None),
        P(("groups", "expert"), "tensor", None),
        P(("groups", "expert"), "tensor", None),
        P(("groups", "expert"), "tensor", None),
        P(("groups", "expert"), "tensor", None, None),
        P(("groups", "expert"), "tensor", None, None),
        P(("groups", "expert")),
        P("tensor", None),
        P(),
        P(("groups", "expert"), None),
        P(("groups", "expert"), None),
        P(("groups", "expert"), None),
        P("expert", None, "tensor"),
        P("expert", None, "tensor"),
        P("expert", "tensor", None),
    )
    out_specs = P(("groups", "expert"), "tensor")
    return jax.shard_map(
        per_device, mesh=mesh, in_specs=in_specs, out_specs=out_specs, check_vma=False
    )
```

```python
import functools

import jax
import jax.numpy as jnp
from jax import lax
from jax.experimental import pallas as pl
from jax.experimental.pallas import tpu as pltpu
from jax.sharding import PartitionSpec as P

EPSILON = 1e-05
GLU_SLOPE = 1.702
WINDOW_FLOPS = 200_000_000_000


def attend(queries, new_keys, new_values, cache_keys, cache_values, cache_lengths):
    sequence_count, head_count, head_dim = queries.shape
    kv_heads = new_keys.shape[1]
    group_size = head_count // kv_heads
    scaling = 1.0 / head_dim**0.5
    query_rows = queries.reshape(sequence_count, kv_heads, group_size, head_dim)
    scores = (
        jnp.einsum("sgqd,sgdc->sgqc", query_rows, cache_keys, preferred_element_type=jnp.float32)
        * scaling
    )
    own_score = (
        jnp.einsum("sgqd,sgd->sgq", query_rows, new_keys, preferred_element_type=jnp.float32)
        * scaling
    )
    positions = jnp.arange(cache_keys.shape[3], dtype=jnp.int32)
    visible = positions[None, :] < cache_lengths[:, None]
    scores = jnp.where(visible[:, None, None, :], scores, -1e30)
    highest = jnp.maximum(jnp.max(scores, axis=3), own_score)
    cache_exp = jnp.exp(scores - highest[..., None])
    own_exp = jnp.exp(own_score - highest)
    totals = jnp.sum(cache_exp, axis=3) + own_exp
    cache_prob = (cache_exp / totals[..., None]).astype(jnp.bfloat16)
    own_prob = (own_exp / totals).astype(jnp.bfloat16)
    attended = jnp.einsum(
        "sgqc,sgdc->sgqd", cache_prob, cache_values, preferred_element_type=jnp.float32
    )
    attended = (
        attended
        + own_prob.astype(jnp.float32)[..., None] * new_values.astype(jnp.float32)[:, :, None, :]
    )
    return attended.astype(jnp.bfloat16).reshape(sequence_count, head_count * head_dim)


VMEM = pl.BlockSpec(memory_space=pltpu.VMEM)
LAST_DIMS = (((1,), (1,)), ((), ()))
FIRST_DIMS = (((0,), (0,)), ((), ()))
MIB = 1 << 20


def call(kernel, outs, args, flops, moved, limit):
    return pl.pallas_call(
        kernel,
        out_shape=[jax.ShapeDtypeStruct(shape, dtype) for shape, dtype in outs],
        in_specs=[VMEM] * len(args),
        out_specs=[VMEM] * len(outs),
        compiler_params=pltpu.CompilerParams(vmem_limit_bytes=limit),
        cost_estimate=pl.CostEstimate(flops=flops, bytes_accessed=moved, transcendentals=0),
    )(*args)


def route_weights(expert_ids, route_probs, route_order, experts):
    picked = jnp.zeros(expert_ids.shape, jnp.float32)
    for column in range(expert_ids.shape[1]):
        picked = picked + jnp.where(route_order == column, route_probs[:, column : column + 1], 0.0)
    weights = picked / jnp.sum(route_probs, axis=1, keepdims=True)
    named = expert_ids[:, :, None] == jnp.arange(experts, dtype=jnp.int32)[None, None, :]
    return jnp.sum(jnp.where(named, weights[:, :, None], 0.0), axis=1)


def exchange(values, axis, ranks):
    step = 1
    while True:
        pairs = [(rank, rank ^ step) for rank in range(ranks)]
        received = lax.ppermute(values.astype(jnp.bfloat16), axis, pairs)
        step *= 2
        if step >= ranks:
            return values, received
        values = values + received.astype(jnp.float32)


def norm_kernel(mine_ref, received_ref, hidden_ref, gain_ref, table_ref, residual_ref, rows_ref):
    width = hidden_ref.shape[1]
    residual = (
        hidden_ref[...].astype(jnp.float32) + mine_ref[...] + received_ref[...].astype(jnp.float32)
    )
    residual_ref[...] = residual
    mean_square = jnp.mean(residual * residual, axis=1, keepdims=True)
    normed = residual * lax.rsqrt(mean_square + EPSILON) * gain_ref[...]
    rows_ref[:, :width] = normed.astype(jnp.bfloat16)
    rows_ref[:, width:] = table_ref[...]


def expert_kernel(blocks, experts, *refs):
    row_refs = refs[:blocks]
    gate_ref, up_ref, down_ref, mine_ref, other_ref = refs[blocks:]
    local_experts, _, width = down_ref.shape
    rows = jnp.concatenate([ref[:, :width] for ref in row_refs], axis=0)
    table = jnp.concatenate([ref[:, width:] for ref in row_refs], axis=0).astype(jnp.float32)
    column = lax.broadcasted_iota(jnp.int32, table.shape, 1)
    total = None
    for local in range(local_experts):
        expert = lax.axis_index("expert") * local_experts + local
        chosen = (column == expert) | (column == expert + experts)
        weight = jnp.sum(jnp.where(chosen, table, 0.0), axis=1, keepdims=True)
        gate = lax.dot_general(
            gate_ref[local], rows, LAST_DIMS, preferred_element_type=jnp.float32
        )
        up = lax.dot_general(up_ref[local], rows, LAST_DIMS, preferred_element_type=jnp.float32)
        active = (gate * jax.nn.sigmoid(GLU_SLOPE * gate) * (up + 1.0)).astype(jnp.bfloat16)
        part = lax.dot_general(
            active, down_ref[local], FIRST_DIMS, preferred_element_type=jnp.float32
        )
        part = part * weight
        total = part if total is None else total + part
    half = mine_ref.shape[0]
    mine_ref[...] = total[:half]
    if other_ref.shape[0] == half:
        other_ref[...] = total[half:].astype(jnp.bfloat16)


def split_kernel(mine_ref, received_ref, kept_ref, *sent_refs):
    size = kept_ref.shape[0]
    kept_ref[...] = mine_ref[:size] + received_ref[:size].astype(jnp.float32)
    for number, sent_ref in enumerate(sent_refs, 1):
        block = pl.ds(number * size, size)
        total = mine_ref[block] + received_ref[block].astype(jnp.float32)
        sent_ref[...] = total.astype(jnp.bfloat16)


def gather_kernel(kept_ref, *refs):
    *received_refs, total_ref = refs
    total = kept_ref[...]
    for received_ref in received_refs:
        total = total + received_ref[...].astype(jnp.float32)
    total_ref[...] = total


def per_device(
    hidden_in,
    queries,
    new_keys,
    new_values,
    cache_keys,
    cache_values,
    cache_lengths,
    out_weight,
    norm_gain,
    expert_ids,
    route_probs,
    route_order,
    gate_weight,
    up_weight,
    down_weight,
):
    sequences, width = hidden_in.shape
    expert_ranks = lax.axis_size("expert")
    tensor_ranks = lax.axis_size("tensor")
    local_experts, hidden_units = down_weight.shape[:2]
    experts = local_experts * expert_ranks
    inner = 2
    outer = expert_ranks // inner
    slab_width = width // tensor_ranks
    offset = lax.axis_index("tensor") * slab_width
    row_width = -(-(width + 2 * experts) // 128) * 128

    def to_outer(values, step):
        pairs = [(rank, rank ^ (step * inner)) for rank in range(expert_ranks)]
        return lax.ppermute(values, "expert", pairs)

    def to_inner(values):
        return lax.ppermute(values, "expert", [(rank, rank ^ 1) for rank in range(expert_ranks)])

    attended = attend(queries, new_keys, new_values, cache_keys, cache_values, cache_lengths)
    partial_sums = jnp.dot(attended, out_weight, preferred_element_type=jnp.float32)
    mine, received = exchange(partial_sums, "tensor", tensor_ranks)

    weights = route_weights(expert_ids, route_probs, route_order, experts)
    high = weights.astype(jnp.bfloat16)
    low = (weights - high.astype(jnp.float32)).astype(jnp.bfloat16)
    spare = jnp.zeros((sequences, row_width - width - 2 * experts), jnp.bfloat16)
    table = jnp.concatenate([high, low, spare], axis=1)

    block = (sequences, width)
    residual, rows = call(
        norm_kernel,
        [(block, jnp.float32), ((sequences, row_width), jnp.bfloat16)],
        (mine, received, hidden_in, norm_gain.reshape(1, width), table),
        flops=WINDOW_FLOPS,
        moved=sequences * width * 16,
        limit=2 * MIB,
    )

    near = [rows] + [to_outer(rows, step) for step in range(1, outer)]
    far = [to_inner(piece) for piece in near]
    half = (outer * sequences, width)
    mine, other = call(
        functools.partial(expert_kernel, 2 * outer, experts),
        [(half, jnp.float32), (half, jnp.bfloat16)],
        (*near, *far, gate_weight.swapaxes(1, 2), up_weight.swapaxes(1, 2), down_weight),
        flops=12 * half[0] * width * hidden_units * local_experts,
        moved=6 * width * hidden_units * local_experts,
        limit=16 * MIB,
    )
    received = to_inner(other)
    kept, *sent = call(
        split_kernel,
        [(block, jnp.float32)] + [(block, jnp.bfloat16)] * (outer - 1),
        (mine, received),
        flops=half[0] * width,
        moved=half[0] * width * 8,
        limit=4 * MIB,
    )
    returned = [to_outer(piece, step) for step, piece in enumerate(sent, 1)]
    (mixture,) = call(
        gather_kernel,
        [(block, jnp.float32)],
        (kept, *returned),
        flops=half[0] * width,
        moved=half[0] * width * 2,
        limit=2 * MIB,
    )
    mine, received = exchange(mixture, "tensor", tensor_ranks)
    total = residual + mine + received.astype(jnp.float32)
    return lax.dynamic_slice_in_dim(total, offset, slab_width, 1).astype(jnp.bfloat16)


def solution(mesh):
    in_specs = (
        P(("groups", "expert"), None),
        P(("groups", "expert"), "tensor", None),
        P(("groups", "expert"), "tensor", None),
        P(("groups", "expert"), "tensor", None),
        P(("groups", "expert"), "tensor", None, None),
        P(("groups", "expert"), "tensor", None, None),
        P(("groups", "expert")),
        P("tensor", None),
        P(),
        P(("groups", "expert"), None),
        P(("groups", "expert"), None),
        P(("groups", "expert"), None),
        P("expert", None, "tensor"),
        P("expert", None, "tensor"),
        P("expert", "tensor", None),
    )
    out_specs = P(("groups", "expert"), "tensor")
    return jax.shard_map(
        per_device, mesh=mesh, in_specs=in_specs, out_specs=out_specs, check_vma=False
    )
```

```python
import functools

import jax
import jax.numpy as jnp
from jax import lax
from jax.experimental import pallas as pl
from jax.experimental.pallas import tpu as pltpu
from jax.sharding import PartitionSpec as P

EPSILON = 1e-05
GLU_SLOPE = 1.702
WINDOW_FLOPS = 200_000_000_000


def attend(queries, new_keys, new_values, cache_keys, cache_values, cache_lengths):
    sequence_count, head_count, head_dim = queries.shape
    kv_heads = new_keys.shape[1]
    group_size = head_count // kv_heads
    scaling = 1.0 / head_dim**0.5
    query_rows = queries.reshape(sequence_count, kv_heads, group_size, head_dim)
    scores = (
        jnp.einsum("sgqd,sgdc->sgqc", query_rows, cache_keys, preferred_element_type=jnp.float32)
        * scaling
    )
    own_score = (
        jnp.einsum("sgqd,sgd->sgq", query_rows, new_keys, preferred_element_type=jnp.float32)
        * scaling
    )
    positions = jnp.arange(cache_keys.shape[3], dtype=jnp.int32)
    visible = positions[None, :] < cache_lengths[:, None]
    scores = jnp.where(visible[:, None, None, :], scores, -1e30)
    highest = jnp.maximum(jnp.max(scores, axis=3), own_score)
    cache_exp = jnp.exp(scores - highest[..., None])
    own_exp = jnp.exp(own_score - highest)
    totals = jnp.sum(cache_exp, axis=3) + own_exp
    cache_prob = (cache_exp / totals[..., None]).astype(jnp.bfloat16)
    own_prob = (own_exp / totals).astype(jnp.bfloat16)
    attended = jnp.einsum(
        "sgqc,sgdc->sgqd", cache_prob, cache_values, preferred_element_type=jnp.float32
    )
    attended = (
        attended
        + own_prob.astype(jnp.float32)[..., None] * new_values.astype(jnp.float32)[:, :, None, :]
    )
    return attended.astype(jnp.bfloat16).reshape(sequence_count, head_count * head_dim)


VMEM = pl.BlockSpec(memory_space=pltpu.VMEM)
LAST_DIMS = (((1,), (1,)), ((), ()))
FIRST_DIMS = (((0,), (0,)), ((), ()))
MIB = 1 << 20


def call(kernel, outs, args, flops, moved, limit):
    return pl.pallas_call(
        kernel,
        out_shape=[jax.ShapeDtypeStruct(shape, dtype) for shape, dtype in outs],
        in_specs=[VMEM] * len(args),
        out_specs=[VMEM] * len(outs),
        compiler_params=pltpu.CompilerParams(vmem_limit_bytes=limit),
        cost_estimate=pl.CostEstimate(flops=flops, bytes_accessed=moved, transcendentals=0),
    )(*args)


def mm(left, right, dims=(((1,), (0,)), ((), ()))):
    return lax.dot_general(left, right, dims, preferred_element_type=jnp.float32)


def iota(shape, dim):
    return lax.broadcasted_iota(jnp.int32, shape, dim)


def attend_kernel(
    lengths_ref,
    queries_ref,
    new_keys_ref,
    new_values_ref,
    keys_hbm,
    values_hbm,
    weight_hbm,
    mine_ref,
    sent_ref,
    keys_ref,
    values_ref,
    weight_ref,
    own_keys_ref,
    own_values_ref,
    attended_ref,
    arrived,
):
    sequences, heads, head_dim = queries_ref.shape
    kv_heads = new_keys_ref.shape[1]
    group = heads // kv_heads
    span = kv_heads * head_dim
    lanes = group * head_dim
    copies = [
        pltpu.make_async_copy(keys_hbm, keys_ref, arrived.at[0]),
        pltpu.make_async_copy(values_hbm, values_ref, arrived.at[1]),
        pltpu.make_async_copy(weight_hbm, weight_ref, arrived.at[2]),
    ]
    for copy in copies:
        copy.start()

    rows = sequences * heads
    scaling = 1.0 / head_dim**0.5
    queries = queries_ref[...].reshape(rows, head_dim)
    for sequence in range(sequences):
        block = pl.ds(sequence * kv_heads, kv_heads)
        own_keys_ref[block] = new_keys_ref[sequence].astype(jnp.float32)
        own_values_ref[block] = new_values_ref[sequence].astype(jnp.float32)
    own_keys = own_keys_ref[...].astype(jnp.bfloat16)
    own_values = own_values_ref[...].astype(jnp.bfloat16)

    spread = (iota((head_dim, span), 0) == iota((head_dim, span), 1) % head_dim).astype(
        jnp.bfloat16
    )
    same_head = iota((rows, span), 1) // head_dim == iota((rows, span), 0) % heads // group
    wide = jnp.where(same_head, mm(queries, spread), 0.0).astype(jnp.bfloat16)
    pairs = (rows, sequences * kv_heads)
    own_pair = iota(pairs, 1) == iota(pairs, 0) // group
    own_score = (
        jnp.sum(jnp.where(own_pair, mm(queries, own_keys, LAST_DIMS), 0.0), axis=1, keepdims=True)
        * scaling
    )

    copies[0].wait()
    slots = keys_ref.shape[2]
    scores = []
    for sequence in range(sequences):
        block = slice(sequence * heads, (sequence + 1) * heads)
        score = mm(wide[block], keys_ref[sequence]) * scaling
        visible = iota((heads, slots), 1) < lengths_ref[sequence]
        scores.append(jnp.where(visible, score, -1e30))
    scores = jnp.concatenate(scores, axis=0)
    highest = jnp.maximum(jnp.max(scores, axis=1, keepdims=True), own_score)
    cache_exp = jnp.exp(scores - highest)
    own_exp = jnp.exp(own_score - highest)
    totals = jnp.sum(cache_exp, axis=1, keepdims=True) + own_exp
    cache_prob = (cache_exp / totals).astype(jnp.bfloat16)
    own_prob = own_exp / totals
    own_prob = jnp.where(own_pair, own_prob, 0.0).astype(jnp.bfloat16)
    own_part = mm(own_prob, mm(own_values, spread).astype(jnp.bfloat16))

    copies[1].wait()
    attended = [
        mm(
            cache_prob[sequence * heads : (sequence + 1) * heads],
            values_ref[sequence],
            LAST_DIMS,
        )
        for sequence in range(sequences)
    ]
    attended = jnp.concatenate(attended, axis=0) + own_part
    attended = jnp.where(same_head, attended, 0.0).astype(jnp.bfloat16)
    repeat = (iota((span, lanes), 0) % head_dim == iota((span, lanes), 1) % head_dim).astype(
        jnp.bfloat16
    )
    own_lanes = iota((rows, lanes), 1) // head_dim == iota((rows, lanes), 0) % group
    placed = jnp.where(own_lanes, mm(attended, repeat), 0.0).astype(jnp.bfloat16)
    sums = (kv_heads * sequences, rows)
    chosen = (iota(sums, 0) % sequences == iota(sums, 1) // heads) & (
        iota(sums, 0) // sequences == iota(sums, 1) % heads // group
    )
    by_head = mm(chosen.astype(jnp.bfloat16), placed)
    for head in range(kv_heads):
        attended_ref[:, head * lanes : (head + 1) * lanes] = by_head[
            head * sequences : (head + 1) * sequences
        ].astype(jnp.bfloat16)
    attended = attended_ref[...]

    copies[2].wait()
    part = mm(weight_ref[...], attended, LAST_DIMS).T
    mine_ref[...] = part
    sent_ref[...] = part.astype(jnp.bfloat16)


def attend_and_project(
    queries, new_keys, new_values, cache_keys, cache_values, cache_lengths, out_weight
):
    sequences, heads, head_dim = queries.shape
    kv_heads, slots = cache_keys.shape[1], cache_keys.shape[3]
    depth, width = out_weight.shape
    span = kv_heads * head_dim
    caches = (sequences, span, slots)
    hbm = pl.BlockSpec(memory_space=pltpu.HBM)
    return pl.pallas_call(
        attend_kernel,
        out_shape=[
            jax.ShapeDtypeStruct((sequences, width), jnp.float32),
            jax.ShapeDtypeStruct((sequences, width), jnp.bfloat16),
        ],
        in_specs=[pl.BlockSpec(memory_space=pltpu.SMEM)] + [VMEM] * 3 + [hbm] * 3,
        out_specs=[VMEM] * 2,
        scratch_shapes=[
            pltpu.VMEM(caches, jnp.bfloat16),
            pltpu.VMEM(caches, jnp.bfloat16),
            pltpu.VMEM((width, depth), jnp.bfloat16),
            pltpu.VMEM((sequences * kv_heads, head_dim), jnp.float32),
            pltpu.VMEM((sequences * kv_heads, head_dim), jnp.float32),
            pltpu.VMEM((sequences, depth), jnp.bfloat16),
            pltpu.SemaphoreType.DMA((3,)),
        ],
        compiler_params=pltpu.CompilerParams(vmem_limit_bytes=60 * MIB),
        cost_estimate=pl.CostEstimate(
            flops=2 * sequences * width * depth,
            bytes_accessed=2 * (width * depth + 2 * sequences * span * slots),
            transcendentals=sequences * heads * slots,
        ),
    )(
        cache_lengths,
        queries,
        new_keys,
        new_values,
        cache_keys.reshape(caches),
        cache_values.reshape(caches),
        out_weight.T,
    )


def route_weights(expert_ids, route_probs, route_order, experts):
    picked = jnp.zeros(expert_ids.shape, jnp.float32)
    for column in range(expert_ids.shape[1]):
        picked = picked + jnp.where(route_order == column, route_probs[:, column : column + 1], 0.0)
    weights = picked / jnp.sum(route_probs, axis=1, keepdims=True)
    named = expert_ids[:, :, None] == jnp.arange(experts, dtype=jnp.int32)[None, None, :]
    return jnp.sum(jnp.where(named, weights[:, :, None], 0.0), axis=1)


def exchange(values, sent, axis, ranks):
    step = 1
    while True:
        pairs = [(rank, rank ^ step) for rank in range(ranks)]
        received = lax.ppermute(sent, axis, pairs)
        step *= 2
        if step >= ranks:
            return values, received
        values = values + received.astype(jnp.float32)
        sent = values.astype(jnp.bfloat16)


def norm_kernel(mine_ref, received_ref, hidden_ref, gain_ref, table_ref, residual_ref, rows_ref):
    width = hidden_ref.shape[1]
    residual = (
        hidden_ref[...].astype(jnp.float32) + mine_ref[...] + received_ref[...].astype(jnp.float32)
    )
    residual_ref[...] = residual
    mean_square = jnp.mean(residual * residual, axis=1, keepdims=True)
    normed = residual * lax.rsqrt(mean_square + EPSILON) * gain_ref[...]
    rows_ref[:, :width] = normed.astype(jnp.bfloat16)
    rows_ref[:, width:] = table_ref[...]


def expert_kernel(blocks, experts, *refs):
    row_refs = refs[:blocks]
    gate_ref, up_ref, down_ref, mine_ref, other_ref = refs[blocks:]
    local_experts, _, width = down_ref.shape
    rows = jnp.concatenate([ref[:, :width] for ref in row_refs], axis=0)
    table = jnp.concatenate([ref[:, width:] for ref in row_refs], axis=0).astype(jnp.float32)
    column = lax.broadcasted_iota(jnp.int32, table.shape, 1)
    total = None
    for local in range(local_experts):
        expert = lax.axis_index("expert") * local_experts + local
        chosen = (column == expert) | (column == expert + experts)
        weight = jnp.sum(jnp.where(chosen, table, 0.0), axis=1, keepdims=True)
        gate = lax.dot_general(
            gate_ref[local], rows, LAST_DIMS, preferred_element_type=jnp.float32
        )
        up = lax.dot_general(up_ref[local], rows, LAST_DIMS, preferred_element_type=jnp.float32)
        active = (gate * jax.nn.sigmoid(GLU_SLOPE * gate) * (up + 1.0)).astype(jnp.bfloat16)
        part = lax.dot_general(
            active, down_ref[local], FIRST_DIMS, preferred_element_type=jnp.float32
        )
        part = part * weight
        total = part if total is None else total + part
    half = mine_ref.shape[0]
    mine_ref[...] = total[:half]
    if other_ref.shape[0] == half:
        other_ref[...] = total[half:].astype(jnp.bfloat16)


def split_kernel(mine_ref, received_ref, kept_ref, *sent_refs):
    size = kept_ref.shape[0]
    kept_ref[...] = mine_ref[:size] + received_ref[:size].astype(jnp.float32)
    for number, sent_ref in enumerate(sent_refs, 1):
        block = pl.ds(number * size, size)
        total = mine_ref[block] + received_ref[block].astype(jnp.float32)
        sent_ref[...] = total.astype(jnp.bfloat16)


def gather_kernel(kept_ref, *refs):
    *received_refs, total_ref = refs
    total = kept_ref[...]
    for received_ref in received_refs:
        total = total + received_ref[...].astype(jnp.float32)
    total_ref[...] = total


def per_device(
    hidden_in,
    queries,
    new_keys,
    new_values,
    cache_keys,
    cache_values,
    cache_lengths,
    out_weight,
    norm_gain,
    expert_ids,
    route_probs,
    route_order,
    gate_weight,
    up_weight,
    down_weight,
):
    sequences, width = hidden_in.shape
    expert_ranks = lax.axis_size("expert")
    tensor_ranks = lax.axis_size("tensor")
    local_experts, hidden_units = down_weight.shape[:2]
    experts = local_experts * expert_ranks
    inner = 2
    outer = expert_ranks // inner
    slab_width = width // tensor_ranks
    offset = lax.axis_index("tensor") * slab_width
    row_width = -(-(width + 2 * experts) // 128) * 128

    def to_outer(values, step):
        pairs = [(rank, rank ^ (step * inner)) for rank in range(expert_ranks)]
        return lax.ppermute(values, "expert", pairs)

    def to_inner(values):
        return lax.ppermute(values, "expert", [(rank, rank ^ 1) for rank in range(expert_ranks)])

    operands = (queries, new_keys, new_values, cache_keys, cache_values, cache_lengths)
    if queries.shape[1] % 16 == 0:
        mine, sent = attend_and_project(*operands, out_weight)
    else:
        mine = jnp.dot(attend(*operands), out_weight, preferred_element_type=jnp.float32)
        sent = mine.astype(jnp.bfloat16)
    mine, received = exchange(mine, sent, "tensor", tensor_ranks)

    weights = route_weights(expert_ids, route_probs, route_order, experts)
    high = weights.astype(jnp.bfloat16)
    low = (weights - high.astype(jnp.float32)).astype(jnp.bfloat16)
    spare = jnp.zeros((sequences, row_width - width - 2 * experts), jnp.bfloat16)
    table = jnp.concatenate([high, low, spare], axis=1)

    block = (sequences, width)
    residual, rows = call(
        norm_kernel,
        [(block, jnp.float32), ((sequences, row_width), jnp.bfloat16)],
        (mine, received, hidden_in, norm_gain.reshape(1, width), table),
        flops=WINDOW_FLOPS,
        moved=sequences * width * 16,
        limit=2 * MIB,
    )

    near = [rows] + [to_outer(rows, step) for step in range(1, outer)]
    far = [to_inner(piece) for piece in near]
    half = (outer * sequences, width)
    mine, other = call(
        functools.partial(expert_kernel, 2 * outer, experts),
        [(half, jnp.float32), (half, jnp.bfloat16)],
        (*near, *far, gate_weight.swapaxes(1, 2), up_weight.swapaxes(1, 2), down_weight),
        flops=12 * half[0] * width * hidden_units * local_experts,
        moved=6 * width * hidden_units * local_experts,
        limit=16 * MIB,
    )
    received = to_inner(other)
    kept, *sent = call(
        split_kernel,
        [(block, jnp.float32)] + [(block, jnp.bfloat16)] * (outer - 1),
        (mine, received),
        flops=half[0] * width,
        moved=half[0] * width * 8,
        limit=4 * MIB,
    )
    returned = [to_outer(piece, step) for step, piece in enumerate(sent, 1)]
    (mixture,) = call(
        gather_kernel,
        [(block, jnp.float32)],
        (kept, *returned),
        flops=half[0] * width,
        moved=half[0] * width * 2,
        limit=2 * MIB,
    )
    mine, received = exchange(mixture, mixture.astype(jnp.bfloat16), "tensor", tensor_ranks)
    total = residual + mine + received.astype(jnp.float32)
    return lax.dynamic_slice_in_dim(total, offset, slab_width, 1).astype(jnp.bfloat16)


def solution(mesh):
    in_specs = (
        P(("groups", "expert"), None),
        P(("groups", "expert"), "tensor", None),
        P(("groups", "expert"), "tensor", None),
        P(("groups", "expert"), "tensor", None),
        P(("groups", "expert"), "tensor", None, None),
        P(("groups", "expert"), "tensor", None, None),
        P(("groups", "expert")),
        P("tensor", None),
        P(),
        P(("groups", "expert"), None),
        P(("groups", "expert"), None),
        P(("groups", "expert"), None),
        P("expert", None, "tensor"),
        P("expert", None, "tensor"),
        P("expert", "tensor", None),
    )
    out_specs = P(("groups", "expert"), "tensor")
    return jax.shard_map(
        per_device, mesh=mesh, in_specs=in_specs, out_specs=out_specs, check_vma=False
    )
```

```python
import functools

import jax
import jax.numpy as jnp
from jax import lax
from jax.experimental import pallas as pl
from jax.experimental.pallas import tpu as pltpu
from jax.sharding import PartitionSpec as P

EPSILON = 1e-05
GLU_SLOPE = 1.702
WINDOW_FLOPS = 200_000_000_000


def attend(queries, new_keys, new_values, cache_keys, cache_values, cache_lengths):
    sequence_count, head_count, head_dim = queries.shape
    kv_heads = new_keys.shape[1]
    group_size = head_count // kv_heads
    scaling = 1.0 / head_dim**0.5
    query_rows = queries.reshape(sequence_count, kv_heads, group_size, head_dim)
    scores = (
        jnp.einsum("sgqd,sgdc->sgqc", query_rows, cache_keys, preferred_element_type=jnp.float32)
        * scaling
    )
    own_score = (
        jnp.einsum("sgqd,sgd->sgq", query_rows, new_keys, preferred_element_type=jnp.float32)
        * scaling
    )
    positions = jnp.arange(cache_keys.shape[3], dtype=jnp.int32)
    visible = positions[None, :] < cache_lengths[:, None]
    scores = jnp.where(visible[:, None, None, :], scores, -1e30)
    highest = jnp.maximum(jnp.max(scores, axis=3), own_score)
    cache_exp = jnp.exp(scores - highest[..., None])
    own_exp = jnp.exp(own_score - highest)
    totals = jnp.sum(cache_exp, axis=3) + own_exp
    cache_prob = (cache_exp / totals[..., None]).astype(jnp.bfloat16)
    own_prob = (own_exp / totals).astype(jnp.bfloat16)
    attended = jnp.einsum(
        "sgqc,sgdc->sgqd", cache_prob, cache_values, preferred_element_type=jnp.float32
    )
    attended = (
        attended
        + own_prob.astype(jnp.float32)[..., None] * new_values.astype(jnp.float32)[:, :, None, :]
    )
    return attended.astype(jnp.bfloat16).reshape(sequence_count, head_count * head_dim)


VMEM = pl.BlockSpec(memory_space=pltpu.VMEM)
LAST_DIMS = (((1,), (1,)), ((), ()))
FIRST_DIMS = (((0,), (0,)), ((), ()))
MIB = 1 << 20


def call(kernel, outs, args, flops, moved, limit):
    return pl.pallas_call(
        kernel,
        out_shape=[jax.ShapeDtypeStruct(shape, dtype) for shape, dtype in outs],
        in_specs=[VMEM] * len(args),
        out_specs=[VMEM] * len(outs),
        compiler_params=pltpu.CompilerParams(vmem_limit_bytes=limit),
        cost_estimate=pl.CostEstimate(flops=flops, bytes_accessed=moved, transcendentals=0),
    )(*args)


def mm(left, right, dims=(((1,), (0,)), ((), ()))):
    return lax.dot_general(left, right, dims, preferred_element_type=jnp.float32)


def iota(shape, dim):
    return lax.broadcasted_iota(jnp.int32, shape, dim)


def attend_kernel(
    lengths_hbm,
    queries_hbm,
    new_keys_hbm,
    new_values_hbm,
    keys_hbm,
    values_hbm,
    weight_hbm,
    mine_ref,
    sent_ref,
    lengths_ref,
    queries_ref,
    new_keys_ref,
    new_values_ref,
    keys_ref,
    values_ref,
    weight_ref,
    own_keys_ref,
    own_values_ref,
    attended_ref,
    arrived,
):
    sequences, heads, head_dim = queries_ref.shape
    kv_heads = new_keys_ref.shape[1]
    group = heads // kv_heads
    span = kv_heads * head_dim
    lanes = group * head_dim
    moves = (
        (lengths_hbm, lengths_ref),
        (queries_hbm, queries_ref),
        (new_keys_hbm, new_keys_ref),
        (new_values_hbm, new_values_ref),
        (keys_hbm, keys_ref),
        (values_hbm, values_ref),
        (weight_hbm, weight_ref),
    )
    copies = [
        pltpu.make_async_copy(source, target, arrived.at[number])
        for number, (source, target) in enumerate(moves)
    ]
    for copy in copies:
        copy.start()

    rows = sequences * heads
    scaling = 1.0 / head_dim**0.5
    for copy in copies[:4]:
        copy.wait()
    queries = queries_ref[...].reshape(rows, head_dim)
    for sequence in range(sequences):
        block = pl.ds(sequence * kv_heads, kv_heads)
        own_keys_ref[block] = new_keys_ref[sequence].astype(jnp.float32)
        own_values_ref[block] = new_values_ref[sequence].astype(jnp.float32)
    own_keys = own_keys_ref[...].astype(jnp.bfloat16)
    own_values = own_values_ref[...].astype(jnp.bfloat16)

    spread = (iota((head_dim, span), 0) == iota((head_dim, span), 1) % head_dim).astype(
        jnp.bfloat16
    )
    same_head = iota((rows, span), 1) // head_dim == iota((rows, span), 0) % heads // group
    wide = jnp.where(same_head, mm(queries, spread), 0.0).astype(jnp.bfloat16)
    pairs = (rows, sequences * kv_heads)
    own_pair = iota(pairs, 1) == iota(pairs, 0) // group
    own_score = (
        jnp.sum(jnp.where(own_pair, mm(queries, own_keys, LAST_DIMS), 0.0), axis=1, keepdims=True)
        * scaling
    )

    copies[4].wait()
    slots = keys_ref.shape[2]
    scores = []
    for sequence in range(sequences):
        block = slice(sequence * heads, (sequence + 1) * heads)
        score = mm(wide[block], keys_ref[sequence]) * scaling
        visible = iota((heads, slots), 1) < lengths_ref[sequence]
        scores.append(jnp.where(visible, score, -1e30))
    scores = jnp.concatenate(scores, axis=0)
    highest = jnp.maximum(jnp.max(scores, axis=1, keepdims=True), own_score)
    cache_exp = jnp.exp(scores - highest)
    own_exp = jnp.exp(own_score - highest)
    totals = jnp.sum(cache_exp, axis=1, keepdims=True) + own_exp
    cache_prob = (cache_exp / totals).astype(jnp.bfloat16)
    own_prob = own_exp / totals
    own_prob = jnp.where(own_pair, own_prob, 0.0).astype(jnp.bfloat16)
    own_part = mm(own_prob, mm(own_values, spread).astype(jnp.bfloat16))

    copies[5].wait()
    attended = [
        mm(
            cache_prob[sequence * heads : (sequence + 1) * heads],
            values_ref[sequence],
            LAST_DIMS,
        )
        for sequence in range(sequences)
    ]
    attended = jnp.concatenate(attended, axis=0) + own_part
    attended = jnp.where(same_head, attended, 0.0).astype(jnp.bfloat16)
    repeat = (iota((span, lanes), 0) % head_dim == iota((span, lanes), 1) % head_dim).astype(
        jnp.bfloat16
    )
    own_lanes = iota((rows, lanes), 1) // head_dim == iota((rows, lanes), 0) % group
    placed = jnp.where(own_lanes, mm(attended, repeat), 0.0).astype(jnp.bfloat16)
    sums = (kv_heads * sequences, rows)
    chosen = (iota(sums, 0) % sequences == iota(sums, 1) // heads) & (
        iota(sums, 0) // sequences == iota(sums, 1) % heads // group
    )
    by_head = mm(chosen.astype(jnp.bfloat16), placed)
    for head in range(kv_heads):
        attended_ref[:, head * lanes : (head + 1) * lanes] = by_head[
            head * sequences : (head + 1) * sequences
        ].astype(jnp.bfloat16)
    attended = attended_ref[...]

    copies[6].wait()
    part = mm(weight_ref[...], attended, LAST_DIMS).T
    mine_ref[...] = part
    sent_ref[...] = part.astype(jnp.bfloat16)


def attend_and_project(
    queries, new_keys, new_values, cache_keys, cache_values, cache_lengths, out_weight
):
    sequences, heads, head_dim = queries.shape
    kv_heads, slots = cache_keys.shape[1], cache_keys.shape[3]
    depth, width = out_weight.shape
    span = kv_heads * head_dim
    caches = (sequences, span, slots)
    hbm = pl.BlockSpec(memory_space=pltpu.HBM)
    arrays = (
        cache_lengths,
        queries,
        new_keys,
        new_values,
        cache_keys.reshape(caches),
        cache_values.reshape(caches),
        out_weight.T,
    )
    return pl.pallas_call(
        attend_kernel,
        out_shape=[
            jax.ShapeDtypeStruct((sequences, width), jnp.float32),
            jax.ShapeDtypeStruct((sequences, width), jnp.bfloat16),
        ],
        in_specs=[hbm] * len(arrays),
        out_specs=[VMEM] * 2,
        scratch_shapes=[pltpu.SMEM(cache_lengths.shape, cache_lengths.dtype)]
        + [pltpu.VMEM(array.shape, array.dtype) for array in arrays[1:]]
        + [
            pltpu.VMEM((sequences * kv_heads, head_dim), jnp.float32),
            pltpu.VMEM((sequences * kv_heads, head_dim), jnp.float32),
            pltpu.VMEM((sequences, depth), jnp.bfloat16),
            pltpu.SemaphoreType.DMA((len(arrays),)),
        ],
        compiler_params=pltpu.CompilerParams(vmem_limit_bytes=53 * MIB),
        cost_estimate=pl.CostEstimate(
            flops=2 * sequences * width * depth,
            bytes_accessed=2 * (width * depth + 2 * sequences * span * slots),
            transcendentals=sequences * heads * slots,
        ),
    )(*[pltpu.with_memory_space_constraint(array, pltpu.HBM) for array in arrays])


def route_weights(expert_ids, route_probs, route_order, experts):
    picked = jnp.zeros(expert_ids.shape, jnp.float32)
    for column in range(expert_ids.shape[1]):
        picked = picked + jnp.where(route_order == column, route_probs[:, column : column + 1], 0.0)
    weights = picked / jnp.sum(route_probs, axis=1, keepdims=True)
    named = expert_ids[:, :, None] == jnp.arange(experts, dtype=jnp.int32)[None, None, :]
    return jnp.sum(jnp.where(named, weights[:, :, None], 0.0), axis=1)


def exchange(values, sent, axis, ranks):
    step = 1
    while True:
        pairs = [(rank, rank ^ step) for rank in range(ranks)]
        received = lax.ppermute(sent, axis, pairs)
        step *= 2
        if step >= ranks:
            return values, received
        values = values + received.astype(jnp.float32)
        sent = values.astype(jnp.bfloat16)


def norm_kernel(mine_ref, received_ref, hidden_ref, gain_ref, table_ref, residual_ref, rows_ref):
    width = hidden_ref.shape[1]
    residual = (
        hidden_ref[...].astype(jnp.float32) + mine_ref[...] + received_ref[...].astype(jnp.float32)
    )
    residual_ref[...] = residual
    mean_square = jnp.mean(residual * residual, axis=1, keepdims=True)
    normed = residual * lax.rsqrt(mean_square + EPSILON) * gain_ref[...]
    rows_ref[:, :width] = normed.astype(jnp.bfloat16)
    rows_ref[:, width:] = table_ref[...]


def expert_kernel(blocks, experts, *refs):
    row_refs = refs[:blocks]
    gate_ref, up_ref, down_ref, mine_ref, other_ref = refs[blocks:]
    local_experts, _, width = down_ref.shape
    rows = jnp.concatenate([ref[:, :width] for ref in row_refs], axis=0)
    table = jnp.concatenate([ref[:, width:] for ref in row_refs], axis=0).astype(jnp.float32)
    column = lax.broadcasted_iota(jnp.int32, table.shape, 1)
    total = None
    for local in range(local_experts):
        expert = lax.axis_index("expert") * local_experts + local
        chosen = (column == expert) | (column == expert + experts)
        weight = jnp.sum(jnp.where(chosen, table, 0.0), axis=1, keepdims=True)
        gate = lax.dot_general(
            gate_ref[local], rows, LAST_DIMS, preferred_element_type=jnp.float32
        )
        up = lax.dot_general(up_ref[local], rows, LAST_DIMS, preferred_element_type=jnp.float32)
        active = (gate * jax.nn.sigmoid(GLU_SLOPE * gate) * (up + 1.0)).astype(jnp.bfloat16)
        part = lax.dot_general(
            active, down_ref[local], FIRST_DIMS, preferred_element_type=jnp.float32
        )
        part = part * weight
        total = part if total is None else total + part
    half = mine_ref.shape[0]
    mine_ref[...] = total[:half]
    if other_ref.shape[0] == half:
        other_ref[...] = total[half:].astype(jnp.bfloat16)


def split_kernel(mine_ref, received_ref, kept_ref, *sent_refs):
    size = kept_ref.shape[0]
    kept_ref[...] = mine_ref[:size] + received_ref[:size].astype(jnp.float32)
    for number, sent_ref in enumerate(sent_refs, 1):
        block = pl.ds(number * size, size)
        total = mine_ref[block] + received_ref[block].astype(jnp.float32)
        sent_ref[...] = total.astype(jnp.bfloat16)


def gather_kernel(kept_ref, *refs):
    *received_refs, total_ref = refs
    total = kept_ref[...]
    for received_ref in received_refs:
        total = total + received_ref[...].astype(jnp.float32)
    total_ref[...] = total


def per_device(
    hidden_in,
    queries,
    new_keys,
    new_values,
    cache_keys,
    cache_values,
    cache_lengths,
    out_weight,
    norm_gain,
    expert_ids,
    route_probs,
    route_order,
    gate_weight,
    up_weight,
    down_weight,
):
    sequences, width = hidden_in.shape
    expert_ranks = lax.axis_size("expert")
    tensor_ranks = lax.axis_size("tensor")
    local_experts, hidden_units = down_weight.shape[:2]
    experts = local_experts * expert_ranks
    inner = 2
    outer = expert_ranks // inner
    slab_width = width // tensor_ranks
    offset = lax.axis_index("tensor") * slab_width
    row_width = -(-(width + 2 * experts) // 128) * 128

    def to_outer(values, step):
        pairs = [(rank, rank ^ (step * inner)) for rank in range(expert_ranks)]
        return lax.ppermute(values, "expert", pairs)

    def to_inner(values):
        return lax.ppermute(values, "expert", [(rank, rank ^ 1) for rank in range(expert_ranks)])

    operands = (queries, new_keys, new_values, cache_keys, cache_values, cache_lengths)
    if queries.shape[1] % 16 == 0:
        mine, sent = attend_and_project(*operands, out_weight)
    else:
        mine = jnp.dot(attend(*operands), out_weight, preferred_element_type=jnp.float32)
        sent = mine.astype(jnp.bfloat16)
    mine, received = exchange(mine, sent, "tensor", tensor_ranks)

    weights = route_weights(expert_ids, route_probs, route_order, experts)
    high = weights.astype(jnp.bfloat16)
    low = (weights - high.astype(jnp.float32)).astype(jnp.bfloat16)
    spare = jnp.zeros((sequences, row_width - width - 2 * experts), jnp.bfloat16)
    table = jnp.concatenate([high, low, spare], axis=1)

    block = (sequences, width)
    residual, rows = call(
        norm_kernel,
        [(block, jnp.float32), ((sequences, row_width), jnp.bfloat16)],
        (mine, received, hidden_in, norm_gain.reshape(1, width), table),
        flops=WINDOW_FLOPS,
        moved=sequences * width * 16,
        limit=2 * MIB,
    )

    near = [rows] + [to_outer(rows, step) for step in range(1, outer)]
    far = [to_inner(piece) for piece in near]
    half = (outer * sequences, width)
    mine, other = call(
        functools.partial(expert_kernel, 2 * outer, experts),
        [(half, jnp.float32), (half, jnp.bfloat16)],
        (*near, *far, gate_weight.swapaxes(1, 2), up_weight.swapaxes(1, 2), down_weight),
        flops=12 * half[0] * width * hidden_units * local_experts,
        moved=6 * width * hidden_units * local_experts,
        limit=16 * MIB,
    )
    received = to_inner(other)
    kept, *sent = call(
        split_kernel,
        [(block, jnp.float32)] + [(block, jnp.bfloat16)] * (outer - 1),
        (mine, received),
        flops=half[0] * width,
        moved=half[0] * width * 8,
        limit=4 * MIB,
    )
    returned = [to_outer(piece, step) for step, piece in enumerate(sent, 1)]
    (mixture,) = call(
        gather_kernel,
        [(block, jnp.float32)],
        (kept, *returned),
        flops=half[0] * width,
        moved=half[0] * width * 2,
        limit=2 * MIB,
    )
    mine, received = exchange(mixture, mixture.astype(jnp.bfloat16), "tensor", tensor_ranks)
    total = residual + mine + received.astype(jnp.float32)
    return lax.dynamic_slice_in_dim(total, offset, slab_width, 1).astype(jnp.bfloat16)


def solution(mesh):
    in_specs = (
        P(("groups", "expert"), None),
        P(("groups", "expert"), "tensor", None),
        P(("groups", "expert"), "tensor", None),
        P(("groups", "expert"), "tensor", None),
        P(("groups", "expert"), "tensor", None, None),
        P(("groups", "expert"), "tensor", None, None),
        P(("groups", "expert")),
        P("tensor", None),
        P(),
        P(("groups", "expert"), None),
        P(("groups", "expert"), None),
        P(("groups", "expert"), None),
        P("expert", None, "tensor"),
        P("expert", None, "tensor"),
        P("expert", "tensor", None),
    )
    out_specs = P(("groups", "expert"), "tensor")
    return jax.shard_map(
        per_device, mesh=mesh, in_specs=in_specs, out_specs=out_specs, check_vma=False
    )
```

```python
import functools

import jax
import jax.numpy as jnp
from jax import lax
from jax.experimental import pallas as pl
from jax.experimental.pallas import tpu as pltpu
from jax.sharding import PartitionSpec as P

EPSILON = 1e-05
GLU_SLOPE = 1.702
WINDOW_FLOPS = 200_000_000_000


def attend(queries, new_keys, new_values, cache_keys, cache_values, cache_lengths):
    sequence_count, head_count, head_dim = queries.shape
    kv_heads = new_keys.shape[1]
    group_size = head_count // kv_heads
    scaling = 1.0 / head_dim**0.5
    query_rows = queries.reshape(sequence_count, kv_heads, group_size, head_dim)
    scores = (
        jnp.einsum("sgqd,sgdc->sgqc", query_rows, cache_keys, preferred_element_type=jnp.float32)
        * scaling
    )
    own_score = (
        jnp.einsum("sgqd,sgd->sgq", query_rows, new_keys, preferred_element_type=jnp.float32)
        * scaling
    )
    positions = jnp.arange(cache_keys.shape[3], dtype=jnp.int32)
    visible = positions[None, :] < cache_lengths[:, None]
    scores = jnp.where(visible[:, None, None, :], scores, -1e30)
    highest = jnp.maximum(jnp.max(scores, axis=3), own_score)
    cache_exp = jnp.exp(scores - highest[..., None])
    own_exp = jnp.exp(own_score - highest)
    totals = jnp.sum(cache_exp, axis=3) + own_exp
    cache_prob = (cache_exp / totals[..., None]).astype(jnp.bfloat16)
    own_prob = (own_exp / totals).astype(jnp.bfloat16)
    attended = jnp.einsum(
        "sgqc,sgdc->sgqd", cache_prob, cache_values, preferred_element_type=jnp.float32
    )
    attended = (
        attended
        + own_prob.astype(jnp.float32)[..., None] * new_values.astype(jnp.float32)[:, :, None, :]
    )
    return attended.astype(jnp.bfloat16).reshape(sequence_count, head_count * head_dim)


VMEM = pl.BlockSpec(memory_space=pltpu.VMEM)
LAST_DIMS = (((1,), (1,)), ((), ()))
FIRST_DIMS = (((0,), (0,)), ((), ()))
MIB = 1 << 20


def call(kernel, outs, args, flops, moved, limit):
    return pl.pallas_call(
        kernel,
        out_shape=[jax.ShapeDtypeStruct(shape, dtype) for shape, dtype in outs],
        in_specs=[VMEM] * len(args),
        out_specs=[VMEM] * len(outs),
        compiler_params=pltpu.CompilerParams(vmem_limit_bytes=limit),
        cost_estimate=pl.CostEstimate(flops=flops, bytes_accessed=moved, transcendentals=0),
    )(*args)


def mm(left, right, dims=(((1,), (0,)), ((), ()))):
    return lax.dot_general(left, right, dims, preferred_element_type=jnp.float32)


def iota(shape, dim):
    return lax.broadcasted_iota(jnp.int32, shape, dim)


def attend_kernel(
    lengths_hbm,
    queries_hbm,
    new_keys_hbm,
    new_values_hbm,
    keys_hbm,
    values_hbm,
    weight_hbm,
    mine_ref,
    sent_ref,
    lengths_ref,
    queries_ref,
    new_keys_ref,
    new_values_ref,
    keys_ref,
    values_ref,
    weight_ref,
    own_keys_ref,
    own_values_ref,
    attended_ref,
    arrived,
):
    sequences, heads, head_dim = queries_ref.shape
    kv_heads = new_keys_ref.shape[1]
    group = heads // kv_heads
    span = kv_heads * head_dim
    lanes = group * head_dim
    moves = (
        (lengths_hbm, lengths_ref),
        (queries_hbm, queries_ref),
        (new_keys_hbm, new_keys_ref),
        (new_values_hbm, new_values_ref),
        (keys_hbm, keys_ref),
        (values_hbm, values_ref),
        (weight_hbm, weight_ref),
    )
    copies = [
        pltpu.make_async_copy(source, target, arrived.at[number])
        for number, (source, target) in enumerate(moves)
    ]
    for copy in copies:
        copy.start()

    rows = sequences * heads
    scaling = 1.0 / head_dim**0.5
    for copy in copies[:4]:
        copy.wait()
    queries = queries_ref[...].reshape(rows, head_dim)
    for sequence in range(sequences):
        block = pl.ds(sequence * kv_heads, kv_heads)
        own_keys_ref[block] = new_keys_ref[sequence].astype(jnp.float32)
        own_values_ref[block] = new_values_ref[sequence].astype(jnp.float32)
    own_keys = own_keys_ref[...].astype(jnp.bfloat16)
    own_values = own_values_ref[...].astype(jnp.bfloat16)

    spread = (iota((head_dim, span), 0) == iota((head_dim, span), 1) % head_dim).astype(
        jnp.bfloat16
    )
    same_head = iota((rows, span), 1) // head_dim == iota((rows, span), 0) % heads // group
    wide = jnp.where(same_head, mm(queries, spread), 0.0).astype(jnp.bfloat16)
    pairs = (rows, sequences * kv_heads)
    own_pair = iota(pairs, 1) == iota(pairs, 0) // group
    own_score = (
        jnp.sum(jnp.where(own_pair, mm(queries, own_keys, LAST_DIMS), 0.0), axis=1, keepdims=True)
        * scaling
    )

    copies[4].wait()
    slots = keys_ref.shape[2]
    scores = []
    for sequence in range(sequences):
        block = slice(sequence * heads, (sequence + 1) * heads)
        score = mm(wide[block], keys_ref[sequence]) * scaling
        visible = iota((heads, slots), 1) < lengths_ref[sequence]
        scores.append(jnp.where(visible, score, -1e30))
    scores = jnp.concatenate(scores, axis=0)
    highest = jnp.maximum(jnp.max(scores, axis=1, keepdims=True), own_score)
    cache_exp = jnp.exp(scores - highest)
    own_exp = jnp.exp(own_score - highest)
    totals = jnp.sum(cache_exp, axis=1, keepdims=True) + own_exp
    cache_prob = (cache_exp / totals).astype(jnp.bfloat16)
    own_prob = own_exp / totals
    own_prob = jnp.where(own_pair, own_prob, 0.0).astype(jnp.bfloat16)
    own_part = mm(own_prob, mm(own_values, spread).astype(jnp.bfloat16))

    copies[5].wait()
    attended = [
        mm(
            cache_prob[sequence * heads : (sequence + 1) * heads],
            values_ref[sequence],
            LAST_DIMS,
        )
        for sequence in range(sequences)
    ]
    attended = jnp.concatenate(attended, axis=0) + own_part
    attended = jnp.where(same_head, attended, 0.0).astype(jnp.bfloat16)
    repeat = (iota((span, lanes), 0) % head_dim == iota((span, lanes), 1) % head_dim).astype(
        jnp.bfloat16
    )
    own_lanes = iota((rows, lanes), 1) // head_dim == iota((rows, lanes), 0) % group
    placed = jnp.where(own_lanes, mm(attended, repeat), 0.0).astype(jnp.bfloat16)
    sums = (kv_heads * sequences, rows)
    chosen = (iota(sums, 0) % sequences == iota(sums, 1) // heads) & (
        iota(sums, 0) // sequences == iota(sums, 1) % heads // group
    )
    by_head = mm(chosen.astype(jnp.bfloat16), placed)
    for head in range(kv_heads):
        attended_ref[:, head * lanes : (head + 1) * lanes] = by_head[
            head * sequences : (head + 1) * sequences
        ].astype(jnp.bfloat16)
    attended = attended_ref[...]

    copies[6].wait()
    part = mm(weight_ref[...], attended, LAST_DIMS).T
    mine_ref[...] = part
    sent_ref[...] = part.astype(jnp.bfloat16)


def attend_and_project(
    queries, new_keys, new_values, cache_keys, cache_values, cache_lengths, out_weight
):
    sequences, heads, head_dim = queries.shape
    kv_heads, slots = cache_keys.shape[1], cache_keys.shape[3]
    depth, width = out_weight.shape
    span = kv_heads * head_dim
    caches = (sequences, span, slots)
    hbm = pl.BlockSpec(memory_space=pltpu.HBM)
    arrays = (
        cache_lengths,
        queries,
        new_keys,
        new_values,
        cache_keys.reshape(caches),
        cache_values.reshape(caches),
        out_weight.T,
    )
    return pl.pallas_call(
        attend_kernel,
        out_shape=[
            jax.ShapeDtypeStruct((sequences, width), jnp.float32),
            jax.ShapeDtypeStruct((sequences, width), jnp.bfloat16),
        ],
        in_specs=[hbm] * len(arrays),
        out_specs=[VMEM] * 2,
        scratch_shapes=[pltpu.SMEM(cache_lengths.shape, cache_lengths.dtype)]
        + [pltpu.VMEM(array.shape, array.dtype) for array in arrays[1:]]
        + [
            pltpu.VMEM((sequences * kv_heads, head_dim), jnp.float32),
            pltpu.VMEM((sequences * kv_heads, head_dim), jnp.float32),
            pltpu.VMEM((sequences, depth), jnp.bfloat16),
            pltpu.SemaphoreType.DMA((len(arrays),)),
        ],
        compiler_params=pltpu.CompilerParams(vmem_limit_bytes=53 * MIB),
        cost_estimate=pl.CostEstimate(
            flops=2 * sequences * width * depth,
            bytes_accessed=2 * (width * depth + 2 * sequences * span * slots),
            transcendentals=sequences * heads * slots,
        ),
    )(*[pltpu.with_memory_space_constraint(array, pltpu.HBM) for array in arrays])


def route_weights(expert_ids, route_probs, route_order, experts):
    picked = jnp.zeros(expert_ids.shape, jnp.float32)
    for column in range(expert_ids.shape[1]):
        picked = picked + jnp.where(route_order == column, route_probs[:, column : column + 1], 0.0)
    weights = picked / jnp.sum(route_probs, axis=1, keepdims=True)
    named = expert_ids[:, :, None] == jnp.arange(experts, dtype=jnp.int32)[None, None, :]
    return jnp.sum(jnp.where(named, weights[:, :, None], 0.0), axis=1)


def exchange(values, sent, axis, ranks):
    step = 1
    while True:
        pairs = [(rank, rank ^ step) for rank in range(ranks)]
        received = lax.ppermute(sent, axis, pairs)
        step *= 2
        if step >= ranks:
            return values, received
        values = values + received.astype(jnp.float32)
        sent = values.astype(jnp.bfloat16)


def norm_kernel(mine_ref, received_ref, hidden_ref, gain_ref, table_ref, residual_ref, rows_ref):
    width = hidden_ref.shape[1]
    residual = (
        hidden_ref[...].astype(jnp.float32) + mine_ref[...] + received_ref[...].astype(jnp.float32)
    )
    residual_ref[...] = residual
    mean_square = jnp.mean(residual * residual, axis=1, keepdims=True)
    normed = residual * lax.rsqrt(mean_square + EPSILON) * gain_ref[...]
    rows_ref[:, :width] = normed.astype(jnp.bfloat16)
    rows_ref[:, width:] = table_ref[...]


def pack_kernel(*refs):
    *piece_refs, packed_ref = refs
    size = piece_refs[0].shape[0]
    for number, piece_ref in enumerate(piece_refs):
        packed_ref[pl.ds(number * size, size)] = piece_ref[...]


def expert_kernel(experts, *refs):
    *row_refs, gate_ref, up_ref, down_ref, mine_ref, other_ref = refs
    local_experts, _, width = down_ref.shape
    rows = jnp.concatenate([ref[:, :width] for ref in row_refs], axis=0)
    table = jnp.concatenate([ref[:, width:] for ref in row_refs], axis=0).astype(jnp.float32)
    column = lax.broadcasted_iota(jnp.int32, table.shape, 1)
    total = None
    for local in range(local_experts):
        expert = lax.axis_index("expert") * local_experts + local
        chosen = (column == expert) | (column == expert + experts)
        weight = jnp.sum(jnp.where(chosen, table, 0.0), axis=1, keepdims=True)
        gate = lax.dot_general(
            gate_ref[local], rows, LAST_DIMS, preferred_element_type=jnp.float32
        )
        up = lax.dot_general(up_ref[local], rows, LAST_DIMS, preferred_element_type=jnp.float32)
        active = (gate * jax.nn.sigmoid(GLU_SLOPE * gate) * (up + 1.0)).astype(jnp.bfloat16)
        part = lax.dot_general(
            active, down_ref[local], FIRST_DIMS, preferred_element_type=jnp.float32
        )
        part = part * weight
        total = part if total is None else total + part
    half = mine_ref.shape[0]
    mine_ref[...] = total[:half]
    other_ref[...] = total[half:].astype(jnp.bfloat16)


def split_kernel(mine_ref, received_ref, kept_ref, *sent_refs):
    size = kept_ref.shape[0]
    kept_ref[...] = mine_ref[:size] + received_ref[:size].astype(jnp.float32)
    for number, sent_ref in enumerate(sent_refs, 1):
        block = pl.ds(number * size, size)
        total = mine_ref[block] + received_ref[block].astype(jnp.float32)
        sent_ref[...] = total.astype(jnp.bfloat16)


def gather_kernel(kept_ref, *refs):
    *received_refs, total_ref = refs
    total = kept_ref[...]
    for received_ref in received_refs:
        total = total + received_ref[...].astype(jnp.float32)
    total_ref[...] = total


def per_device(
    hidden_in,
    queries,
    new_keys,
    new_values,
    cache_keys,
    cache_values,
    cache_lengths,
    out_weight,
    norm_gain,
    expert_ids,
    route_probs,
    route_order,
    gate_weight,
    up_weight,
    down_weight,
):
    sequences, width = hidden_in.shape
    expert_ranks = lax.axis_size("expert")
    tensor_ranks = lax.axis_size("tensor")
    local_experts, hidden_units = down_weight.shape[:2]
    experts = local_experts * expert_ranks
    inner = 2
    outer = expert_ranks // inner
    slab_width = width // tensor_ranks
    offset = lax.axis_index("tensor") * slab_width
    row_width = -(-(width + 2 * experts) // 128) * 128

    def to_outer(values, step):
        pairs = [(rank, rank ^ (step * inner)) for rank in range(expert_ranks)]
        return lax.ppermute(values, "expert", pairs)

    def to_inner(values):
        return lax.ppermute(values, "expert", [(rank, rank ^ 1) for rank in range(expert_ranks)])

    operands = (queries, new_keys, new_values, cache_keys, cache_values, cache_lengths)
    if queries.shape[1] % 16 == 0:
        mine, sent = attend_and_project(*operands, out_weight)
    else:
        mine = jnp.dot(attend(*operands), out_weight, preferred_element_type=jnp.float32)
        sent = mine.astype(jnp.bfloat16)
    mine, received = exchange(mine, sent, "tensor", tensor_ranks)

    weights = route_weights(expert_ids, route_probs, route_order, experts)
    high = weights.astype(jnp.bfloat16)
    low = (weights - high.astype(jnp.float32)).astype(jnp.bfloat16)
    spare = jnp.zeros((sequences, row_width - width - 2 * experts), jnp.bfloat16)
    table = jnp.concatenate([high, low, spare], axis=1)

    block = (sequences, width)
    residual, rows = call(
        norm_kernel,
        [(block, jnp.float32), ((sequences, row_width), jnp.bfloat16)],
        (mine, received, hidden_in, norm_gain.reshape(1, width), table),
        flops=WINDOW_FLOPS,
        moved=sequences * width * 16,
        limit=2 * MIB,
    )

    near = [rows]
    for step in range(1, outer):
        near.append(to_outer(rows, step))
    (near,) = call(
        pack_kernel,
        [((outer * sequences, row_width), jnp.bfloat16)],
        near,
        flops=sequences,
        moved=4 * outer * sequences * row_width,
        limit=2 * MIB,
    )
    far = to_inner(near)
    half = (outer * sequences, width)
    mine, other = call(
        functools.partial(expert_kernel, experts),
        [(half, jnp.float32), (half, jnp.bfloat16)],
        (near, far, gate_weight.swapaxes(1, 2), up_weight.swapaxes(1, 2), down_weight),
        flops=12 * half[0] * width * hidden_units * local_experts,
        moved=6 * width * hidden_units * local_experts,
        limit=16 * MIB,
    )
    received = to_inner(other)
    kept, *sent = call(
        split_kernel,
        [(block, jnp.float32)] + [(block, jnp.bfloat16)] * (outer - 1),
        (mine, received),
        flops=half[0] * width,
        moved=half[0] * width * 8,
        limit=4 * MIB,
    )
    returned = []
    for step, piece in enumerate(sent, 1):
        returned.append(to_outer(piece, step))
    (mixture,) = call(
        gather_kernel,
        [(block, jnp.float32)],
        (kept, *returned),
        flops=half[0] * width,
        moved=half[0] * width * 2,
        limit=2 * MIB,
    )
    mine, received = exchange(mixture, mixture.astype(jnp.bfloat16), "tensor", tensor_ranks)
    total = residual + mine + received.astype(jnp.float32)
    return lax.dynamic_slice_in_dim(total, offset, slab_width, 1).astype(jnp.bfloat16)


def solution(mesh):
    in_specs = (
        P(("groups", "expert"), None),
        P(("groups", "expert"), "tensor", None),
        P(("groups", "expert"), "tensor", None),
        P(("groups", "expert"), "tensor", None),
        P(("groups", "expert"), "tensor", None, None),
        P(("groups", "expert"), "tensor", None, None),
        P(("groups", "expert")),
        P("tensor", None),
        P(),
        P(("groups", "expert"), None),
        P(("groups", "expert"), None),
        P(("groups", "expert"), None),
        P("expert", None, "tensor"),
        P("expert", None, "tensor"),
        P("expert", "tensor", None),
    )
    out_specs = P(("groups", "expert"), "tensor")

    return jax.shard_map(
        per_device, mesh=mesh, in_specs=in_specs, out_specs=out_specs, check_vma=False
    )
```

```python
import functools

import jax
import jax.numpy as jnp
from jax import lax
from jax.experimental import pallas as pl
from jax.experimental.pallas import tpu as pltpu
from jax.sharding import PartitionSpec as P

EPSILON = 1e-05
GLU_SLOPE = 1.702
WINDOW_FLOPS = 200_000_000_000


def attend(queries, new_keys, new_values, cache_keys, cache_values, cache_lengths):
    sequence_count, head_count, head_dim = queries.shape
    kv_heads = new_keys.shape[1]
    group_size = head_count // kv_heads
    scaling = 1.0 / head_dim**0.5
    query_rows = queries.reshape(sequence_count, kv_heads, group_size, head_dim)
    scores = (
        jnp.einsum("sgqd,sgdc->sgqc", query_rows, cache_keys, preferred_element_type=jnp.float32)
        * scaling
    )
    own_score = (
        jnp.einsum("sgqd,sgd->sgq", query_rows, new_keys, preferred_element_type=jnp.float32)
        * scaling
    )
    positions = jnp.arange(cache_keys.shape[3], dtype=jnp.int32)
    visible = positions[None, :] < cache_lengths[:, None]
    scores = jnp.where(visible[:, None, None, :], scores, -1e30)
    highest = jnp.maximum(jnp.max(scores, axis=3), own_score)
    cache_exp = jnp.exp(scores - highest[..., None])
    own_exp = jnp.exp(own_score - highest)
    totals = jnp.sum(cache_exp, axis=3) + own_exp
    cache_prob = (cache_exp / totals[..., None]).astype(jnp.bfloat16)
    own_prob = (own_exp / totals).astype(jnp.bfloat16)
    attended = jnp.einsum(
        "sgqc,sgdc->sgqd", cache_prob, cache_values, preferred_element_type=jnp.float32
    )
    attended = (
        attended
        + own_prob.astype(jnp.float32)[..., None] * new_values.astype(jnp.float32)[:, :, None, :]
    )
    return attended.astype(jnp.bfloat16).reshape(sequence_count, head_count * head_dim)


VMEM = pl.BlockSpec(memory_space=pltpu.VMEM)
LAST_DIMS = (((1,), (1,)), ((), ()))
FIRST_DIMS = (((0,), (0,)), ((), ()))
MIB = 1 << 20


def call(kernel, outs, args, flops, moved, limit):
    return pl.pallas_call(
        kernel,
        out_shape=[jax.ShapeDtypeStruct(shape, dtype) for shape, dtype in outs],
        in_specs=[VMEM] * len(args),
        out_specs=[VMEM] * len(outs),
        compiler_params=pltpu.CompilerParams(vmem_limit_bytes=limit),
        cost_estimate=pl.CostEstimate(flops=flops, bytes_accessed=moved, transcendentals=0),
    )(*args)


def mm(left, right, dims=(((1,), (0,)), ((), ()))):
    return lax.dot_general(left, right, dims, preferred_element_type=jnp.float32)


def iota(shape, dim):
    return lax.broadcasted_iota(jnp.int32, shape, dim)


def attend_kernel(
    pieces,
    lengths_hbm,
    queries_hbm,
    new_keys_hbm,
    new_values_hbm,
    keys_hbm,
    values_hbm,
    weight_hbm,
    mine_ref,
    sent_ref,
    lengths_ref,
    queries_ref,
    new_keys_ref,
    new_values_ref,
    keys_ref,
    values_ref,
    weight_ref,
    own_keys_ref,
    own_values_ref,
    attended_ref,
    arrived,
):
    sequences, heads, head_dim = queries_ref.shape
    kv_heads = new_keys_ref.shape[1]
    group = heads // kv_heads
    span = kv_heads * head_dim
    lanes = group * head_dim
    moves = (
        (lengths_hbm, lengths_ref),
        (queries_hbm, queries_ref),
        (new_keys_hbm, new_keys_ref),
        (new_values_hbm, new_values_ref),
        (keys_hbm, keys_ref),
        (values_hbm, values_ref),
        *((weight_hbm.at[pl.ds(*piece)], weight_ref.at[pl.ds(*piece)]) for piece in pieces),
    )
    copies = [
        pltpu.make_async_copy(source, target, arrived.at[number])
        for number, (source, target) in enumerate(moves)
    ]
    for copy in copies:
        copy.start()

    rows = sequences * heads
    scaling = 1.0 / head_dim**0.5
    for copy in copies[:4]:
        copy.wait()
    queries = queries_ref[...].reshape(rows, head_dim)
    for sequence in range(sequences):
        block = pl.ds(sequence * kv_heads, kv_heads)
        own_keys_ref[block] = new_keys_ref[sequence].astype(jnp.float32)
        own_values_ref[block] = new_values_ref[sequence].astype(jnp.float32)
    own_keys = own_keys_ref[...].astype(jnp.bfloat16)
    own_values = own_values_ref[...].astype(jnp.bfloat16)

    spread = (iota((head_dim, span), 0) == iota((head_dim, span), 1) % head_dim).astype(
        jnp.bfloat16
    )
    same_head = iota((rows, span), 1) // head_dim == iota((rows, span), 0) % heads // group
    wide = jnp.where(same_head, mm(queries, spread), 0.0).astype(jnp.bfloat16)
    pairs = (rows, sequences * kv_heads)
    own_pair = iota(pairs, 1) == iota(pairs, 0) // group
    own_score = (
        jnp.sum(jnp.where(own_pair, mm(queries, own_keys, LAST_DIMS), 0.0), axis=1, keepdims=True)
        * scaling
    )

    copies[4].wait()
    slots = keys_ref.shape[2]
    scores = []
    for sequence in range(sequences):
        block = slice(sequence * heads, (sequence + 1) * heads)
        score = mm(wide[block], keys_ref[sequence]) * scaling
        visible = iota((heads, slots), 1) < lengths_ref[sequence]
        scores.append(jnp.where(visible, score, -1e30))
    scores = jnp.concatenate(scores, axis=0)
    highest = jnp.maximum(jnp.max(scores, axis=1, keepdims=True), own_score)
    cache_exp = jnp.exp(scores - highest)
    own_exp = jnp.exp(own_score - highest)
    totals = jnp.sum(cache_exp, axis=1, keepdims=True) + own_exp
    cache_prob = (cache_exp / totals).astype(jnp.bfloat16)
    own_prob = own_exp / totals
    own_prob = jnp.where(own_pair, own_prob, 0.0).astype(jnp.bfloat16)
    own_part = mm(own_prob, mm(own_values, spread).astype(jnp.bfloat16))

    copies[5].wait()
    attended = [
        mm(
            cache_prob[sequence * heads : (sequence + 1) * heads],
            values_ref[sequence],
            LAST_DIMS,
        )
        for sequence in range(sequences)
    ]
    attended = jnp.concatenate(attended, axis=0) + own_part
    attended = jnp.where(same_head, attended, 0.0).astype(jnp.bfloat16)
    repeat = (iota((span, lanes), 0) % head_dim == iota((span, lanes), 1) % head_dim).astype(
        jnp.bfloat16
    )
    own_lanes = iota((rows, lanes), 1) // head_dim == iota((rows, lanes), 0) % group
    placed = jnp.where(own_lanes, mm(attended, repeat), 0.0).astype(jnp.bfloat16)
    sums = (kv_heads * sequences, rows)
    chosen = (iota(sums, 0) % sequences == iota(sums, 1) // heads) & (
        iota(sums, 0) // sequences == iota(sums, 1) % heads // group
    )
    by_head = mm(chosen.astype(jnp.bfloat16), placed)
    for head in range(kv_heads):
        attended_ref[:, head * lanes : (head + 1) * lanes] = by_head[
            head * sequences : (head + 1) * sequences
        ].astype(jnp.bfloat16)
    attended = attended_ref[...]

    for copy, (start, size) in zip(copies[6:], pieces):
        copy.wait()
        part = mm(attended, weight_ref[pl.ds(start, size)], LAST_DIMS)
        mine_ref[:, start : start + size] = part
        sent_ref[:, start : start + size] = part.astype(jnp.bfloat16)


def attend_and_project(
    queries, new_keys, new_values, cache_keys, cache_values, cache_lengths, out_weight
):
    sequences, heads, head_dim = queries.shape
    kv_heads, slots = cache_keys.shape[1], cache_keys.shape[3]
    depth, width = out_weight.shape
    span = kv_heads * head_dim
    caches = (sequences, span, slots)
    hbm = pl.BlockSpec(memory_space=pltpu.HBM)
    arrays = (
        cache_lengths,
        queries,
        new_keys,
        new_values,
        cache_keys.reshape(caches),
        cache_values.reshape(caches),
        out_weight.T,
    )
    first = -(-width // 512) * 256
    pieces = ((0, first), (first, width - first))
    return pl.pallas_call(
        functools.partial(attend_kernel, pieces),
        out_shape=[
            jax.ShapeDtypeStruct((sequences, width), jnp.float32),
            jax.ShapeDtypeStruct((sequences, width), jnp.bfloat16),
        ],
        in_specs=[hbm] * len(arrays),
        out_specs=[VMEM] * 2,
        scratch_shapes=[pltpu.SMEM(cache_lengths.shape, cache_lengths.dtype)]
        + [pltpu.VMEM(array.shape, array.dtype) for array in arrays[1:]]
        + [
            pltpu.VMEM((sequences * kv_heads, head_dim), jnp.float32),
            pltpu.VMEM((sequences * kv_heads, head_dim), jnp.float32),
            pltpu.VMEM((sequences, depth), jnp.bfloat16),
            pltpu.SemaphoreType.DMA((len(arrays) - 1 + len(pieces),)),
        ],
        compiler_params=pltpu.CompilerParams(vmem_limit_bytes=53 * MIB),
        cost_estimate=pl.CostEstimate(
            flops=2 * sequences * width * depth,
            bytes_accessed=2 * (width * depth + 2 * sequences * span * slots),
            transcendentals=sequences * heads * slots,
        ),
    )(*[pltpu.with_memory_space_constraint(array, pltpu.HBM) for array in arrays])


def route_weights(expert_ids, route_probs, route_order, experts):
    picked = jnp.zeros(expert_ids.shape, jnp.float32)
    for column in range(expert_ids.shape[1]):
        picked = picked + jnp.where(route_order == column, route_probs[:, column : column + 1], 0.0)
    weights = picked / jnp.sum(route_probs, axis=1, keepdims=True)
    named = expert_ids[:, :, None] == jnp.arange(experts, dtype=jnp.int32)[None, None, :]
    return jnp.sum(jnp.where(named, weights[:, :, None], 0.0), axis=1)


def exchange(values, sent, axis, ranks):
    step = 1
    while True:
        pairs = [(rank, rank ^ step) for rank in range(ranks)]
        received = lax.ppermute(sent, axis, pairs)
        step *= 2
        if step >= ranks:
            return values, received
        values = values + received.astype(jnp.float32)
        sent = values.astype(jnp.bfloat16)


def norm_kernel(mine_ref, received_ref, hidden_ref, gain_ref, table_ref, residual_ref, rows_ref):
    width = hidden_ref.shape[1]
    residual = (
        hidden_ref[...].astype(jnp.float32) + mine_ref[...] + received_ref[...].astype(jnp.float32)
    )
    residual_ref[...] = residual
    mean_square = jnp.mean(residual * residual, axis=1, keepdims=True)
    normed = residual * lax.rsqrt(mean_square + EPSILON) * gain_ref[...]
    rows_ref[:, :width] = normed.astype(jnp.bfloat16)
    rows_ref[:, width:] = table_ref[...]


def pack_kernel(*refs):
    *piece_refs, packed_ref = refs
    size = piece_refs[0].shape[0]
    for number, piece_ref in enumerate(piece_refs):
        packed_ref[pl.ds(number * size, size)] = piece_ref[...]


def expert_kernel(experts, *refs):
    *row_refs, gate_ref, up_ref, down_ref, mine_ref, other_ref = refs
    local_experts, _, width = down_ref.shape
    rows = jnp.concatenate([ref[:, :width] for ref in row_refs], axis=0)
    table = jnp.concatenate([ref[:, width:] for ref in row_refs], axis=0).astype(jnp.float32)
    column = lax.broadcasted_iota(jnp.int32, table.shape, 1)
    total = None
    for local in range(local_experts):
        expert = lax.axis_index("expert") * local_experts + local
        chosen = (column == expert) | (column == expert + experts)
        weight = jnp.sum(jnp.where(chosen, table, 0.0), axis=1, keepdims=True)
        gate = lax.dot_general(
            gate_ref[local], rows, LAST_DIMS, preferred_element_type=jnp.float32
        )
        up = lax.dot_general(up_ref[local], rows, LAST_DIMS, preferred_element_type=jnp.float32)
        active = (gate * jax.nn.sigmoid(GLU_SLOPE * gate) * (up + 1.0)).astype(jnp.bfloat16)
        part = lax.dot_general(
            active, down_ref[local], FIRST_DIMS, preferred_element_type=jnp.float32
        )
        part = part * weight
        total = part if total is None else total + part
    half = mine_ref.shape[0]
    mine_ref[...] = total[:half]
    other_ref[...] = total[half:].astype(jnp.bfloat16)


def split_kernel(mine_ref, received_ref, kept_ref, *sent_refs):
    size = kept_ref.shape[0]
    kept_ref[...] = mine_ref[:size] + received_ref[:size].astype(jnp.float32)
    for number, sent_ref in enumerate(sent_refs, 1):
        block = pl.ds(number * size, size)
        total = mine_ref[block] + received_ref[block].astype(jnp.float32)
        sent_ref[...] = total.astype(jnp.bfloat16)


def return_kernel(received, residual_ref, *refs):
    kept_ref, *received_refs = refs[: 1 + received]
    base_ref, *sent_refs = refs[1 + received :]
    total = kept_ref[...]
    for received_ref in received_refs:
        total = total + received_ref[...].astype(jnp.float32)
    width = base_ref.shape[1]
    rank = lax.axis_index("tensor")

    def slab_of(values, owner):
        slab = values[:, :width]
        for number in range(1, values.shape[1] // width):
            piece = values[:, number * width : (number + 1) * width]
            slab = jnp.where(owner == number, piece, slab)
        return slab

    base_ref[...] = slab_of(total + residual_ref[...], rank)
    for step, sent_ref in enumerate(sent_refs, 1):
        sent_ref[...] = slab_of(total, rank ^ step).astype(jnp.bfloat16)


def per_device(
    hidden_in,
    queries,
    new_keys,
    new_values,
    cache_keys,
    cache_values,
    cache_lengths,
    out_weight,
    norm_gain,
    expert_ids,
    route_probs,
    route_order,
    gate_weight,
    up_weight,
    down_weight,
):
    sequences, width = hidden_in.shape
    expert_ranks = lax.axis_size("expert")
    tensor_ranks = lax.axis_size("tensor")
    local_experts, hidden_units = down_weight.shape[:2]
    experts = local_experts * expert_ranks
    inner = 2
    outer = expert_ranks // inner
    row_width = -(-(width + 2 * experts) // 128) * 128

    def to_outer(values, step):
        pairs = [(rank, rank ^ (step * inner)) for rank in range(expert_ranks)]
        return lax.ppermute(values, "expert", pairs)

    def to_inner(values):
        return lax.ppermute(values, "expert", [(rank, rank ^ 1) for rank in range(expert_ranks)])

    operands = (queries, new_keys, new_values, cache_keys, cache_values, cache_lengths)
    if queries.shape[1] % 16 == 0:
        mine, sent = attend_and_project(*operands, out_weight)
    else:
        mine = jnp.dot(attend(*operands), out_weight, preferred_element_type=jnp.float32)
        sent = mine.astype(jnp.bfloat16)
    mine, received = exchange(mine, sent, "tensor", tensor_ranks)

    weights = route_weights(expert_ids, route_probs, route_order, experts)
    high = weights.astype(jnp.bfloat16)
    low = (weights - high.astype(jnp.float32)).astype(jnp.bfloat16)
    spare = jnp.zeros((sequences, row_width - width - 2 * experts), jnp.bfloat16)
    table = jnp.concatenate([high, low, spare], axis=1)

    block = (sequences, width)
    residual, rows = call(
        norm_kernel,
        [(block, jnp.float32), ((sequences, row_width), jnp.bfloat16)],
        (mine, received, hidden_in, norm_gain.reshape(1, width), table),
        flops=WINDOW_FLOPS,
        moved=sequences * width * 16,
        limit=2 * MIB,
    )

    near = [rows]
    for step in range(1, outer):
        near.append(to_outer(rows, step))
    (near,) = call(
        pack_kernel,
        [((outer * sequences, row_width), jnp.bfloat16)],
        near,
        flops=sequences,
        moved=4 * outer * sequences * row_width,
        limit=2 * MIB,
    )
    far = to_inner(near)
    half = (outer * sequences, width)
    mine, other = call(
        functools.partial(expert_kernel, experts),
        [(half, jnp.float32), (half, jnp.bfloat16)],
        (near, far, gate_weight.swapaxes(1, 2), up_weight.swapaxes(1, 2), down_weight),
        flops=12 * half[0] * width * hidden_units * local_experts,
        moved=6 * width * hidden_units * local_experts,
        limit=16 * MIB,
    )
    received = to_inner(other)
    kept, *sent = call(
        split_kernel,
        [(block, jnp.float32)] + [(block, jnp.bfloat16)] * (outer - 1),
        (mine, received),
        flops=half[0] * width,
        moved=half[0] * width * 8,
        limit=4 * MIB,
    )
    returned = []
    for step, piece in enumerate(sent, 1):
        returned.append(to_outer(piece, step))
    slab = (sequences, width // tensor_ranks)
    total, *sent = call(
        functools.partial(return_kernel, len(returned)),
        [(slab, jnp.float32)] + [(slab, jnp.bfloat16)] * (tensor_ranks - 1),
        (residual, kept, *returned),
        flops=half[0] * width,
        moved=half[0] * width * 2,
        limit=2 * MIB,
    )
    for step, piece in enumerate(sent, 1):
        pairs = [(rank, rank ^ step) for rank in range(tensor_ranks)]
        total = total + lax.ppermute(piece, "tensor", pairs).astype(jnp.float32)
    return total.astype(jnp.bfloat16)


def solution(mesh):
    in_specs = (
        P(("groups", "expert"), None),
        P(("groups", "expert"), "tensor", None),
        P(("groups", "expert"), "tensor", None),
        P(("groups", "expert"), "tensor", None),
        P(("groups", "expert"), "tensor", None, None),
        P(("groups", "expert"), "tensor", None, None),
        P(("groups", "expert")),
        P("tensor", None),
        P(),
        P(("groups", "expert"), None),
        P(("groups", "expert"), None),
        P(("groups", "expert"), None),
        P("expert", None, "tensor"),
        P("expert", None, "tensor"),
        P("expert", "tensor", None),
    )
    out_specs = P(("groups", "expert"), "tensor")

    return jax.shard_map(
        per_device, mesh=mesh, in_specs=in_specs, out_specs=out_specs, check_vma=False
    )
```

```python
import functools

import jax
import jax.numpy as jnp
from jax import lax
from jax.experimental import pallas as pl
from jax.experimental.pallas import tpu as pltpu
from jax.sharding import PartitionSpec as P

EPSILON = 1e-05
GLU_SLOPE = 1.702
WINDOW_FLOPS = 200_000_000_000


def attend(queries, new_keys, new_values, cache_keys, cache_values, cache_lengths):
    sequence_count, head_count, head_dim = queries.shape
    kv_heads = new_keys.shape[1]
    group_size = head_count // kv_heads
    scaling = 1.0 / head_dim**0.5
    query_rows = queries.reshape(sequence_count, kv_heads, group_size, head_dim)
    scores = (
        jnp.einsum("sgqd,sgdc->sgqc", query_rows, cache_keys, preferred_element_type=jnp.float32)
        * scaling
    )
    own_score = (
        jnp.einsum("sgqd,sgd->sgq", query_rows, new_keys, preferred_element_type=jnp.float32)
        * scaling
    )
    positions = jnp.arange(cache_keys.shape[3], dtype=jnp.int32)
    visible = positions[None, :] < cache_lengths[:, None]
    scores = jnp.where(visible[:, None, None, :], scores, -1e30)
    highest = jnp.maximum(jnp.max(scores, axis=3), own_score)
    cache_exp = jnp.exp(scores - highest[..., None])
    own_exp = jnp.exp(own_score - highest)
    totals = jnp.sum(cache_exp, axis=3) + own_exp
    cache_prob = (cache_exp / totals[..., None]).astype(jnp.bfloat16)
    own_prob = (own_exp / totals).astype(jnp.bfloat16)
    attended = jnp.einsum(
        "sgqc,sgdc->sgqd", cache_prob, cache_values, preferred_element_type=jnp.float32
    )
    attended = (
        attended
        + own_prob.astype(jnp.float32)[..., None] * new_values.astype(jnp.float32)[:, :, None, :]
    )
    return attended.astype(jnp.bfloat16).reshape(sequence_count, head_count * head_dim)


VMEM = pl.BlockSpec(memory_space=pltpu.VMEM)
LAST_DIMS = (((1,), (1,)), ((), ()))
MIB = 1 << 20


def call(kernel, outs, args, flops, moved, limit):
    return pl.pallas_call(
        kernel,
        out_shape=[jax.ShapeDtypeStruct(shape, dtype) for shape, dtype in outs],
        in_specs=[VMEM] * len(args),
        out_specs=[VMEM] * len(outs),
        compiler_params=pltpu.CompilerParams(vmem_limit_bytes=limit),
        cost_estimate=pl.CostEstimate(flops=flops, bytes_accessed=moved, transcendentals=0),
    )(*args)


def mm(left, right, dims=(((1,), (0,)), ((), ()))):
    return lax.dot_general(left, right, dims, preferred_element_type=jnp.float32)


def iota(shape, dim):
    return lax.broadcasted_iota(jnp.int32, shape, dim)


def attend_kernel(
    pieces,
    lengths_hbm,
    queries_hbm,
    new_keys_hbm,
    new_values_hbm,
    keys_hbm,
    values_hbm,
    weight_hbm,
    mine_ref,
    sent_ref,
    lengths_ref,
    queries_ref,
    new_keys_ref,
    new_values_ref,
    keys_ref,
    values_ref,
    weight_ref,
    own_keys_ref,
    own_values_ref,
    attended_ref,
    arrived,
):
    sequences, heads, head_dim = queries_ref.shape
    kv_heads = new_keys_ref.shape[1]
    group = heads // kv_heads
    span = kv_heads * head_dim
    lanes = group * head_dim
    moves = (
        (lengths_hbm, lengths_ref),
        (queries_hbm, queries_ref),
        (new_keys_hbm, new_keys_ref),
        (new_values_hbm, new_values_ref),
        (keys_hbm, keys_ref),
        (values_hbm, values_ref),
        *((weight_hbm.at[pl.ds(*piece)], weight_ref.at[pl.ds(*piece)]) for piece in pieces),
    )
    copies = [
        pltpu.make_async_copy(source, target, arrived.at[number])
        for number, (source, target) in enumerate(moves)
    ]
    for copy in copies:
        copy.start()

    rows = sequences * heads
    scaling = 1.0 / head_dim**0.5
    for copy in copies[:4]:
        copy.wait()
    queries = queries_ref[...].reshape(rows, head_dim)
    for sequence in range(sequences):
        block = pl.ds(sequence * kv_heads, kv_heads)
        own_keys_ref[block] = new_keys_ref[sequence].astype(jnp.float32)
        own_values_ref[block] = new_values_ref[sequence].astype(jnp.float32)
    own_keys = own_keys_ref[...].astype(jnp.bfloat16)
    own_values = own_values_ref[...].astype(jnp.bfloat16)

    spread = (iota((head_dim, span), 0) == iota((head_dim, span), 1) % head_dim).astype(
        jnp.bfloat16
    )
    same_head = iota((rows, span), 1) // head_dim == iota((rows, span), 0) % heads // group
    wide = jnp.where(same_head, mm(queries, spread), 0.0).astype(jnp.bfloat16)
    pairs = (rows, sequences * kv_heads)
    own_pair = iota(pairs, 1) == iota(pairs, 0) // group
    own_score = (
        jnp.sum(jnp.where(own_pair, mm(queries, own_keys, LAST_DIMS), 0.0), axis=1, keepdims=True)
        * scaling
    )

    copies[4].wait()
    slots = keys_ref.shape[2]
    scores = []
    for sequence in range(sequences):
        block = slice(sequence * heads, (sequence + 1) * heads)
        score = mm(wide[block], keys_ref[sequence]) * scaling
        visible = iota((heads, slots), 1) < lengths_ref[sequence]
        scores.append(jnp.where(visible, score, -1e30))
    scores = jnp.concatenate(scores, axis=0)
    highest = jnp.maximum(jnp.max(scores, axis=1, keepdims=True), own_score)
    cache_exp = jnp.exp(scores - highest)
    own_exp = jnp.exp(own_score - highest)
    totals = jnp.sum(cache_exp, axis=1, keepdims=True) + own_exp
    cache_prob = (cache_exp / totals).astype(jnp.bfloat16)
    own_prob = own_exp / totals
    own_prob = jnp.where(own_pair, own_prob, 0.0).astype(jnp.bfloat16)
    own_part = mm(own_prob, mm(own_values, spread).astype(jnp.bfloat16))

    copies[5].wait()
    attended = [
        mm(
            cache_prob[sequence * heads : (sequence + 1) * heads],
            values_ref[sequence],
            LAST_DIMS,
        )
        for sequence in range(sequences)
    ]
    attended = jnp.concatenate(attended, axis=0) + own_part
    attended = jnp.where(same_head, attended, 0.0).astype(jnp.bfloat16)
    repeat = (iota((span, lanes), 0) % head_dim == iota((span, lanes), 1) % head_dim).astype(
        jnp.bfloat16
    )
    own_lanes = iota((rows, lanes), 1) // head_dim == iota((rows, lanes), 0) % group
    placed = jnp.where(own_lanes, mm(attended, repeat), 0.0).astype(jnp.bfloat16)
    sums = (kv_heads * sequences, rows)
    chosen = (iota(sums, 0) % sequences == iota(sums, 1) // heads) & (
        iota(sums, 0) // sequences == iota(sums, 1) % heads // group
    )
    by_head = mm(chosen.astype(jnp.bfloat16), placed)
    for head in range(kv_heads):
        attended_ref[:, head * lanes : (head + 1) * lanes] = by_head[
            head * sequences : (head + 1) * sequences
        ].astype(jnp.bfloat16)
    attended = attended_ref[...]

    for copy, (start, size) in zip(copies[6:], pieces):
        copy.wait()
        part = mm(attended, weight_ref[pl.ds(start, size)], LAST_DIMS)
        mine_ref[:, start : start + size] = part
        sent_ref[:, start : start + size] = part.astype(jnp.bfloat16)


def attend_and_project(
    queries, new_keys, new_values, cache_keys, cache_values, cache_lengths, out_weight
):
    sequences, heads, head_dim = queries.shape
    kv_heads, slots = cache_keys.shape[1], cache_keys.shape[3]
    depth, width = out_weight.shape
    span = kv_heads * head_dim
    caches = (sequences, span, slots)
    hbm = pl.BlockSpec(memory_space=pltpu.HBM)
    arrays = (
        cache_lengths,
        queries,
        new_keys,
        new_values,
        cache_keys.reshape(caches),
        cache_values.reshape(caches),
        out_weight.T,
    )
    first = -(-width // 512) * 256
    pieces = ((0, first), (first, width - first))
    return pl.pallas_call(
        functools.partial(attend_kernel, pieces),
        out_shape=[
            jax.ShapeDtypeStruct((sequences, width), jnp.float32),
            jax.ShapeDtypeStruct((sequences, width), jnp.bfloat16),
        ],
        in_specs=[hbm] * len(arrays),
        out_specs=[VMEM] * 2,
        scratch_shapes=[pltpu.SMEM(cache_lengths.shape, cache_lengths.dtype)]
        + [pltpu.VMEM(array.shape, array.dtype) for array in arrays[1:]]
        + [
            pltpu.VMEM((sequences * kv_heads, head_dim), jnp.float32),
            pltpu.VMEM((sequences * kv_heads, head_dim), jnp.float32),
            pltpu.VMEM((sequences, depth), jnp.bfloat16),
            pltpu.SemaphoreType.DMA((len(arrays) - 1 + len(pieces),)),
        ],
        compiler_params=pltpu.CompilerParams(vmem_limit_bytes=53 * MIB),
        cost_estimate=pl.CostEstimate(
            flops=2 * sequences * width * depth,
            bytes_accessed=2 * (width * depth + 2 * sequences * span * slots),
            transcendentals=sequences * heads * slots,
        ),
    )(*[pltpu.with_memory_space_constraint(array, pltpu.HBM) for array in arrays])


def route_weights(expert_ids, route_probs, route_order, experts):
    picked = jnp.zeros(expert_ids.shape, jnp.float32)
    for column in range(expert_ids.shape[1]):
        picked = picked + jnp.where(route_order == column, route_probs[:, column : column + 1], 0.0)
    weights = picked / jnp.sum(route_probs, axis=1, keepdims=True)
    named = expert_ids[:, :, None] == jnp.arange(experts, dtype=jnp.int32)[None, None, :]
    return jnp.sum(jnp.where(named, weights[:, :, None], 0.0), axis=1)


def exchange(values, sent, axis, ranks):
    step = 1
    while True:
        pairs = [(rank, rank ^ step) for rank in range(ranks)]
        received = lax.ppermute(sent, axis, pairs)
        step *= 2
        if step >= ranks:
            return values, received
        values = values + received.astype(jnp.float32)
        sent = values.astype(jnp.bfloat16)


def norm_kernel(mine_ref, received_ref, hidden_ref, gain_ref, table_ref, residual_ref, rows_ref):
    width = hidden_ref.shape[1]
    residual = (
        hidden_ref[...].astype(jnp.float32) + mine_ref[...] + received_ref[...].astype(jnp.float32)
    )
    residual_ref[...] = residual
    mean_square = jnp.mean(residual * residual, axis=1, keepdims=True)
    normed = residual * lax.rsqrt(mean_square + EPSILON) * gain_ref[...]
    rows_ref[:, :width] = normed.astype(jnp.bfloat16)
    rows_ref[:, width:] = table_ref[...]


def pack_kernel(*refs):
    *piece_refs, _, packed_ref = refs
    size = piece_refs[0].shape[0]
    for number, piece_ref in enumerate(piece_refs):
        packed_ref[pl.ds(number * size, size)] = piece_ref[...]


def turn_kernel(source_ref, target_ref):
    for local in range(source_ref.shape[0]):
        target_ref[local] = source_ref[local].T


def turn(weight):
    count, _, _ = weight.shape
    (turned,) = call(
        turn_kernel,
        [(weight.shape, weight.dtype)],
        (weight.swapaxes(1, 2),),
        flops=count,
        moved=count,
        limit=6 * MIB,
    )
    return turned


def expert_kernel(experts, *refs):
    *row_refs, gate_ref, up_ref, down_ref, mine_ref, other_ref = refs
    local_experts, _, width = down_ref.shape
    rows = jnp.concatenate([ref[:, :width] for ref in row_refs], axis=0)
    table = jnp.concatenate([ref[:, width:] for ref in row_refs], axis=0).astype(jnp.float32)
    column = lax.broadcasted_iota(jnp.int32, table.shape, 1)
    total = None
    for local in range(local_experts):
        expert = lax.axis_index("expert") * local_experts + local
        chosen = (column == expert) | (column == expert + experts)
        weight = jnp.sum(jnp.where(chosen, table, 0.0), axis=1, keepdims=True)
        gate = mm(rows, gate_ref[local])
        up = mm(rows, up_ref[local])
        active = (gate * jax.nn.sigmoid(GLU_SLOPE * gate) * (up + 1.0)).astype(jnp.bfloat16)
        part = mm(active, down_ref[local])
        part = part * weight
        total = part if total is None else total + part
    half = mine_ref.shape[0]
    mine_ref[...] = total[:half]
    other_ref[...] = total[half:].astype(jnp.bfloat16)


def split_kernel(mine_ref, received_ref, kept_ref, *sent_refs):
    size = kept_ref.shape[0]
    kept_ref[...] = mine_ref[:size] + received_ref[:size].astype(jnp.float32)
    for number, sent_ref in enumerate(sent_refs, 1):
        block = pl.ds(number * size, size)
        total = mine_ref[block] + received_ref[block].astype(jnp.float32)
        sent_ref[...] = total.astype(jnp.bfloat16)


def return_kernel(received, residual_ref, *refs):
    kept_ref, *received_refs = refs[: 1 + received]
    base_ref, *sent_refs = refs[1 + received :]
    total = kept_ref[...]
    for received_ref in received_refs:
        total = total + received_ref[...].astype(jnp.float32)
    width = base_ref.shape[1]
    rank = lax.axis_index("tensor")

    def slab_of(values, owner):
        slab = values[:, :width]
        for number in range(1, values.shape[1] // width):
            piece = values[:, number * width : (number + 1) * width]
            slab = jnp.where(owner == number, piece, slab)
        return slab

    base_ref[...] = slab_of(total + residual_ref[...], rank)
    for step, sent_ref in enumerate(sent_refs, 1):
        sent_ref[...] = slab_of(total, rank ^ step).astype(jnp.bfloat16)


def per_device(
    hidden_in,
    queries,
    new_keys,
    new_values,
    cache_keys,
    cache_values,
    cache_lengths,
    out_weight,
    norm_gain,
    expert_ids,
    route_probs,
    route_order,
    gate_weight,
    up_weight,
    down_weight,
):
    sequences, width = hidden_in.shape
    expert_ranks = lax.axis_size("expert")
    tensor_ranks = lax.axis_size("tensor")
    local_experts, hidden_units = down_weight.shape[:2]
    experts = local_experts * expert_ranks
    inner = 2
    outer = expert_ranks // inner
    row_width = -(-(width + 2 * experts) // 128) * 128

    def to_outer(values, step):
        pairs = [(rank, rank ^ (step * inner)) for rank in range(expert_ranks)]
        return lax.ppermute(values, "expert", pairs)

    def to_inner(values):
        return lax.ppermute(values, "expert", [(rank, rank ^ 1) for rank in range(expert_ranks)])

    operands = (queries, new_keys, new_values, cache_keys, cache_values, cache_lengths)
    if queries.shape[1] % 16 == 0:
        mine, sent = attend_and_project(*operands, out_weight)
    else:
        mine = jnp.dot(attend(*operands), out_weight, preferred_element_type=jnp.float32)
        sent = mine.astype(jnp.bfloat16)
    mine, received = exchange(mine, sent, "tensor", tensor_ranks)

    weights = route_weights(expert_ids, route_probs, route_order, experts)
    high = weights.astype(jnp.bfloat16)
    low = (weights - high.astype(jnp.float32)).astype(jnp.bfloat16)
    spare = jnp.zeros((sequences, row_width - width - 2 * experts), jnp.bfloat16)
    table = jnp.concatenate([high, low, spare], axis=1)

    block = (sequences, width)
    residual, rows = call(
        norm_kernel,
        [(block, jnp.float32), ((sequences, row_width), jnp.bfloat16)],
        (mine, received, hidden_in, norm_gain.reshape(1, width), table),
        flops=WINDOW_FLOPS,
        moved=sequences * width * 16,
        limit=2 * MIB,
    )

    near = [rows]
    for step in range(1, outer):
        near.append(to_outer(rows, step))
    gate_weight = turn(gate_weight)
    (near,) = call(
        pack_kernel,
        [((outer * sequences, row_width), jnp.bfloat16)],
        (*near, down_weight),
        flops=sequences,
        moved=4 * outer * sequences * row_width,
        limit=2 * MIB,
    )
    far = to_inner(near)
    up_weight = turn(up_weight)
    half = (outer * sequences, width)
    mine, other = call(
        functools.partial(expert_kernel, experts),
        [(half, jnp.float32), (half, jnp.bfloat16)],
        (near, far, gate_weight, up_weight, down_weight),
        flops=12 * half[0] * width * hidden_units * local_experts,
        moved=6 * width * hidden_units * local_experts,
        limit=16 * MIB,
    )
    received = to_inner(other)
    kept, *sent = call(
        split_kernel,
        [(block, jnp.float32)] + [(block, jnp.bfloat16)] * (outer - 1),
        (mine, received),
        flops=half[0] * width,
        moved=half[0] * width * 8,
        limit=4 * MIB,
    )
    returned = []
    for step, piece in enumerate(sent, 1):
        returned.append(to_outer(piece, step))
    slab = (sequences, width // tensor_ranks)
    total, *sent = call(
        functools.partial(return_kernel, len(returned)),
        [(slab, jnp.float32)] + [(slab, jnp.bfloat16)] * (tensor_ranks - 1),
        (residual, kept, *returned),
        flops=half[0] * width,
        moved=half[0] * width * 2,
        limit=2 * MIB,
    )
    for step, piece in enumerate(sent, 1):
        pairs = [(rank, rank ^ step) for rank in range(tensor_ranks)]
        total = total + lax.ppermute(piece, "tensor", pairs).astype(jnp.float32)
    return total.astype(jnp.bfloat16)


def solution(mesh):
    in_specs = (
        P(("groups", "expert"), None),
        P(("groups", "expert"), "tensor", None),
        P(("groups", "expert"), "tensor", None),
        P(("groups", "expert"), "tensor", None),
        P(("groups", "expert"), "tensor", None, None),
        P(("groups", "expert"), "tensor", None, None),
        P(("groups", "expert")),
        P("tensor", None),
        P(),
        P(("groups", "expert"), None),
        P(("groups", "expert"), None),
        P(("groups", "expert"), None),
        P("expert", None, "tensor"),
        P("expert", None, "tensor"),
        P("expert", "tensor", None),
    )
    out_specs = P(("groups", "expert"), "tensor")

    return jax.shard_map(
        per_device, mesh=mesh, in_specs=in_specs, out_specs=out_specs, check_vma=False
    )
```

```python
import functools

import jax
import jax.numpy as jnp
from jax import lax
from jax.experimental import pallas as pl
from jax.experimental.pallas import tpu as pltpu
from jax.sharding import PartitionSpec as P

EPSILON = 1e-05
GLU_SLOPE = 1.702
WINDOW_FLOPS = 200_000_000_000


def attend(queries, new_keys, new_values, cache_keys, cache_values, cache_lengths):
    sequence_count, head_count, head_dim = queries.shape
    kv_heads = new_keys.shape[1]
    group_size = head_count // kv_heads
    scaling = 1.0 / head_dim**0.5
    query_rows = queries.reshape(sequence_count, kv_heads, group_size, head_dim)
    scores = (
        jnp.einsum("sgqd,sgdc->sgqc", query_rows, cache_keys, preferred_element_type=jnp.float32)
        * scaling
    )
    own_score = (
        jnp.einsum("sgqd,sgd->sgq", query_rows, new_keys, preferred_element_type=jnp.float32)
        * scaling
    )
    positions = jnp.arange(cache_keys.shape[3], dtype=jnp.int32)
    visible = positions[None, :] < cache_lengths[:, None]
    scores = jnp.where(visible[:, None, None, :], scores, -1e30)
    highest = jnp.maximum(jnp.max(scores, axis=3), own_score)
    cache_exp = jnp.exp(scores - highest[..., None])
    own_exp = jnp.exp(own_score - highest)
    totals = jnp.sum(cache_exp, axis=3) + own_exp
    cache_prob = (cache_exp / totals[..., None]).astype(jnp.bfloat16)
    own_prob = (own_exp / totals).astype(jnp.bfloat16)
    attended = jnp.einsum(
        "sgqc,sgdc->sgqd", cache_prob, cache_values, preferred_element_type=jnp.float32
    )
    attended = (
        attended
        + own_prob.astype(jnp.float32)[..., None] * new_values.astype(jnp.float32)[:, :, None, :]
    )
    return attended.astype(jnp.bfloat16).reshape(sequence_count, head_count * head_dim)


VMEM = pl.BlockSpec(memory_space=pltpu.VMEM)
LAST_DIMS = (((1,), (1,)), ((), ()))
MIB = 1 << 20


def call(kernel, outs, args, flops, moved, limit):
    return pl.pallas_call(
        kernel,
        out_shape=[jax.ShapeDtypeStruct(shape, dtype) for shape, dtype in outs],
        in_specs=[VMEM] * len(args),
        out_specs=[VMEM] * len(outs),
        compiler_params=pltpu.CompilerParams(vmem_limit_bytes=limit),
        cost_estimate=pl.CostEstimate(flops=flops, bytes_accessed=moved, transcendentals=0),
    )(*args)


def mm(left, right, dims=(((1,), (0,)), ((), ()))):
    return lax.dot_general(left, right, dims, preferred_element_type=jnp.float32)


def iota(shape, dim):
    return lax.broadcasted_iota(jnp.int32, shape, dim)


def attend_kernel(
    pieces,
    lengths_hbm,
    queries_hbm,
    new_keys_hbm,
    new_values_hbm,
    keys_hbm,
    values_hbm,
    weight_hbm,
    mine_ref,
    sent_ref,
    lengths_ref,
    queries_ref,
    new_keys_ref,
    new_values_ref,
    keys_ref,
    values_ref,
    weight_ref,
    own_keys_ref,
    own_values_ref,
    attended_ref,
    arrived,
):
    sequences, heads, head_dim = queries_ref.shape
    kv_heads = new_keys_ref.shape[1]
    group = heads // kv_heads
    span = kv_heads * head_dim
    lanes = group * head_dim
    moves = (
        (lengths_hbm, lengths_ref),
        (queries_hbm, queries_ref),
        (new_keys_hbm, new_keys_ref),
        (new_values_hbm, new_values_ref),
        (keys_hbm, keys_ref),
        (values_hbm, values_ref),
        *((weight_hbm.at[pl.ds(*piece)], weight_ref.at[pl.ds(*piece)]) for piece in pieces),
    )
    copies = [
        pltpu.make_async_copy(source, target, arrived.at[number])
        for number, (source, target) in enumerate(moves)
    ]
    for copy in copies:
        copy.start()

    rows = sequences * heads
    scaling = 1.0 / head_dim**0.5
    for copy in copies[:4]:
        copy.wait()
    queries = queries_ref[...].reshape(rows, head_dim)
    for sequence in range(sequences):
        block = pl.ds(sequence * kv_heads, kv_heads)
        own_keys_ref[block] = new_keys_ref[sequence].astype(jnp.float32)
        own_values_ref[block] = new_values_ref[sequence].astype(jnp.float32)
    own_keys = own_keys_ref[...].astype(jnp.bfloat16)
    own_values = own_values_ref[...].astype(jnp.bfloat16)

    spread = (iota((head_dim, span), 0) == iota((head_dim, span), 1) % head_dim).astype(
        jnp.bfloat16
    )
    same_head = iota((rows, span), 1) // head_dim == iota((rows, span), 0) % heads // group
    wide = jnp.where(same_head, mm(queries, spread), 0.0).astype(jnp.bfloat16)
    pairs = (rows, sequences * kv_heads)
    own_pair = iota(pairs, 1) == iota(pairs, 0) // group
    own_score = (
        jnp.sum(jnp.where(own_pair, mm(queries, own_keys, LAST_DIMS), 0.0), axis=1, keepdims=True)
        * scaling
    )

    copies[4].wait()
    slots = keys_ref.shape[2]
    scores = []
    for sequence in range(sequences):
        block = slice(sequence * heads, (sequence + 1) * heads)
        score = mm(wide[block], keys_ref[sequence]) * scaling
        visible = iota((heads, slots), 1) < lengths_ref[sequence]
        scores.append(jnp.where(visible, score, -1e30))
    scores = jnp.concatenate(scores, axis=0)
    highest = jnp.maximum(jnp.max(scores, axis=1, keepdims=True), own_score)
    cache_exp = jnp.exp(scores - highest)
    own_exp = jnp.exp(own_score - highest)
    totals = jnp.sum(cache_exp, axis=1, keepdims=True) + own_exp
    cache_prob = (cache_exp / totals).astype(jnp.bfloat16)
    own_prob = own_exp / totals
    own_prob = jnp.where(own_pair, own_prob, 0.0).astype(jnp.bfloat16)
    own_part = mm(own_prob, mm(own_values, spread).astype(jnp.bfloat16))

    copies[5].wait()
    attended = [
        mm(
            cache_prob[sequence * heads : (sequence + 1) * heads],
            values_ref[sequence],
            LAST_DIMS,
        )
        for sequence in range(sequences)
    ]
    attended = jnp.concatenate(attended, axis=0) + own_part
    attended = jnp.where(same_head, attended, 0.0).astype(jnp.bfloat16)
    repeat = (iota((span, lanes), 0) % head_dim == iota((span, lanes), 1) % head_dim).astype(
        jnp.bfloat16
    )
    own_lanes = iota((rows, lanes), 1) // head_dim == iota((rows, lanes), 0) % group
    placed = jnp.where(own_lanes, mm(attended, repeat), 0.0).astype(jnp.bfloat16)
    sums = (kv_heads * sequences, rows)
    chosen = (iota(sums, 0) % sequences == iota(sums, 1) // heads) & (
        iota(sums, 0) // sequences == iota(sums, 1) % heads // group
    )
    by_head = mm(chosen.astype(jnp.bfloat16), placed)
    for head in range(kv_heads):
        attended_ref[:, head * lanes : (head + 1) * lanes] = by_head[
            head * sequences : (head + 1) * sequences
        ].astype(jnp.bfloat16)
    attended = attended_ref[...]

    for copy, (start, size) in zip(copies[6:], pieces):
        copy.wait()
        part = mm(attended, weight_ref[pl.ds(start, size)], LAST_DIMS)
        mine_ref[:, start : start + size] = part
        sent_ref[:, start : start + size] = part.astype(jnp.bfloat16)


def attend_and_project(
    queries, new_keys, new_values, cache_keys, cache_values, cache_lengths, out_weight
):
    sequences, heads, head_dim = queries.shape
    kv_heads, slots = cache_keys.shape[1], cache_keys.shape[3]
    depth, width = out_weight.shape
    span = kv_heads * head_dim
    caches = (sequences, span, slots)
    hbm = pl.BlockSpec(memory_space=pltpu.HBM)
    arrays = (
        cache_lengths,
        queries,
        new_keys,
        new_values,
        cache_keys.reshape(caches),
        cache_values.reshape(caches),
        out_weight.T,
    )
    first = -(-width // 512) * 256
    pieces = ((0, first), (first, width - first))
    return pl.pallas_call(
        functools.partial(attend_kernel, pieces),
        out_shape=[
            jax.ShapeDtypeStruct((sequences, width), jnp.float32),
            jax.ShapeDtypeStruct((sequences, width), jnp.bfloat16),
        ],
        in_specs=[hbm] * len(arrays),
        out_specs=[VMEM] * 2,
        scratch_shapes=[pltpu.SMEM(cache_lengths.shape, cache_lengths.dtype)]
        + [pltpu.VMEM(array.shape, array.dtype) for array in arrays[1:]]
        + [
            pltpu.VMEM((sequences * kv_heads, head_dim), jnp.float32),
            pltpu.VMEM((sequences * kv_heads, head_dim), jnp.float32),
            pltpu.VMEM((sequences, depth), jnp.bfloat16),
            pltpu.SemaphoreType.DMA((len(arrays) - 1 + len(pieces),)),
        ],
        compiler_params=pltpu.CompilerParams(vmem_limit_bytes=53 * MIB),
        cost_estimate=pl.CostEstimate(
            flops=2 * sequences * width * depth,
            bytes_accessed=2 * (width * depth + 2 * sequences * span * slots),
            transcendentals=sequences * heads * slots,
        ),
    )(*[pltpu.with_memory_space_constraint(array, pltpu.HBM) for array in arrays])


def route_weights(expert_ids, route_probs, route_order, experts):
    picked = jnp.zeros(expert_ids.shape, jnp.float32)
    for column in range(expert_ids.shape[1]):
        picked = picked + jnp.where(route_order == column, route_probs[:, column : column + 1], 0.0)
    weights = picked / jnp.sum(route_probs, axis=1, keepdims=True)
    named = expert_ids[:, :, None] == jnp.arange(experts, dtype=jnp.int32)[None, None, :]
    return jnp.sum(jnp.where(named, weights[:, :, None], 0.0), axis=1)


def exchange(values, sent, axis, ranks):
    step = 1
    while True:
        pairs = [(rank, rank ^ step) for rank in range(ranks)]
        received = lax.ppermute(sent, axis, pairs)
        step *= 2
        if step >= ranks:
            return values, received
        values = values + received.astype(jnp.float32)
        sent = values.astype(jnp.bfloat16)


def norm_kernel(mine_ref, received_ref, hidden_ref, gain_ref, table_ref, residual_ref, rows_ref):
    width = hidden_ref.shape[1]
    residual = (
        hidden_ref[...].astype(jnp.float32) + mine_ref[...] + received_ref[...].astype(jnp.float32)
    )
    residual_ref[...] = residual
    mean_square = jnp.mean(residual * residual, axis=1, keepdims=True)
    normed = residual * lax.rsqrt(mean_square + EPSILON) * gain_ref[...]
    rows_ref[:, :width] = normed.astype(jnp.bfloat16)
    rows_ref[:, width:] = table_ref[...]


def pack_kernel(*refs):
    *piece_refs, packed_ref = refs
    size = piece_refs[0].shape[0]
    for number, piece_ref in enumerate(piece_refs):
        packed_ref[pl.ds(number * size, size)] = piece_ref[...]


def turn_kernel(*refs):
    for source_ref, target_ref in zip(refs[: len(refs) // 2], refs[len(refs) // 2 :]):
        for local in range(source_ref.shape[0]):
            target_ref[local] = source_ref[local].T


def turn(*weights):
    return call(
        turn_kernel,
        [(weight.shape, weight.dtype) for weight in weights],
        [weight.swapaxes(1, 2) for weight in weights],
        flops=1,
        moved=1,
        limit=6 * MIB,
    )


def expert_kernel(experts, *refs):
    *row_refs, gate_ref, up_ref, down_ref, mine_ref, other_ref = refs
    local_experts, _, width = down_ref.shape
    rows = jnp.concatenate([ref[:, :width] for ref in row_refs], axis=0)
    table = jnp.concatenate([ref[:, width:] for ref in row_refs], axis=0).astype(jnp.float32)
    column = lax.broadcasted_iota(jnp.int32, table.shape, 1)
    total = None
    for local in range(local_experts):
        expert = lax.axis_index("expert") * local_experts + local
        chosen = (column == expert) | (column == expert + experts)
        weight = jnp.sum(jnp.where(chosen, table, 0.0), axis=1, keepdims=True)
        gate = mm(rows, gate_ref[local])
        up = mm(rows, up_ref[local])
        active = (gate * jax.nn.sigmoid(GLU_SLOPE * gate) * (up + 1.0)).astype(jnp.bfloat16)
        part = mm(active, down_ref[local])
        part = part * weight
        total = part if total is None else total + part
    half = mine_ref.shape[0]
    mine_ref[...] = total[:half]
    other_ref[...] = total[half:].astype(jnp.bfloat16)


def split_kernel(mine_ref, received_ref, kept_ref, *sent_refs):
    size = kept_ref.shape[0]
    kept_ref[...] = mine_ref[:size] + received_ref[:size].astype(jnp.float32)
    for number, sent_ref in enumerate(sent_refs, 1):
        block = pl.ds(number * size, size)
        total = mine_ref[block] + received_ref[block].astype(jnp.float32)
        sent_ref[...] = total.astype(jnp.bfloat16)


def return_kernel(received, residual_ref, *refs):
    kept_ref, *received_refs = refs[: 1 + received]
    base_ref, *sent_refs = refs[1 + received :]
    total = kept_ref[...]
    for received_ref in received_refs:
        total = total + received_ref[...].astype(jnp.float32)
    width = base_ref.shape[1]
    rank = lax.axis_index("tensor")

    def slab_of(values, owner):
        slab = values[:, :width]
        for number in range(1, values.shape[1] // width):
            piece = values[:, number * width : (number + 1) * width]
            slab = jnp.where(owner == number, piece, slab)
        return slab

    base_ref[...] = slab_of(total + residual_ref[...], rank)
    for step, sent_ref in enumerate(sent_refs, 1):
        sent_ref[...] = slab_of(total, rank ^ step).astype(jnp.bfloat16)


def per_device(
    hidden_in,
    queries,
    new_keys,
    new_values,
    cache_keys,
    cache_values,
    cache_lengths,
    out_weight,
    norm_gain,
    expert_ids,
    route_probs,
    route_order,
    gate_weight,
    up_weight,
    down_weight,
):
    sequences, width = hidden_in.shape
    expert_ranks = lax.axis_size("expert")
    tensor_ranks = lax.axis_size("tensor")
    local_experts, hidden_units = down_weight.shape[:2]
    experts = local_experts * expert_ranks
    inner = 2
    outer = expert_ranks // inner
    row_width = -(-(width + 2 * experts) // 128) * 128

    def to_outer(values, step):
        pairs = [(rank, rank ^ (step * inner)) for rank in range(expert_ranks)]
        return lax.ppermute(values, "expert", pairs)

    def to_inner(values):
        return lax.ppermute(values, "expert", [(rank, rank ^ 1) for rank in range(expert_ranks)])

    operands = (queries, new_keys, new_values, cache_keys, cache_values, cache_lengths)
    if queries.shape[1] % 16 == 0:
        mine, sent = attend_and_project(*operands, out_weight)
    else:
        mine = jnp.dot(attend(*operands), out_weight, preferred_element_type=jnp.float32)
        sent = mine.astype(jnp.bfloat16)
    mine, received = exchange(mine, sent, "tensor", tensor_ranks)

    weights = route_weights(expert_ids, route_probs, route_order, experts)
    high = weights.astype(jnp.bfloat16)
    low = (weights - high.astype(jnp.float32)).astype(jnp.bfloat16)
    spare = jnp.zeros((sequences, row_width - width - 2 * experts), jnp.bfloat16)
    table = jnp.concatenate([high, low, spare], axis=1)

    block = (sequences, width)
    residual, rows = call(
        norm_kernel,
        [(block, jnp.float32), ((sequences, row_width), jnp.bfloat16)],
        (mine, received, hidden_in, norm_gain.reshape(1, width), table),
        flops=WINDOW_FLOPS,
        moved=sequences * width * 16,
        limit=2 * MIB,
    )

    near = [rows]
    for step in range(1, outer):
        near.append(to_outer(rows, step))
    gate_weight, up_weight = turn(gate_weight, up_weight)
    (near,) = call(
        pack_kernel,
        [((outer * sequences, row_width), jnp.bfloat16)],
        near,
        flops=sequences,
        moved=4 * outer * sequences * row_width,
        limit=2 * MIB,
    )
    far = to_inner(near)
    half = (outer * sequences, width)
    mine, other = call(
        functools.partial(expert_kernel, experts),
        [(half, jnp.float32), (half, jnp.bfloat16)],
        (near, far, gate_weight, up_weight, down_weight),
        flops=12 * half[0] * width * hidden_units * local_experts,
        moved=6 * width * hidden_units * local_experts,
        limit=16 * MIB,
    )
    received = to_inner(other)
    kept, *sent = call(
        split_kernel,
        [(block, jnp.float32)] + [(block, jnp.bfloat16)] * (outer - 1),
        (mine, received),
        flops=half[0] * width,
        moved=half[0] * width * 8,
        limit=4 * MIB,
    )
    returned = []
    for step, piece in enumerate(sent, 1):
        returned.append(to_outer(piece, step))
    slab = (sequences, width // tensor_ranks)
    total, *sent = call(
        functools.partial(return_kernel, len(returned)),
        [(slab, jnp.float32)] + [(slab, jnp.bfloat16)] * (tensor_ranks - 1),
        (residual, kept, *returned),
        flops=half[0] * width,
        moved=half[0] * width * 2,
        limit=2 * MIB,
    )
    for step, piece in enumerate(sent, 1):
        pairs = [(rank, rank ^ step) for rank in range(tensor_ranks)]
        total = total + lax.ppermute(piece, "tensor", pairs).astype(jnp.float32)
    return total.astype(jnp.bfloat16)


def solution(mesh):
    in_specs = (
        P(("groups", "expert"), None),
        P(("groups", "expert"), "tensor", None),
        P(("groups", "expert"), "tensor", None),
        P(("groups", "expert"), "tensor", None),
        P(("groups", "expert"), "tensor", None, None),
        P(("groups", "expert"), "tensor", None, None),
        P(("groups", "expert")),
        P("tensor", None),
        P(),
        P(("groups", "expert"), None),
        P(("groups", "expert"), None),
        P(("groups", "expert"), None),
        P("expert", None, "tensor"),
        P("expert", None, "tensor"),
        P("expert", "tensor", None),
    )
    out_specs = P(("groups", "expert"), "tensor")

    return jax.shard_map(
        per_device, mesh=mesh, in_specs=in_specs, out_specs=out_specs, check_vma=False
    )
```

```python
import functools

import jax
import jax.numpy as jnp
from jax import lax
from jax.experimental import pallas as pl
from jax.experimental.pallas import tpu as pltpu
from jax.sharding import PartitionSpec as P

EPSILON = 1e-05
GLU_SLOPE = 1.702
WINDOW_FLOPS = 50_000_000_000


def attend(queries, new_keys, new_values, cache_keys, cache_values, cache_lengths):
    sequence_count, head_count, head_dim = queries.shape
    kv_heads = new_keys.shape[1]
    group_size = head_count // kv_heads
    scaling = 1.0 / head_dim**0.5
    query_rows = queries.reshape(sequence_count, kv_heads, group_size, head_dim)
    scores = (
        jnp.einsum("sgqd,sgdc->sgqc", query_rows, cache_keys, preferred_element_type=jnp.float32)
        * scaling
    )
    own_score = (
        jnp.einsum("sgqd,sgd->sgq", query_rows, new_keys, preferred_element_type=jnp.float32)
        * scaling
    )
    positions = jnp.arange(cache_keys.shape[3], dtype=jnp.int32)
    visible = positions[None, :] < cache_lengths[:, None]
    scores = jnp.where(visible[:, None, None, :], scores, -1e30)
    highest = jnp.maximum(jnp.max(scores, axis=3), own_score)
    cache_exp = jnp.exp(scores - highest[..., None])
    own_exp = jnp.exp(own_score - highest)
    totals = jnp.sum(cache_exp, axis=3) + own_exp
    cache_prob = (cache_exp / totals[..., None]).astype(jnp.bfloat16)
    own_prob = (own_exp / totals).astype(jnp.bfloat16)
    attended = jnp.einsum(
        "sgqc,sgdc->sgqd", cache_prob, cache_values, preferred_element_type=jnp.float32
    )
    attended = (
        attended
        + own_prob.astype(jnp.float32)[..., None] * new_values.astype(jnp.float32)[:, :, None, :]
    )
    return attended.astype(jnp.bfloat16).reshape(sequence_count, head_count * head_dim)


VMEM = pl.BlockSpec(memory_space=pltpu.VMEM)
LAST_DIMS = (((1,), (1,)), ((), ()))
MIB = 1 << 20


def call(kernel, outs, args, flops, moved, limit):
    return pl.pallas_call(
        kernel,
        out_shape=[jax.ShapeDtypeStruct(shape, dtype) for shape, dtype in outs],
        in_specs=[VMEM] * len(args),
        out_specs=[VMEM] * len(outs),
        compiler_params=pltpu.CompilerParams(vmem_limit_bytes=limit),
        cost_estimate=pl.CostEstimate(flops=flops, bytes_accessed=moved, transcendentals=0),
    )(*args)


def mm(left, right, dims=(((1,), (0,)), ((), ()))):
    return lax.dot_general(left, right, dims, preferred_element_type=jnp.float32)


def iota(shape, dim):
    return lax.broadcasted_iota(jnp.int32, shape, dim)


def attend_kernel(
    pieces,
    lengths_hbm,
    queries_hbm,
    new_keys_hbm,
    new_values_hbm,
    keys_hbm,
    values_hbm,
    weight_hbm,
    mine_ref,
    sent_ref,
    lengths_ref,
    queries_ref,
    new_keys_ref,
    new_values_ref,
    keys_ref,
    values_ref,
    weight_ref,
    own_keys_ref,
    own_values_ref,
    attended_ref,
    arrived,
):
    sequences, heads, head_dim = queries_ref.shape
    kv_heads = new_keys_ref.shape[1]
    group = heads // kv_heads
    span = kv_heads * head_dim
    lanes = group * head_dim
    moves = (
        (lengths_hbm, lengths_ref),
        (queries_hbm, queries_ref),
        (new_keys_hbm, new_keys_ref),
        (new_values_hbm, new_values_ref),
        (keys_hbm, keys_ref),
        (values_hbm, values_ref),
        *((weight_hbm.at[pl.ds(*piece)], weight_ref.at[pl.ds(*piece)]) for piece in pieces),
    )
    copies = [
        pltpu.make_async_copy(source, target, arrived.at[number])
        for number, (source, target) in enumerate(moves)
    ]
    for copy in copies:
        copy.start()

    rows = sequences * heads
    scaling = 1.0 / head_dim**0.5
    for copy in copies[:4]:
        copy.wait()
    queries = queries_ref[...].reshape(rows, head_dim)
    for sequence in range(sequences):
        block = pl.ds(sequence * kv_heads, kv_heads)
        own_keys_ref[block] = new_keys_ref[sequence].astype(jnp.float32)
        own_values_ref[block] = new_values_ref[sequence].astype(jnp.float32)
    own_keys = own_keys_ref[...].astype(jnp.bfloat16)
    own_values = own_values_ref[...].astype(jnp.bfloat16)

    spread = (iota((head_dim, span), 0) == iota((head_dim, span), 1) % head_dim).astype(
        jnp.bfloat16
    )
    same_head = iota((rows, span), 1) // head_dim == iota((rows, span), 0) % heads // group
    wide = jnp.where(same_head, mm(queries, spread), 0.0).astype(jnp.bfloat16)
    pairs = (rows, sequences * kv_heads)
    own_pair = iota(pairs, 1) == iota(pairs, 0) // group
    own_score = (
        jnp.sum(jnp.where(own_pair, mm(queries, own_keys, LAST_DIMS), 0.0), axis=1, keepdims=True)
        * scaling
    )

    copies[4].wait()
    slots = keys_ref.shape[2]
    scores = []
    for sequence in range(sequences):
        block = slice(sequence * heads, (sequence + 1) * heads)
        score = mm(wide[block], keys_ref[sequence]) * scaling
        visible = iota((heads, slots), 1) < lengths_ref[sequence]
        scores.append(jnp.where(visible, score, -1e30))
    scores = jnp.concatenate(scores, axis=0)
    highest = jnp.maximum(jnp.max(scores, axis=1, keepdims=True), own_score)
    cache_exp = jnp.exp(scores - highest)
    own_exp = jnp.exp(own_score - highest)
    totals = jnp.sum(cache_exp, axis=1, keepdims=True) + own_exp
    cache_prob = (cache_exp / totals).astype(jnp.bfloat16)
    own_prob = own_exp / totals
    own_prob = jnp.where(own_pair, own_prob, 0.0).astype(jnp.bfloat16)
    own_part = mm(own_prob, mm(own_values, spread).astype(jnp.bfloat16))

    copies[5].wait()
    attended = [
        mm(
            cache_prob[sequence * heads : (sequence + 1) * heads],
            values_ref[sequence],
            LAST_DIMS,
        )
        for sequence in range(sequences)
    ]
    attended = jnp.concatenate(attended, axis=0) + own_part
    attended = jnp.where(same_head, attended, 0.0).astype(jnp.bfloat16)
    repeat = (iota((span, lanes), 0) % head_dim == iota((span, lanes), 1) % head_dim).astype(
        jnp.bfloat16
    )
    own_lanes = iota((rows, lanes), 1) // head_dim == iota((rows, lanes), 0) % group
    placed = jnp.where(own_lanes, mm(attended, repeat), 0.0).astype(jnp.bfloat16)
    sums = (kv_heads * sequences, rows)
    chosen = (iota(sums, 0) % sequences == iota(sums, 1) // heads) & (
        iota(sums, 0) // sequences == iota(sums, 1) % heads // group
    )
    by_head = mm(chosen.astype(jnp.bfloat16), placed)
    for head in range(kv_heads):
        attended_ref[:, head * lanes : (head + 1) * lanes] = by_head[
            head * sequences : (head + 1) * sequences
        ].astype(jnp.bfloat16)
    attended = attended_ref[...]

    for copy, (start, size) in zip(copies[6:], pieces):
        copy.wait()
        part = mm(attended, weight_ref[pl.ds(start, size)], LAST_DIMS)
        mine_ref[:, start : start + size] = part
        sent_ref[:, start : start + size] = part.astype(jnp.bfloat16)


def attend_and_project(
    queries, new_keys, new_values, cache_keys, cache_values, cache_lengths, out_weight
):
    sequences, heads, head_dim = queries.shape
    kv_heads, slots = cache_keys.shape[1], cache_keys.shape[3]
    depth, width = out_weight.shape
    span = kv_heads * head_dim
    caches = (sequences, span, slots)
    hbm = pl.BlockSpec(memory_space=pltpu.HBM)
    arrays = (
        cache_lengths,
        queries,
        new_keys,
        new_values,
        cache_keys.reshape(caches),
        cache_values.reshape(caches),
        out_weight.T,
    )
    first = -(-width // 512) * 256
    pieces = ((0, first), (first, width - first))
    return pl.pallas_call(
        functools.partial(attend_kernel, pieces),
        out_shape=[
            jax.ShapeDtypeStruct((sequences, width), jnp.float32),
            jax.ShapeDtypeStruct((sequences, width), jnp.bfloat16),
        ],
        in_specs=[hbm] * len(arrays),
        out_specs=[VMEM] * 2,
        scratch_shapes=[pltpu.SMEM(cache_lengths.shape, cache_lengths.dtype)]
        + [pltpu.VMEM(array.shape, array.dtype) for array in arrays[1:]]
        + [
            pltpu.VMEM((sequences * kv_heads, head_dim), jnp.float32),
            pltpu.VMEM((sequences * kv_heads, head_dim), jnp.float32),
            pltpu.VMEM((sequences, depth), jnp.bfloat16),
            pltpu.SemaphoreType.DMA((len(arrays) - 1 + len(pieces),)),
        ],
        compiler_params=pltpu.CompilerParams(vmem_limit_bytes=53 * MIB),
        cost_estimate=pl.CostEstimate(
            flops=2 * sequences * width * depth,
            bytes_accessed=2 * (width * depth + 2 * sequences * span * slots),
            transcendentals=sequences * heads * slots,
        ),
    )(*[pltpu.with_memory_space_constraint(array, pltpu.HBM) for array in arrays])


def route_weights(expert_ids, route_probs, route_order, experts):
    picked = jnp.zeros(expert_ids.shape, jnp.float32)
    for column in range(expert_ids.shape[1]):
        picked = picked + jnp.where(route_order == column, route_probs[:, column : column + 1], 0.0)
    weights = picked / jnp.sum(route_probs, axis=1, keepdims=True)
    named = expert_ids[:, :, None] == jnp.arange(experts, dtype=jnp.int32)[None, None, :]
    return jnp.sum(jnp.where(named, weights[:, :, None], 0.0), axis=1)


def exchange(values, sent, axis, ranks):
    step = 1
    while True:
        pairs = [(rank, rank ^ step) for rank in range(ranks)]
        received = lax.ppermute(sent, axis, pairs)
        step *= 2
        if step >= ranks:
            return values, received
        values = values + received.astype(jnp.float32)
        sent = values.astype(jnp.bfloat16)


def table_kernel(weights_ref, table_ref):
    experts = weights_ref.shape[1]
    weights = weights_ref[...]
    high = weights.astype(jnp.bfloat16)
    low = (weights - high.astype(jnp.float32)).astype(jnp.bfloat16)
    table_ref[...] = jnp.zeros_like(table_ref)
    table_ref[:, :experts] = high
    table_ref[:, experts : 2 * experts] = low


def norm_kernel(mine_ref, received_ref, hidden_ref, gain_ref, table_ref, residual_ref, rows_ref):
    width = hidden_ref.shape[1]
    residual = (
        hidden_ref[...].astype(jnp.float32) + mine_ref[...] + received_ref[...].astype(jnp.float32)
    )
    residual_ref[...] = residual
    mean_square = jnp.mean(residual * residual, axis=1, keepdims=True)
    normed = residual * lax.rsqrt(mean_square + EPSILON) * gain_ref[...]
    rows_ref[:, :width] = normed.astype(jnp.bfloat16)
    rows_ref[:, width:] = table_ref[...]


def pack_kernel(*refs):
    *piece_refs, packed_ref = refs
    size = piece_refs[0].shape[0]
    for number, piece_ref in enumerate(piece_refs):
        packed_ref[pl.ds(number * size, size)] = piece_ref[...]


def turn_kernel(*refs):
    for source_ref, target_ref in zip(refs[: len(refs) // 2], refs[len(refs) // 2 :]):
        for local in range(source_ref.shape[0]):
            target_ref[local] = source_ref[local].T


def turn(*weights):
    return call(
        turn_kernel,
        [(weight.shape, weight.dtype) for weight in weights],
        [weight.swapaxes(1, 2) for weight in weights],
        flops=1,
        moved=1,
        limit=6 * MIB,
    )


def expert_kernel(experts, *refs):
    *row_refs, gate_ref, up_ref, down_ref, mine_ref, other_ref = refs
    local_experts, _, width = down_ref.shape
    rows = jnp.concatenate([ref[:, :width] for ref in row_refs], axis=0)
    table = jnp.concatenate([ref[:, width:] for ref in row_refs], axis=0).astype(jnp.float32)
    column = lax.broadcasted_iota(jnp.int32, table.shape, 1)
    total = None
    for local in range(local_experts):
        expert = lax.axis_index("expert") * local_experts + local
        chosen = (column == expert) | (column == expert + experts)
        weight = jnp.sum(jnp.where(chosen, table, 0.0), axis=1, keepdims=True)
        gate = mm(rows, gate_ref[local])
        up = mm(rows, up_ref[local])
        active = (gate * jax.nn.sigmoid(GLU_SLOPE * gate) * (up + 1.0)).astype(jnp.bfloat16)
        part = mm(active, down_ref[local])
        part = part * weight
        total = part if total is None else total + part
    half = mine_ref.shape[0]
    mine_ref[...] = total[:half]
    other_ref[...] = total[half:].astype(jnp.bfloat16)


def split_kernel(mine_ref, received_ref, kept_ref, *sent_refs):
    size = kept_ref.shape[0]
    kept_ref[...] = mine_ref[:size] + received_ref[:size].astype(jnp.float32)
    for number, sent_ref in enumerate(sent_refs, 1):
        block = pl.ds(number * size, size)
        total = mine_ref[block] + received_ref[block].astype(jnp.float32)
        sent_ref[...] = total.astype(jnp.bfloat16)


def return_kernel(received, residual_ref, *refs):
    kept_ref, *received_refs = refs[: 1 + received]
    base_ref, *sent_refs = refs[1 + received :]
    total = kept_ref[...]
    for received_ref in received_refs:
        total = total + received_ref[...].astype(jnp.float32)
    width = base_ref.shape[1]
    rank = lax.axis_index("tensor")

    def slab_of(values, owner):
        slab = values[:, :width]
        for number in range(1, values.shape[1] // width):
            piece = values[:, number * width : (number + 1) * width]
            slab = jnp.where(owner == number, piece, slab)
        return slab

    base_ref[...] = slab_of(total + residual_ref[...], rank)
    for step, sent_ref in enumerate(sent_refs, 1):
        sent_ref[...] = slab_of(total, rank ^ step).astype(jnp.bfloat16)


def per_device(
    hidden_in,
    queries,
    new_keys,
    new_values,
    cache_keys,
    cache_values,
    cache_lengths,
    out_weight,
    norm_gain,
    expert_ids,
    route_probs,
    route_order,
    gate_weight,
    up_weight,
    down_weight,
):
    sequences, width = hidden_in.shape
    expert_ranks = lax.axis_size("expert")
    tensor_ranks = lax.axis_size("tensor")
    local_experts, hidden_units = down_weight.shape[:2]
    experts = local_experts * expert_ranks
    inner = 2
    outer = expert_ranks // inner
    row_width = -(-(width + 2 * experts) // 128) * 128

    def to_outer(values, step):
        pairs = [(rank, rank ^ (step * inner)) for rank in range(expert_ranks)]
        return lax.ppermute(values, "expert", pairs)

    def to_inner(values):
        return lax.ppermute(values, "expert", [(rank, rank ^ 1) for rank in range(expert_ranks)])

    operands = (queries, new_keys, new_values, cache_keys, cache_values, cache_lengths)
    if queries.shape[1] % 16 == 0:
        mine, sent = attend_and_project(*operands, out_weight)
    else:
        mine = jnp.dot(attend(*operands), out_weight, preferred_element_type=jnp.float32)
        sent = mine.astype(jnp.bfloat16)
    mine, received = exchange(mine, sent, "tensor", tensor_ranks)

    weights = route_weights(expert_ids, route_probs, route_order, experts)
    (table,) = call(
        table_kernel,
        [((sequences, row_width - width), jnp.bfloat16)],
        (weights,),
        flops=WINDOW_FLOPS,
        moved=sequences * row_width,
        limit=MIB,
    )

    block = (sequences, width)
    residual, rows = call(
        norm_kernel,
        [(block, jnp.float32), ((sequences, row_width), jnp.bfloat16)],
        (mine, received, hidden_in, norm_gain.reshape(1, width), table),
        flops=16 * sequences * width,
        moved=sequences * width * 16,
        limit=2 * MIB,
    )

    near = [rows]
    for step in range(1, outer):
        near.append(to_outer(rows, step))
    gate_weight, up_weight = turn(gate_weight, up_weight)
    (near,) = call(
        pack_kernel,
        [((outer * sequences, row_width), jnp.bfloat16)],
        near,
        flops=sequences,
        moved=4 * outer * sequences * row_width,
        limit=2 * MIB,
    )
    far = to_inner(near)
    half = (outer * sequences, width)
    mine, other = call(
        functools.partial(expert_kernel, experts),
        [(half, jnp.float32), (half, jnp.bfloat16)],
        (near, far, gate_weight, up_weight, down_weight),
        flops=12 * half[0] * width * hidden_units * local_experts,
        moved=6 * width * hidden_units * local_experts,
        limit=16 * MIB,
    )
    received = to_inner(other)
    kept, *sent = call(
        split_kernel,
        [(block, jnp.float32)] + [(block, jnp.bfloat16)] * (outer - 1),
        (mine, received),
        flops=half[0] * width,
        moved=half[0] * width * 8,
        limit=4 * MIB,
    )
    returned = []
    for step, piece in enumerate(sent, 1):
        returned.append(to_outer(piece, step))
    slab = (sequences, width // tensor_ranks)
    total, *sent = call(
        functools.partial(return_kernel, len(returned)),
        [(slab, jnp.float32)] + [(slab, jnp.bfloat16)] * (tensor_ranks - 1),
        (residual, kept, *returned),
        flops=half[0] * width,
        moved=half[0] * width * 2,
        limit=2 * MIB,
    )
    for step, piece in enumerate(sent, 1):
        pairs = [(rank, rank ^ step) for rank in range(tensor_ranks)]
        total = total + lax.ppermute(piece, "tensor", pairs).astype(jnp.float32)
    return total.astype(jnp.bfloat16)


def solution(mesh):
    in_specs = (
        P(("groups", "expert"), None),
        P(("groups", "expert"), "tensor", None),
        P(("groups", "expert"), "tensor", None),
        P(("groups", "expert"), "tensor", None),
        P(("groups", "expert"), "tensor", None, None),
        P(("groups", "expert"), "tensor", None, None),
        P(("groups", "expert")),
        P("tensor", None),
        P(),
        P(("groups", "expert"), None),
        P(("groups", "expert"), None),
        P(("groups", "expert"), None),
        P("expert", None, "tensor"),
        P("expert", None, "tensor"),
        P("expert", "tensor", None),
    )
    out_specs = P(("groups", "expert"), "tensor")

    return jax.shard_map(
        per_device, mesh=mesh, in_specs=in_specs, out_specs=out_specs, check_vma=False
    )
```

```python
import functools

import jax
import jax.numpy as jnp
from jax import lax
from jax.experimental import pallas as pl
from jax.experimental.pallas import tpu as pltpu
from jax.sharding import PartitionSpec as P

EPSILON = 1e-05
GLU_SLOPE = 1.702
WINDOW_FLOPS = 50_000_000_000


def attend(queries, new_keys, new_values, cache_keys, cache_values, cache_lengths):
    sequence_count, head_count, head_dim = queries.shape
    kv_heads = new_keys.shape[1]
    group_size = head_count // kv_heads
    scaling = 1.0 / head_dim**0.5
    query_rows = queries.reshape(sequence_count, kv_heads, group_size, head_dim)
    scores = (
        jnp.einsum("sgqd,sgdc->sgqc", query_rows, cache_keys, preferred_element_type=jnp.float32)
        * scaling
    )
    own_score = (
        jnp.einsum("sgqd,sgd->sgq", query_rows, new_keys, preferred_element_type=jnp.float32)
        * scaling
    )
    positions = jnp.arange(cache_keys.shape[3], dtype=jnp.int32)
    visible = positions[None, :] < cache_lengths[:, None]
    scores = jnp.where(visible[:, None, None, :], scores, -1e30)
    highest = jnp.maximum(jnp.max(scores, axis=3), own_score)
    cache_exp = jnp.exp(scores - highest[..., None])
    own_exp = jnp.exp(own_score - highest)
    totals = jnp.sum(cache_exp, axis=3) + own_exp
    cache_prob = (cache_exp / totals[..., None]).astype(jnp.bfloat16)
    own_prob = (own_exp / totals).astype(jnp.bfloat16)
    attended = jnp.einsum(
        "sgqc,sgdc->sgqd", cache_prob, cache_values, preferred_element_type=jnp.float32
    )
    attended = (
        attended
        + own_prob.astype(jnp.float32)[..., None] * new_values.astype(jnp.float32)[:, :, None, :]
    )
    return attended.astype(jnp.bfloat16).reshape(sequence_count, head_count * head_dim)


VMEM = pl.BlockSpec(memory_space=pltpu.VMEM)
LAST_DIMS = (((1,), (1,)), ((), ()))
MIB = 1 << 20


def call(kernel, outs, args, flops, moved, limit):
    return pl.pallas_call(
        kernel,
        out_shape=[jax.ShapeDtypeStruct(shape, dtype) for shape, dtype in outs],
        in_specs=[VMEM] * len(args),
        out_specs=[VMEM] * len(outs),
        compiler_params=pltpu.CompilerParams(vmem_limit_bytes=limit),
        cost_estimate=pl.CostEstimate(flops=flops, bytes_accessed=moved, transcendentals=0),
    )(*args)


def mm(left, right, dims=(((1,), (0,)), ((), ()))):
    return lax.dot_general(left, right, dims, preferred_element_type=jnp.float32)


def iota(shape, dim):
    return lax.broadcasted_iota(jnp.int32, shape, dim)


def attend_kernel(
    pieces,
    lengths_hbm,
    queries_hbm,
    new_keys_hbm,
    new_values_hbm,
    keys_hbm,
    values_hbm,
    weight_hbm,
    mine_ref,
    sent_ref,
    lengths_ref,
    queries_ref,
    new_keys_ref,
    new_values_ref,
    keys_ref,
    values_ref,
    weight_ref,
    own_keys_ref,
    own_values_ref,
    attended_ref,
    arrived,
):
    sequences, heads, head_dim = queries_ref.shape
    kv_heads = new_keys_ref.shape[1]
    group = heads // kv_heads
    span = kv_heads * head_dim
    lanes = group * head_dim
    moves = (
        (lengths_hbm, lengths_ref),
        (queries_hbm, queries_ref),
        (new_keys_hbm, new_keys_ref),
        (new_values_hbm, new_values_ref),
        (keys_hbm, keys_ref),
        (values_hbm, values_ref),
        *((weight_hbm.at[pl.ds(*piece)], weight_ref.at[pl.ds(*piece)]) for piece in pieces),
    )
    copies = [
        pltpu.make_async_copy(source, target, arrived.at[number])
        for number, (source, target) in enumerate(moves)
    ]
    for copy in copies:
        copy.start()

    rows = sequences * heads
    scaling = 1.0 / head_dim**0.5
    for copy in copies[:4]:
        copy.wait()
    queries = queries_ref[...].reshape(rows, head_dim)
    for sequence in range(sequences):
        block = pl.ds(sequence * kv_heads, kv_heads)
        own_keys_ref[block] = new_keys_ref[sequence].astype(jnp.float32)
        own_values_ref[block] = new_values_ref[sequence].astype(jnp.float32)
    own_keys = own_keys_ref[...].astype(jnp.bfloat16)
    own_values = own_values_ref[...].astype(jnp.bfloat16)

    spread = (iota((head_dim, span), 0) == iota((head_dim, span), 1) % head_dim).astype(
        jnp.bfloat16
    )
    same_head = iota((rows, span), 1) // head_dim == iota((rows, span), 0) % heads // group
    wide = jnp.where(same_head, mm(queries, spread), 0.0).astype(jnp.bfloat16)
    pairs = (rows, sequences * kv_heads)
    own_pair = iota(pairs, 1) == iota(pairs, 0) // group
    own_score = (
        jnp.sum(jnp.where(own_pair, mm(queries, own_keys, LAST_DIMS), 0.0), axis=1, keepdims=True)
        * scaling
    )

    copies[4].wait()
    slots = keys_ref.shape[2]
    scores = []
    for sequence in range(sequences):
        block = slice(sequence * heads, (sequence + 1) * heads)
        score = mm(wide[block], keys_ref[sequence]) * scaling
        visible = iota((heads, slots), 1) < lengths_ref[sequence]
        scores.append(jnp.where(visible, score, -1e30))
    scores = jnp.concatenate(scores, axis=0)
    highest = jnp.maximum(jnp.max(scores, axis=1, keepdims=True), own_score)
    cache_exp = jnp.exp(scores - highest)
    own_exp = jnp.exp(own_score - highest)
    totals = jnp.sum(cache_exp, axis=1, keepdims=True) + own_exp
    cache_prob = (cache_exp / totals).astype(jnp.bfloat16)
    own_prob = own_exp / totals
    own_prob = jnp.where(own_pair, own_prob, 0.0).astype(jnp.bfloat16)
    own_part = mm(own_prob, mm(own_values, spread).astype(jnp.bfloat16))

    copies[5].wait()
    attended = [
        mm(
            cache_prob[sequence * heads : (sequence + 1) * heads],
            values_ref[sequence],
            LAST_DIMS,
        )
        for sequence in range(sequences)
    ]
    attended = jnp.concatenate(attended, axis=0) + own_part
    attended = jnp.where(same_head, attended, 0.0).astype(jnp.bfloat16)
    repeat = (iota((span, lanes), 0) % head_dim == iota((span, lanes), 1) % head_dim).astype(
        jnp.bfloat16
    )
    own_lanes = iota((rows, lanes), 1) // head_dim == iota((rows, lanes), 0) % group
    placed = jnp.where(own_lanes, mm(attended, repeat), 0.0).astype(jnp.bfloat16)
    sums = (kv_heads * sequences, rows)
    chosen = (iota(sums, 0) % sequences == iota(sums, 1) // heads) & (
        iota(sums, 0) // sequences == iota(sums, 1) % heads // group
    )
    by_head = mm(chosen.astype(jnp.bfloat16), placed)
    for head in range(kv_heads):
        attended_ref[:, head * lanes : (head + 1) * lanes] = by_head[
            head * sequences : (head + 1) * sequences
        ].astype(jnp.bfloat16)
    attended = attended_ref[...]

    for copy, (start, size) in zip(copies[6:], pieces):
        copy.wait()
        part = mm(attended, weight_ref[pl.ds(start, size)], LAST_DIMS)
        mine_ref[:, start : start + size] = part
        sent_ref[:, start : start + size] = part.astype(jnp.bfloat16)


def attend_and_project(
    queries, new_keys, new_values, cache_keys, cache_values, cache_lengths, out_weight
):
    sequences, heads, head_dim = queries.shape
    kv_heads, slots = cache_keys.shape[1], cache_keys.shape[3]
    depth, width = out_weight.shape
    span = kv_heads * head_dim
    caches = (sequences, span, slots)
    hbm = pl.BlockSpec(memory_space=pltpu.HBM)
    arrays = (
        cache_lengths,
        queries,
        new_keys,
        new_values,
        cache_keys.reshape(caches),
        cache_values.reshape(caches),
        out_weight.T,
    )
    first = -(-width // 512) * 256
    pieces = ((0, first), (first, width - first))
    return pl.pallas_call(
        functools.partial(attend_kernel, pieces),
        out_shape=[
            jax.ShapeDtypeStruct((sequences, width), jnp.float32),
            jax.ShapeDtypeStruct((sequences, width), jnp.bfloat16),
        ],
        in_specs=[hbm] * len(arrays),
        out_specs=[VMEM] * 2,
        scratch_shapes=[pltpu.SMEM(cache_lengths.shape, cache_lengths.dtype)]
        + [pltpu.VMEM(array.shape, array.dtype) for array in arrays[1:]]
        + [
            pltpu.VMEM((sequences * kv_heads, head_dim), jnp.float32),
            pltpu.VMEM((sequences * kv_heads, head_dim), jnp.float32),
            pltpu.VMEM((sequences, depth), jnp.bfloat16),
            pltpu.SemaphoreType.DMA((len(arrays) - 1 + len(pieces),)),
        ],
        compiler_params=pltpu.CompilerParams(vmem_limit_bytes=53 * MIB),
        cost_estimate=pl.CostEstimate(
            flops=2 * sequences * width * depth,
            bytes_accessed=2 * (width * depth + 2 * sequences * span * slots),
            transcendentals=sequences * heads * slots,
        ),
    )(*[pltpu.with_memory_space_constraint(array, pltpu.HBM) for array in arrays])


def route_weights(expert_ids, route_probs, route_order, experts):
    picked = jnp.zeros(expert_ids.shape, jnp.float32)
    for column in range(expert_ids.shape[1]):
        picked = picked + jnp.where(route_order == column, route_probs[:, column : column + 1], 0.0)
    weights = picked / jnp.sum(route_probs, axis=1, keepdims=True)
    named = expert_ids[:, :, None] == jnp.arange(experts, dtype=jnp.int32)[None, None, :]
    return jnp.sum(jnp.where(named, weights[:, :, None], 0.0), axis=1)


def exchange(values, sent, axis, ranks):
    step = 1
    while True:
        pairs = [(rank, rank ^ step) for rank in range(ranks)]
        received = lax.ppermute(sent, axis, pairs)
        step *= 2
        if step >= ranks:
            return values, received
        values = values + received.astype(jnp.float32)
        sent = values.astype(jnp.bfloat16)


def table_kernel(weights_ref, table_ref):
    experts = weights_ref.shape[1]
    weights = weights_ref[...]
    high = weights.astype(jnp.bfloat16)
    low = (weights - high.astype(jnp.float32)).astype(jnp.bfloat16)
    table_ref[...] = jnp.zeros_like(table_ref)
    table_ref[:, :experts] = high
    table_ref[:, experts : 2 * experts] = low


def norm_kernel(mine_ref, received_ref, hidden_ref, gain_ref, table_ref, residual_ref, rows_ref):
    width = hidden_ref.shape[1]
    residual = (
        hidden_ref[...].astype(jnp.float32) + mine_ref[...] + received_ref[...].astype(jnp.float32)
    )
    residual_ref[...] = residual
    mean_square = jnp.mean(residual * residual, axis=1, keepdims=True)
    normed = residual * lax.rsqrt(mean_square + EPSILON) * gain_ref[...]
    rows_ref[:, :width] = normed.astype(jnp.bfloat16)
    rows_ref[:, width:] = table_ref[...]


def pack_kernel(*refs):
    *piece_refs, packed_ref = refs
    size = piece_refs[0].shape[0]
    for number, piece_ref in enumerate(piece_refs):
        packed_ref[pl.ds(number * size, size)] = piece_ref[...]


def turn_kernel(pieces, *refs):
    for (start, size), source_ref, target_ref in zip(
        pieces, refs[: len(pieces)], refs[len(pieces) :]
    ):
        for local in range(source_ref.shape[0]):
            target_ref[local] = source_ref[local, pl.ds(start, size)].T


def turn(*sources):
    weights = [weight for weight, _, _ in sources]
    pieces = [(start, size) for _, start, size in sources]
    return call(
        functools.partial(turn_kernel, pieces),
        [(weight.shape[:2] + (size,), weight.dtype) for weight, _, size in sources],
        [weight.swapaxes(1, 2) for weight in weights],
        flops=1,
        moved=1,
        limit=6 * MIB,
    )


def expert_kernel(experts, *refs):
    *row_refs, gate_ref, first_ref, second_ref, down_ref, mine_ref, other_ref = refs
    local_experts, _, width = down_ref.shape
    rows = jnp.concatenate([ref[:, :width] for ref in row_refs], axis=0)
    table = jnp.concatenate([ref[:, width:] for ref in row_refs], axis=0).astype(jnp.float32)
    column = lax.broadcasted_iota(jnp.int32, table.shape, 1)
    total = None
    for local in range(local_experts):
        expert = lax.axis_index("expert") * local_experts + local
        chosen = (column == expert) | (column == expert + experts)
        weight = jnp.sum(jnp.where(chosen, table, 0.0), axis=1, keepdims=True)
        part = None
        start = 0
        for up_ref in (first_ref, second_ref):
            piece = pl.ds(start, up_ref.shape[2])
            gate = mm(rows, gate_ref[local, :, piece])
            up = mm(rows, up_ref[local])
            active = (gate * jax.nn.sigmoid(GLU_SLOPE * gate) * (up + 1.0)).astype(jnp.bfloat16)
            term = mm(active, down_ref[local, piece])
            part = term if part is None else part + term
            start += up_ref.shape[2]
        part = part * weight
        total = part if total is None else total + part
    half = mine_ref.shape[0]
    mine_ref[...] = total[:half]
    other_ref[...] = total[half:].astype(jnp.bfloat16)


def split_kernel(mine_ref, received_ref, kept_ref, *sent_refs):
    size = kept_ref.shape[0]
    kept_ref[...] = mine_ref[:size] + received_ref[:size].astype(jnp.float32)
    for number, sent_ref in enumerate(sent_refs, 1):
        block = pl.ds(number * size, size)
        total = mine_ref[block] + received_ref[block].astype(jnp.float32)
        sent_ref[...] = total.astype(jnp.bfloat16)


def return_kernel(received, residual_ref, *refs):
    kept_ref, *received_refs = refs[: 1 + received]
    base_ref, *sent_refs = refs[1 + received :]
    total = kept_ref[...]
    for received_ref in received_refs:
        total = total + received_ref[...].astype(jnp.float32)
    width = base_ref.shape[1]
    rank = lax.axis_index("tensor")

    def slab_of(values, owner):
        slab = values[:, :width]
        for number in range(1, values.shape[1] // width):
            piece = values[:, number * width : (number + 1) * width]
            slab = jnp.where(owner == number, piece, slab)
        return slab

    base_ref[...] = slab_of(total + residual_ref[...], rank)
    for step, sent_ref in enumerate(sent_refs, 1):
        sent_ref[...] = slab_of(total, rank ^ step).astype(jnp.bfloat16)


def per_device(
    hidden_in,
    queries,
    new_keys,
    new_values,
    cache_keys,
    cache_values,
    cache_lengths,
    out_weight,
    norm_gain,
    expert_ids,
    route_probs,
    route_order,
    gate_weight,
    up_weight,
    down_weight,
):
    sequences, width = hidden_in.shape
    expert_ranks = lax.axis_size("expert")
    tensor_ranks = lax.axis_size("tensor")
    local_experts, hidden_units = down_weight.shape[:2]
    experts = local_experts * expert_ranks
    inner = 2
    outer = expert_ranks // inner
    cut = 3 * hidden_units // 4 // 128 * 128
    row_width = -(-(width + 2 * experts) // 128) * 128

    def to_outer(values, step):
        pairs = [(rank, rank ^ (step * inner)) for rank in range(expert_ranks)]
        return lax.ppermute(values, "expert", pairs)

    def to_inner(values):
        return lax.ppermute(values, "expert", [(rank, rank ^ 1) for rank in range(expert_ranks)])

    operands = (queries, new_keys, new_values, cache_keys, cache_values, cache_lengths)
    if queries.shape[1] % 16 == 0:
        mine, sent = attend_and_project(*operands, out_weight)
    else:
        mine = jnp.dot(attend(*operands), out_weight, preferred_element_type=jnp.float32)
        sent = mine.astype(jnp.bfloat16)
    mine, received = exchange(mine, sent, "tensor", tensor_ranks)

    weights = route_weights(expert_ids, route_probs, route_order, experts)
    (table,) = call(
        table_kernel,
        [((sequences, row_width - width), jnp.bfloat16)],
        (weights,),
        flops=WINDOW_FLOPS,
        moved=sequences * row_width,
        limit=MIB,
    )

    block = (sequences, width)
    residual, rows = call(
        norm_kernel,
        [(block, jnp.float32), ((sequences, row_width), jnp.bfloat16)],
        (mine, received, hidden_in, norm_gain.reshape(1, width), table),
        flops=16 * sequences * width,
        moved=sequences * width * 16,
        limit=2 * MIB,
    )

    near = [rows]
    for step in range(1, outer):
        near.append(to_outer(rows, step))
    gate_turned, up_first = turn((gate_weight, 0, hidden_units), (up_weight, 0, cut))
    (near,) = call(
        pack_kernel,
        [((outer * sequences, row_width), jnp.bfloat16)],
        near,
        flops=sequences,
        moved=4 * outer * sequences * row_width,
        limit=2 * MIB,
    )
    far = to_inner(near)
    (up_second,) = turn((up_weight, cut, hidden_units - cut))
    half = (outer * sequences, width)
    mine, other = call(
        functools.partial(expert_kernel, experts),
        [(half, jnp.float32), (half, jnp.bfloat16)],
        (near, far, gate_turned, up_first, up_second, down_weight),
        flops=12 * half[0] * width * hidden_units * local_experts,
        moved=6 * width * hidden_units * local_experts,
        limit=16 * MIB,
    )
    received = to_inner(other)
    kept, *sent = call(
        split_kernel,
        [(block, jnp.float32)] + [(block, jnp.bfloat16)] * (outer - 1),
        (mine, received),
        flops=half[0] * width,
        moved=half[0] * width * 8,
        limit=4 * MIB,
    )
    returned = []
    for step, piece in enumerate(sent, 1):
        returned.append(to_outer(piece, step))
    slab = (sequences, width // tensor_ranks)
    total, *sent = call(
        functools.partial(return_kernel, len(returned)),
        [(slab, jnp.float32)] + [(slab, jnp.bfloat16)] * (tensor_ranks - 1),
        (residual, kept, *returned),
        flops=half[0] * width,
        moved=half[0] * width * 2,
        limit=2 * MIB,
    )
    for step, piece in enumerate(sent, 1):
        pairs = [(rank, rank ^ step) for rank in range(tensor_ranks)]
        total = total + lax.ppermute(piece, "tensor", pairs).astype(jnp.float32)
    return total.astype(jnp.bfloat16)


def solution(mesh):
    in_specs = (
        P(("groups", "expert"), None),
        P(("groups", "expert"), "tensor", None),
        P(("groups", "expert"), "tensor", None),
        P(("groups", "expert"), "tensor", None),
        P(("groups", "expert"), "tensor", None, None),
        P(("groups", "expert"), "tensor", None, None),
        P(("groups", "expert")),
        P("tensor", None),
        P(),
        P(("groups", "expert"), None),
        P(("groups", "expert"), None),
        P(("groups", "expert"), None),
        P("expert", None, "tensor"),
        P("expert", None, "tensor"),
        P("expert", "tensor", None),
    )
    out_specs = P(("groups", "expert"), "tensor")

    return jax.shard_map(
        per_device, mesh=mesh, in_specs=in_specs, out_specs=out_specs, check_vma=False
    )
```

```python
import functools

import jax
import jax.numpy as jnp
from jax import lax
from jax.experimental import pallas as pl
from jax.experimental.pallas import tpu as pltpu
from jax.sharding import PartitionSpec as P

EPSILON = 1e-05
GLU_SLOPE = 1.702
WINDOW_FLOPS = 50_000_000_000


def attend(queries, new_keys, new_values, cache_keys, cache_values, cache_lengths):
    sequence_count, head_count, head_dim = queries.shape
    kv_heads = new_keys.shape[1]
    group_size = head_count // kv_heads
    scaling = 1.0 / head_dim**0.5
    query_rows = queries.reshape(sequence_count, kv_heads, group_size, head_dim)
    scores = (
        jnp.einsum("sgqd,sgdc->sgqc", query_rows, cache_keys, preferred_element_type=jnp.float32)
        * scaling
    )
    own_score = (
        jnp.einsum("sgqd,sgd->sgq", query_rows, new_keys, preferred_element_type=jnp.float32)
        * scaling
    )
    positions = jnp.arange(cache_keys.shape[3], dtype=jnp.int32)
    visible = positions[None, :] < cache_lengths[:, None]
    scores = jnp.where(visible[:, None, None, :], scores, -1e30)
    highest = jnp.maximum(jnp.max(scores, axis=3), own_score)
    cache_exp = jnp.exp(scores - highest[..., None])
    own_exp = jnp.exp(own_score - highest)
    totals = jnp.sum(cache_exp, axis=3) + own_exp
    cache_prob = (cache_exp / totals[..., None]).astype(jnp.bfloat16)
    own_prob = (own_exp / totals).astype(jnp.bfloat16)
    attended = jnp.einsum(
        "sgqc,sgdc->sgqd", cache_prob, cache_values, preferred_element_type=jnp.float32
    )
    attended = (
        attended
        + own_prob.astype(jnp.float32)[..., None] * new_values.astype(jnp.float32)[:, :, None, :]
    )
    return attended.astype(jnp.bfloat16).reshape(sequence_count, head_count * head_dim)


VMEM = pl.BlockSpec(memory_space=pltpu.VMEM)
LAST_DIMS = (((1,), (1,)), ((), ()))
MIB = 1 << 20


def call(kernel, outs, args, flops, moved, limit):
    return pl.pallas_call(
        kernel,
        out_shape=[jax.ShapeDtypeStruct(shape, dtype) for shape, dtype in outs],
        in_specs=[VMEM] * len(args),
        out_specs=[VMEM] * len(outs),
        compiler_params=pltpu.CompilerParams(vmem_limit_bytes=limit),
        cost_estimate=pl.CostEstimate(flops=flops, bytes_accessed=moved, transcendentals=0),
    )(*args)


def mm(left, right, dims=(((1,), (0,)), ((), ()))):
    return lax.dot_general(left, right, dims, preferred_element_type=jnp.float32)


def iota(shape, dim):
    return lax.broadcasted_iota(jnp.int32, shape, dim)


def attend_kernel(
    pieces,
    lengths_hbm,
    queries_hbm,
    new_keys_hbm,
    new_values_hbm,
    keys_hbm,
    values_hbm,
    weight_hbm,
    mine_ref,
    sent_ref,
    lengths_ref,
    queries_ref,
    new_keys_ref,
    new_values_ref,
    keys_ref,
    values_ref,
    weight_ref,
    own_keys_ref,
    own_values_ref,
    attended_ref,
    arrived,
):
    sequences, heads, head_dim = queries_ref.shape
    kv_heads = new_keys_ref.shape[1]
    group = heads // kv_heads
    span = kv_heads * head_dim
    lanes = group * head_dim
    moves = (
        (lengths_hbm, lengths_ref),
        (queries_hbm, queries_ref),
        (new_keys_hbm, new_keys_ref),
        (new_values_hbm, new_values_ref),
        (keys_hbm, keys_ref),
        (values_hbm, values_ref),
        *((weight_hbm.at[pl.ds(*piece)], weight_ref.at[pl.ds(*piece)]) for piece in pieces),
    )
    copies = [
        pltpu.make_async_copy(source, target, arrived.at[number])
        for number, (source, target) in enumerate(moves)
    ]
    for copy in copies:
        copy.start()

    rows = sequences * heads
    scaling = 1.0 / head_dim**0.5
    for copy in copies[:4]:
        copy.wait()
    queries = queries_ref[...].reshape(rows, head_dim)
    for sequence in range(sequences):
        block = pl.ds(sequence * kv_heads, kv_heads)
        own_keys_ref[block] = new_keys_ref[sequence].astype(jnp.float32)
        own_values_ref[block] = new_values_ref[sequence].astype(jnp.float32)
    own_keys = own_keys_ref[...].astype(jnp.bfloat16)
    own_values = own_values_ref[...].astype(jnp.bfloat16)

    spread = (iota((head_dim, span), 0) == iota((head_dim, span), 1) % head_dim).astype(
        jnp.bfloat16
    )
    same_head = iota((rows, span), 1) // head_dim == iota((rows, span), 0) % heads // group
    wide = jnp.where(same_head, mm(queries, spread), 0.0).astype(jnp.bfloat16)
    pairs = (rows, sequences * kv_heads)
    own_pair = iota(pairs, 1) == iota(pairs, 0) // group
    own_score = (
        jnp.sum(jnp.where(own_pair, mm(queries, own_keys, LAST_DIMS), 0.0), axis=1, keepdims=True)
        * scaling
    )

    copies[4].wait()
    slots = keys_ref.shape[2]
    scores = []
    for sequence in range(sequences):
        block = slice(sequence * heads, (sequence + 1) * heads)
        score = mm(wide[block], keys_ref[sequence]) * scaling
        visible = iota((heads, slots), 1) < lengths_ref[sequence]
        scores.append(jnp.where(visible, score, -1e30))
    scores = jnp.concatenate(scores, axis=0)
    highest = jnp.maximum(jnp.max(scores, axis=1, keepdims=True), own_score)
    cache_exp = jnp.exp(scores - highest)
    own_exp = jnp.exp(own_score - highest)
    totals = jnp.sum(cache_exp, axis=1, keepdims=True) + own_exp
    cache_prob = (cache_exp / totals).astype(jnp.bfloat16)
    own_prob = own_exp / totals
    own_prob = jnp.where(own_pair, own_prob, 0.0).astype(jnp.bfloat16)
    own_part = mm(own_prob, mm(own_values, spread).astype(jnp.bfloat16))

    copies[5].wait()
    attended = [
        mm(
            cache_prob[sequence * heads : (sequence + 1) * heads],
            values_ref[sequence],
            LAST_DIMS,
        )
        for sequence in range(sequences)
    ]
    attended = jnp.concatenate(attended, axis=0) + own_part
    attended = jnp.where(same_head, attended, 0.0).astype(jnp.bfloat16)
    repeat = (iota((span, lanes), 0) % head_dim == iota((span, lanes), 1) % head_dim).astype(
        jnp.bfloat16
    )
    own_lanes = iota((rows, lanes), 1) // head_dim == iota((rows, lanes), 0) % group
    placed = jnp.where(own_lanes, mm(attended, repeat), 0.0).astype(jnp.bfloat16)
    sums = (kv_heads * sequences, rows)
    chosen = (iota(sums, 0) % sequences == iota(sums, 1) // heads) & (
        iota(sums, 0) // sequences == iota(sums, 1) % heads // group
    )
    by_head = mm(chosen.astype(jnp.bfloat16), placed)
    for head in range(kv_heads):
        attended_ref[:, head * lanes : (head + 1) * lanes] = by_head[
            head * sequences : (head + 1) * sequences
        ].astype(jnp.bfloat16)
    attended = attended_ref[...]

    for copy, (start, size) in zip(copies[6:], pieces):
        copy.wait()
        part = mm(attended, weight_ref[pl.ds(start, size)], LAST_DIMS)
        mine_ref[:, start : start + size] = part
        sent_ref[:, start : start + size] = part.astype(jnp.bfloat16)


def attend_and_project(
    queries, new_keys, new_values, cache_keys, cache_values, cache_lengths, out_weight
):
    sequences, heads, head_dim = queries.shape
    kv_heads, slots = cache_keys.shape[1], cache_keys.shape[3]
    depth, width = out_weight.shape
    span = kv_heads * head_dim
    caches = (sequences, span, slots)
    hbm = pl.BlockSpec(memory_space=pltpu.HBM)
    arrays = (
        cache_lengths,
        queries,
        new_keys,
        new_values,
        cache_keys.reshape(caches),
        cache_values.reshape(caches),
        out_weight.T,
    )
    first = -(-width // 512) * 256
    pieces = ((0, first), (first, width - first))
    return pl.pallas_call(
        functools.partial(attend_kernel, pieces),
        out_shape=[
            jax.ShapeDtypeStruct((sequences, width), jnp.float32),
            jax.ShapeDtypeStruct((sequences, width), jnp.bfloat16),
        ],
        in_specs=[hbm] * len(arrays),
        out_specs=[VMEM] * 2,
        scratch_shapes=[pltpu.SMEM(cache_lengths.shape, cache_lengths.dtype)]
        + [pltpu.VMEM(array.shape, array.dtype) for array in arrays[1:]]
        + [
            pltpu.VMEM((sequences * kv_heads, head_dim), jnp.float32),
            pltpu.VMEM((sequences * kv_heads, head_dim), jnp.float32),
            pltpu.VMEM((sequences, depth), jnp.bfloat16),
            pltpu.SemaphoreType.DMA((len(arrays) - 1 + len(pieces),)),
        ],
        compiler_params=pltpu.CompilerParams(vmem_limit_bytes=53 * MIB),
        cost_estimate=pl.CostEstimate(
            flops=2 * sequences * width * depth,
            bytes_accessed=2 * (width * depth + 2 * sequences * span * slots),
            transcendentals=sequences * heads * slots,
        ),
    )(*[pltpu.with_memory_space_constraint(array, pltpu.HBM) for array in arrays])


def route_weights(expert_ids, route_probs, route_order, experts):
    picked = jnp.zeros(expert_ids.shape, jnp.float32)
    for column in range(expert_ids.shape[1]):
        picked = picked + jnp.where(route_order == column, route_probs[:, column : column + 1], 0.0)
    weights = picked / jnp.sum(route_probs, axis=1, keepdims=True)
    named = expert_ids[:, :, None] == jnp.arange(experts, dtype=jnp.int32)[None, None, :]
    return jnp.sum(jnp.where(named, weights[:, :, None], 0.0), axis=1)


def exchange(values, sent, axis, ranks):
    step = 1
    while True:
        pairs = [(rank, rank ^ step) for rank in range(ranks)]
        received = lax.ppermute(sent, axis, pairs)
        step *= 2
        if step >= ranks:
            return values, received
        values = values + received.astype(jnp.float32)
        sent = values.astype(jnp.bfloat16)


def table_kernel(weights_ref, table_ref):
    experts = weights_ref.shape[1]
    weights = weights_ref[...]
    high = weights.astype(jnp.bfloat16)
    low = (weights - high.astype(jnp.float32)).astype(jnp.bfloat16)
    table_ref[...] = jnp.zeros_like(table_ref)
    table_ref[:, :experts] = high
    table_ref[:, experts : 2 * experts] = low


def norm_kernel(mine_ref, received_ref, hidden_ref, gain_ref, table_ref, residual_ref, rows_ref):
    width = hidden_ref.shape[1]
    residual = (
        hidden_ref[...].astype(jnp.float32) + mine_ref[...] + received_ref[...].astype(jnp.float32)
    )
    residual_ref[...] = residual
    mean_square = jnp.mean(residual * residual, axis=1, keepdims=True)
    normed = residual * lax.rsqrt(mean_square + EPSILON) * gain_ref[...]
    rows_ref[:, :width] = normed.astype(jnp.bfloat16)
    rows_ref[:, width:] = table_ref[...]


def pack_kernel(*refs):
    *piece_refs, packed_ref = refs
    size = piece_refs[0].shape[0]
    for number, piece_ref in enumerate(piece_refs):
        packed_ref[pl.ds(number * size, size)] = piece_ref[...]


def turn_kernel(pieces, *refs):
    for (start, size), source_ref, target_ref in zip(
        pieces, refs[: len(pieces)], refs[len(pieces) :]
    ):
        for local in range(source_ref.shape[0]):
            target_ref[local] = source_ref[local, pl.ds(start, size)].T


def turn(*sources):
    weights = [weight for weight, _, _ in sources]
    pieces = [(start, size) for _, start, size in sources]
    return call(
        functools.partial(turn_kernel, pieces),
        [(weight.shape[:2] + (size,), weight.dtype) for weight, _, size in sources],
        [weight.swapaxes(1, 2) for weight in weights],
        flops=1,
        moved=1,
        limit=6 * MIB,
    )


def expert_kernel(experts, *refs):
    *row_refs, gate_ref, first_ref, second_ref, down_ref, mine_ref, other_ref = refs
    local_experts, _, width = down_ref.shape
    rows = jnp.concatenate([ref[:, :width] for ref in row_refs], axis=0)
    table = jnp.concatenate([ref[:, width:] for ref in row_refs], axis=0).astype(jnp.float32)
    column = lax.broadcasted_iota(jnp.int32, table.shape, 1)
    total = None
    for local in range(local_experts):
        expert = lax.axis_index("expert") * local_experts + local
        chosen = (column == expert) | (column == expert + experts)
        weight = jnp.sum(jnp.where(chosen, table, 0.0), axis=1, keepdims=True)
        gate = mm(rows, gate_ref[local])
        up = [mm(rows, up_ref[local]) for up_ref in (first_ref, second_ref)]
        up = jnp.concatenate(up, axis=1)
        active = (gate * jax.nn.sigmoid(GLU_SLOPE * gate) * (up + 1.0)).astype(jnp.bfloat16)
        part = mm(active, down_ref[local])
        part = part * weight
        total = part if total is None else total + part
    half = mine_ref.shape[0]
    mine_ref[...] = total[:half]
    other_ref[...] = total[half:].astype(jnp.bfloat16)


def split_kernel(mine_ref, received_ref, kept_ref, *sent_refs):
    size = kept_ref.shape[0]
    kept_ref[...] = mine_ref[:size] + received_ref[:size].astype(jnp.float32)
    for number, sent_ref in enumerate(sent_refs, 1):
        block = pl.ds(number * size, size)
        total = mine_ref[block] + received_ref[block].astype(jnp.float32)
        sent_ref[...] = total.astype(jnp.bfloat16)


def return_kernel(received, residual_ref, *refs):
    kept_ref, *received_refs = refs[: 1 + received]
    base_ref, *sent_refs = refs[1 + received :]
    total = kept_ref[...]
    for received_ref in received_refs:
        total = total + received_ref[...].astype(jnp.float32)
    width = base_ref.shape[1]
    rank = lax.axis_index("tensor")

    def slab_of(values, owner):
        slab = values[:, :width]
        for number in range(1, values.shape[1] // width):
            piece = values[:, number * width : (number + 1) * width]
            slab = jnp.where(owner == number, piece, slab)
        return slab

    base_ref[...] = slab_of(total + residual_ref[...], rank)
    for step, sent_ref in enumerate(sent_refs, 1):
        sent_ref[...] = slab_of(total, rank ^ step).astype(jnp.bfloat16)


def output_kernel(base_ref, *refs):
    *received_refs, output_ref = refs
    total = base_ref[...]
    for received_ref in received_refs:
        total = total + received_ref[...].astype(jnp.float32)
    output_ref[...] = total.astype(jnp.bfloat16)


def per_device(
    hidden_in,
    queries,
    new_keys,
    new_values,
    cache_keys,
    cache_values,
    cache_lengths,
    out_weight,
    norm_gain,
    expert_ids,
    route_probs,
    route_order,
    gate_weight,
    up_weight,
    down_weight,
):
    sequences, width = hidden_in.shape
    expert_ranks = lax.axis_size("expert")
    tensor_ranks = lax.axis_size("tensor")
    local_experts, hidden_units = down_weight.shape[:2]
    experts = local_experts * expert_ranks
    inner = 2
    outer = expert_ranks // inner
    cut = 3 * hidden_units // 4 // 128 * 128
    row_width = -(-(width + 2 * experts) // 128) * 128

    def to_outer(values, step):
        pairs = [(rank, rank ^ (step * inner)) for rank in range(expert_ranks)]
        return lax.ppermute(values, "expert", pairs)

    def to_inner(values):
        return lax.ppermute(values, "expert", [(rank, rank ^ 1) for rank in range(expert_ranks)])

    operands = (queries, new_keys, new_values, cache_keys, cache_values, cache_lengths)
    if queries.shape[1] % 16 == 0:
        mine, sent = attend_and_project(*operands, out_weight)
    else:
        mine = jnp.dot(attend(*operands), out_weight, preferred_element_type=jnp.float32)
        sent = mine.astype(jnp.bfloat16)
    mine, received = exchange(mine, sent, "tensor", tensor_ranks)

    weights = route_weights(expert_ids, route_probs, route_order, experts)
    (table,) = call(
        table_kernel,
        [((sequences, row_width - width), jnp.bfloat16)],
        (weights,),
        flops=WINDOW_FLOPS,
        moved=sequences * row_width,
        limit=MIB,
    )

    block = (sequences, width)
    residual, rows = call(
        norm_kernel,
        [(block, jnp.float32), ((sequences, row_width), jnp.bfloat16)],
        (mine, received, hidden_in, norm_gain.reshape(1, width), table),
        flops=16 * sequences * width,
        moved=sequences * width * 16,
        limit=2 * MIB,
    )

    near = [rows]
    for step in range(1, outer):
        near.append(to_outer(rows, step))
    gate_turned, up_first = turn((gate_weight, 0, hidden_units), (up_weight, 0, cut))
    (near,) = call(
        pack_kernel,
        [((outer * sequences, row_width), jnp.bfloat16)],
        near,
        flops=sequences,
        moved=4 * outer * sequences * row_width,
        limit=2 * MIB,
    )
    far = to_inner(near)
    (up_second,) = turn((up_weight, cut, hidden_units - cut))
    half = (outer * sequences, width)
    mine, other = call(
        functools.partial(expert_kernel, experts),
        [(half, jnp.float32), (half, jnp.bfloat16)],
        (near, far, gate_turned, up_first, up_second, down_weight),
        flops=12 * half[0] * width * hidden_units * local_experts,
        moved=6 * width * hidden_units * local_experts,
        limit=16 * MIB,
    )
    received = to_inner(other)
    kept, *sent = call(
        split_kernel,
        [(block, jnp.float32)] + [(block, jnp.bfloat16)] * (outer - 1),
        (mine, received),
        flops=half[0] * width,
        moved=half[0] * width * 8,
        limit=4 * MIB,
    )
    returned = []
    for step, piece in enumerate(sent, 1):
        returned.append(to_outer(piece, step))
    slab = (sequences, width // tensor_ranks)
    total, *sent = call(
        functools.partial(return_kernel, len(returned)),
        [(slab, jnp.float32)] + [(slab, jnp.bfloat16)] * (tensor_ranks - 1),
        (residual, kept, *returned),
        flops=half[0] * width,
        moved=half[0] * width * 2,
        limit=2 * MIB,
    )
    arrived = []
    for step, piece in enumerate(sent, 1):
        pairs = [(rank, rank ^ step) for rank in range(tensor_ranks)]
        arrived.append(lax.ppermute(piece, "tensor", pairs))
    (output,) = call(
        output_kernel,
        [(slab, jnp.bfloat16)],
        (total, *arrived),
        flops=slab[0] * slab[1] * tensor_ranks,
        moved=slab[0] * slab[1] * 2,
        limit=2 * MIB,
    )
    return output


def solution(mesh):
    in_specs = (
        P(("groups", "expert"), None),
        P(("groups", "expert"), "tensor", None),
        P(("groups", "expert"), "tensor", None),
        P(("groups", "expert"), "tensor", None),
        P(("groups", "expert"), "tensor", None, None),
        P(("groups", "expert"), "tensor", None, None),
        P(("groups", "expert")),
        P("tensor", None),
        P(),
        P(("groups", "expert"), None),
        P(("groups", "expert"), None),
        P(("groups", "expert"), None),
        P("expert", None, "tensor"),
        P("expert", None, "tensor"),
        P("expert", "tensor", None),
    )
    out_specs = P(("groups", "expert"), "tensor")

    return jax.shard_map(
        per_device, mesh=mesh, in_specs=in_specs, out_specs=out_specs, check_vma=False
    )
```

```python
import functools

import jax
import jax.numpy as jnp
from jax import lax
from jax.experimental import pallas as pl
from jax.experimental.pallas import tpu as pltpu
from jax.sharding import PartitionSpec as P

EPSILON = 1e-05
GLU_SLOPE = 1.702
WINDOW_FLOPS = 50_000_000_000


def attend(queries, new_keys, new_values, cache_keys, cache_values, cache_lengths):
    sequence_count, head_count, head_dim = queries.shape
    kv_heads = new_keys.shape[1]
    group_size = head_count // kv_heads
    scaling = 1.0 / head_dim**0.5
    query_rows = queries.reshape(sequence_count, kv_heads, group_size, head_dim)
    scores = (
        jnp.einsum("sgqd,sgdc->sgqc", query_rows, cache_keys, preferred_element_type=jnp.float32)
        * scaling
    )
    own_score = (
        jnp.einsum("sgqd,sgd->sgq", query_rows, new_keys, preferred_element_type=jnp.float32)
        * scaling
    )
    positions = jnp.arange(cache_keys.shape[3], dtype=jnp.int32)
    visible = positions[None, :] < cache_lengths[:, None]
    scores = jnp.where(visible[:, None, None, :], scores, -1e30)
    highest = jnp.maximum(jnp.max(scores, axis=3), own_score)
    cache_exp = jnp.exp(scores - highest[..., None])
    own_exp = jnp.exp(own_score - highest)
    totals = jnp.sum(cache_exp, axis=3) + own_exp
    cache_prob = (cache_exp / totals[..., None]).astype(jnp.bfloat16)
    own_prob = (own_exp / totals).astype(jnp.bfloat16)
    attended = jnp.einsum(
        "sgqc,sgdc->sgqd", cache_prob, cache_values, preferred_element_type=jnp.float32
    )
    attended = (
        attended
        + own_prob.astype(jnp.float32)[..., None] * new_values.astype(jnp.float32)[:, :, None, :]
    )
    return attended.astype(jnp.bfloat16).reshape(sequence_count, head_count * head_dim)


VMEM = pl.BlockSpec(memory_space=pltpu.VMEM)
LAST_DIMS = (((1,), (1,)), ((), ()))
MIB = 1 << 20


def call(kernel, outs, args, flops, moved, limit):
    return pl.pallas_call(
        kernel,
        out_shape=[jax.ShapeDtypeStruct(shape, dtype) for shape, dtype in outs],
        in_specs=[VMEM] * len(args),
        out_specs=[VMEM] * len(outs),
        compiler_params=pltpu.CompilerParams(vmem_limit_bytes=limit),
        cost_estimate=pl.CostEstimate(flops=flops, bytes_accessed=moved, transcendentals=0),
    )(*args)


def mm(left, right, dims=(((1,), (0,)), ((), ()))):
    return lax.dot_general(left, right, dims, preferred_element_type=jnp.float32)


def iota(shape, dim):
    return lax.broadcasted_iota(jnp.int32, shape, dim)


def attend_kernel(
    pieces,
    lengths_hbm,
    queries_hbm,
    new_keys_hbm,
    new_values_hbm,
    keys_hbm,
    values_hbm,
    weight_hbm,
    mine_ref,
    sent_ref,
    lengths_ref,
    queries_ref,
    new_keys_ref,
    new_values_ref,
    keys_ref,
    values_ref,
    weight_ref,
    own_keys_ref,
    own_values_ref,
    attended_ref,
    arrived,
):
    sequences, heads, head_dim = queries_ref.shape
    kv_heads = new_keys_ref.shape[1]
    group = heads // kv_heads
    span = kv_heads * head_dim
    lanes = group * head_dim
    moves = (
        (lengths_hbm, lengths_ref),
        (queries_hbm, queries_ref),
        (new_keys_hbm, new_keys_ref),
        (new_values_hbm, new_values_ref),
        (keys_hbm, keys_ref),
        (values_hbm, values_ref),
        *((weight_hbm.at[pl.ds(*piece)], weight_ref.at[pl.ds(*piece)]) for piece in pieces),
    )
    copies = [
        pltpu.make_async_copy(source, target, arrived.at[number])
        for number, (source, target) in enumerate(moves)
    ]
    for copy in copies:
        copy.start()

    rows = sequences * heads
    scaling = 1.0 / head_dim**0.5
    for copy in copies[:4]:
        copy.wait()
    queries = queries_ref[...].reshape(rows, head_dim)
    for sequence in range(sequences):
        block = pl.ds(sequence * kv_heads, kv_heads)
        own_keys_ref[block] = new_keys_ref[sequence].astype(jnp.float32)
        own_values_ref[block] = new_values_ref[sequence].astype(jnp.float32)
    own_keys = own_keys_ref[...].astype(jnp.bfloat16)
    own_values = own_values_ref[...].astype(jnp.bfloat16)

    spread = (iota((head_dim, span), 0) == iota((head_dim, span), 1) % head_dim).astype(
        jnp.bfloat16
    )
    same_head = iota((rows, span), 1) // head_dim == iota((rows, span), 0) % heads // group
    wide = jnp.where(same_head, mm(queries, spread), 0.0).astype(jnp.bfloat16)
    pairs = (rows, sequences * kv_heads)
    own_pair = iota(pairs, 1) == iota(pairs, 0) // group
    own_score = (
        jnp.sum(jnp.where(own_pair, mm(queries, own_keys, LAST_DIMS), 0.0), axis=1, keepdims=True)
        * scaling
    )

    copies[4].wait()
    slots = keys_ref.shape[2]
    scores = []
    for sequence in range(sequences):
        block = slice(sequence * heads, (sequence + 1) * heads)
        score = mm(wide[block], keys_ref[sequence]) * scaling
        visible = iota((heads, slots), 1) < lengths_ref[sequence]
        scores.append(jnp.where(visible, score, -1e30))
    scores = jnp.concatenate(scores, axis=0)
    highest = jnp.maximum(jnp.max(scores, axis=1, keepdims=True), own_score)
    cache_exp = jnp.exp(scores - highest)
    own_exp = jnp.exp(own_score - highest)
    totals = jnp.sum(cache_exp, axis=1, keepdims=True) + own_exp
    cache_prob = (cache_exp / totals).astype(jnp.bfloat16)
    own_prob = own_exp / totals
    own_prob = jnp.where(own_pair, own_prob, 0.0).astype(jnp.bfloat16)
    own_part = mm(own_prob, mm(own_values, spread).astype(jnp.bfloat16))

    copies[5].wait()
    attended = [
        mm(
            cache_prob[sequence * heads : (sequence + 1) * heads],
            values_ref[sequence],
            LAST_DIMS,
        )
        for sequence in range(sequences)
    ]
    attended = jnp.concatenate(attended, axis=0) + own_part
    attended = jnp.where(same_head, attended, 0.0).astype(jnp.bfloat16)
    repeat = (iota((span, lanes), 0) % head_dim == iota((span, lanes), 1) % head_dim).astype(
        jnp.bfloat16
    )
    own_lanes = iota((rows, lanes), 1) // head_dim == iota((rows, lanes), 0) % group
    placed = jnp.where(own_lanes, mm(attended, repeat), 0.0).astype(jnp.bfloat16)
    sums = (kv_heads * sequences, rows)
    chosen = (iota(sums, 0) % sequences == iota(sums, 1) // heads) & (
        iota(sums, 0) // sequences == iota(sums, 1) % heads // group
    )
    by_head = mm(chosen.astype(jnp.bfloat16), placed)
    for head in range(kv_heads):
        attended_ref[:, head * lanes : (head + 1) * lanes] = by_head[
            head * sequences : (head + 1) * sequences
        ].astype(jnp.bfloat16)
    attended = attended_ref[...]

    for copy, (start, size) in zip(copies[6:], pieces):
        copy.wait()
        part = mm(attended, weight_ref[pl.ds(start, size)], LAST_DIMS)
        mine_ref[:, start : start + size] = part
        sent_ref[:, start : start + size] = part.astype(jnp.bfloat16)


def attend_and_project(
    queries, new_keys, new_values, cache_keys, cache_values, cache_lengths, out_weight
):
    sequences, heads, head_dim = queries.shape
    kv_heads, slots = cache_keys.shape[1], cache_keys.shape[3]
    depth, width = out_weight.shape
    span = kv_heads * head_dim
    caches = (sequences, span, slots)
    hbm = pl.BlockSpec(memory_space=pltpu.HBM)
    arrays = (
        cache_lengths,
        queries,
        new_keys,
        new_values,
        cache_keys.reshape(caches),
        cache_values.reshape(caches),
        out_weight.T,
    )
    first = -(-width // 512) * 256
    pieces = ((0, first), (first, width - first))
    return pl.pallas_call(
        functools.partial(attend_kernel, pieces),
        out_shape=[
            jax.ShapeDtypeStruct((sequences, width), jnp.float32),
            jax.ShapeDtypeStruct((sequences, width), jnp.bfloat16),
        ],
        in_specs=[hbm] * len(arrays),
        out_specs=[VMEM] * 2,
        scratch_shapes=[pltpu.SMEM(cache_lengths.shape, cache_lengths.dtype)]
        + [pltpu.VMEM(array.shape, array.dtype) for array in arrays[1:]]
        + [
            pltpu.VMEM((sequences * kv_heads, head_dim), jnp.float32),
            pltpu.VMEM((sequences * kv_heads, head_dim), jnp.float32),
            pltpu.VMEM((sequences, depth), jnp.bfloat16),
            pltpu.SemaphoreType.DMA((len(arrays) - 1 + len(pieces),)),
        ],
        compiler_params=pltpu.CompilerParams(vmem_limit_bytes=53 * MIB),
        cost_estimate=pl.CostEstimate(
            flops=2 * sequences * width * depth,
            bytes_accessed=2 * (width * depth + 2 * sequences * span * slots),
            transcendentals=sequences * heads * slots,
        ),
    )(*[pltpu.with_memory_space_constraint(array, pltpu.HBM) for array in arrays])


def route_weights(expert_ids, route_probs, route_order, experts):
    picked = jnp.zeros(expert_ids.shape, jnp.float32)
    for column in range(expert_ids.shape[1]):
        picked = picked + jnp.where(route_order == column, route_probs[:, column : column + 1], 0.0)
    weights = picked / jnp.sum(route_probs, axis=1, keepdims=True)
    named = expert_ids[:, :, None] == jnp.arange(experts, dtype=jnp.int32)[None, None, :]
    return jnp.sum(jnp.where(named, weights[:, :, None], 0.0), axis=1)


def exchange(values, sent, axis, ranks):
    step = 1
    while True:
        pairs = [(rank, rank ^ step) for rank in range(ranks)]
        received = lax.ppermute(sent, axis, pairs)
        step *= 2
        if step >= ranks:
            return values, received
        values = values + received.astype(jnp.float32)
        sent = values.astype(jnp.bfloat16)


def table_kernel(weights_ref, table_ref):
    experts = weights_ref.shape[1]
    weights = weights_ref[...]
    high = weights.astype(jnp.bfloat16)
    low = (weights - high.astype(jnp.float32)).astype(jnp.bfloat16)
    table_ref[...] = jnp.zeros_like(table_ref)
    table_ref[:, :experts] = high
    table_ref[:, experts : 2 * experts] = low


def norm_kernel(mine_ref, received_ref, hidden_ref, gain_ref, table_ref, residual_ref, rows_ref):
    width = hidden_ref.shape[1]
    residual = (
        hidden_ref[...].astype(jnp.float32) + mine_ref[...] + received_ref[...].astype(jnp.float32)
    )
    residual_ref[...] = residual
    mean_square = jnp.mean(residual * residual, axis=1, keepdims=True)
    normed = residual * lax.rsqrt(mean_square + EPSILON) * gain_ref[...]
    rows_ref[:, :width] = normed.astype(jnp.bfloat16)
    rows_ref[:, width:] = table_ref[...]


def pack_kernel(*refs):
    *piece_refs, packed_ref = refs
    size = piece_refs[0].shape[0]
    for number, piece_ref in enumerate(piece_refs):
        packed_ref[pl.ds(number * size, size)] = piece_ref[...]


def turn_kernel(pieces, *refs):
    for (start, size), source_ref, target_ref in zip(
        pieces, refs[: len(pieces)], refs[len(pieces) :]
    ):
        for local in range(source_ref.shape[0]):
            target_ref[local] = source_ref[local, pl.ds(start, size)].T


def turn(*sources):
    weights = [weight for weight, _, _ in sources]
    pieces = [(start, size) for _, start, size in sources]
    return call(
        functools.partial(turn_kernel, pieces),
        [(weight.shape[:2] + (size,), weight.dtype) for weight, _, size in sources],
        [weight.swapaxes(1, 2) for weight in weights],
        flops=1,
        moved=1,
        limit=6 * MIB,
    )


def expert_kernel(experts, *refs):
    *row_refs, gate_ref, first_ref, second_ref, down_ref, mine_ref, other_ref = refs
    local_experts, _, width = down_ref.shape
    rows = jnp.concatenate([ref[:, :width] for ref in row_refs], axis=0)
    table = jnp.concatenate([ref[:, width:] for ref in row_refs], axis=0).astype(jnp.float32)
    column = lax.broadcasted_iota(jnp.int32, table.shape, 1)
    total = None
    for local in range(local_experts):
        expert = lax.axis_index("expert") * local_experts + local
        chosen = (column == expert) | (column == expert + experts)
        weight = jnp.sum(jnp.where(chosen, table, 0.0), axis=1, keepdims=True)
        gate = mm(rows, gate_ref[local])
        up = [mm(rows, up_ref[local]) for up_ref in (first_ref, second_ref)]
        up = jnp.concatenate(up, axis=1)
        active = (gate * jax.nn.sigmoid(GLU_SLOPE * gate) * (up + 1.0)).astype(jnp.bfloat16)
        part = mm(active, down_ref[local])
        part = part * weight
        total = part if total is None else total + part
    half = mine_ref.shape[0]
    mine_ref[...] = total[:half]
    other_ref[...] = total[half:].astype(jnp.bfloat16)


def split_kernel(mine_ref, received_ref, kept_ref, *sent_refs):
    size = kept_ref.shape[0]
    kept_ref[...] = mine_ref[:size] + received_ref[:size].astype(jnp.float32)
    for number, sent_ref in enumerate(sent_refs, 1):
        block = pl.ds(number * size, size)
        total = mine_ref[block] + received_ref[block].astype(jnp.float32)
        sent_ref[...] = total.astype(jnp.bfloat16)


def return_kernel(received, residual_ref, *refs):
    kept_ref, *received_refs = refs[: 1 + received]
    base_ref, *sent_refs = refs[1 + received :]
    total = kept_ref[...]
    for received_ref in received_refs:
        total = total + received_ref[...].astype(jnp.float32)
    width = base_ref.shape[1]
    rank = lax.axis_index("tensor")

    def slab_of(values, owner):
        slab = values[:, :width]
        for number in range(1, values.shape[1] // width):
            piece = values[:, number * width : (number + 1) * width]
            slab = jnp.where(owner == number, piece, slab)
        return slab

    base_ref[...] = slab_of(total + residual_ref[...], rank)
    for step, sent_ref in enumerate(sent_refs, 1):
        sent_ref[...] = slab_of(total, rank ^ step).astype(jnp.bfloat16)


def per_device(
    hidden_in,
    queries,
    new_keys,
    new_values,
    cache_keys,
    cache_values,
    cache_lengths,
    out_weight,
    norm_gain,
    expert_ids,
    route_probs,
    route_order,
    gate_weight,
    up_weight,
    down_weight,
):
    sequences, width = hidden_in.shape
    expert_ranks = lax.axis_size("expert")
    tensor_ranks = lax.axis_size("tensor")
    local_experts, hidden_units = down_weight.shape[:2]
    experts = local_experts * expert_ranks
    inner = 2
    outer = expert_ranks // inner
    cut = -(-hidden_units // 256) * 128
    row_width = -(-(width + 2 * experts) // 128) * 128

    def to_outer(values, step):
        pairs = [(rank, rank ^ (step * inner)) for rank in range(expert_ranks)]
        return lax.ppermute(values, "expert", pairs)

    def to_inner(values):
        return lax.ppermute(values, "expert", [(rank, rank ^ 1) for rank in range(expert_ranks)])

    operands = (queries, new_keys, new_values, cache_keys, cache_values, cache_lengths)
    if queries.shape[1] % 16 == 0:
        mine, sent = attend_and_project(*operands, out_weight)
    else:
        mine = jnp.dot(attend(*operands), out_weight, preferred_element_type=jnp.float32)
        sent = mine.astype(jnp.bfloat16)
    mine, received = exchange(mine, sent, "tensor", tensor_ranks)

    weights = route_weights(expert_ids, route_probs, route_order, experts)
    (table,) = call(
        table_kernel,
        [((sequences, row_width - width), jnp.bfloat16)],
        (weights,),
        flops=WINDOW_FLOPS,
        moved=sequences * row_width,
        limit=MIB,
    )

    block = (sequences, width)
    residual, rows = call(
        norm_kernel,
        [(block, jnp.float32), ((sequences, row_width), jnp.bfloat16)],
        (mine, received, hidden_in, norm_gain.reshape(1, width), table),
        flops=16 * sequences * width,
        moved=sequences * width * 16,
        limit=2 * MIB,
    )

    near = [rows]
    for step in range(1, outer):
        near.append(to_outer(rows, step))
    gate_turned, up_first = turn((gate_weight, 0, hidden_units), (up_weight, 0, cut))
    (near,) = call(
        pack_kernel,
        [((outer * sequences, row_width), jnp.bfloat16)],
        near,
        flops=sequences,
        moved=4 * outer * sequences * row_width,
        limit=2 * MIB,
    )
    far = to_inner(near)
    (up_second,) = turn((up_weight, cut, hidden_units - cut))
    half = (outer * sequences, width)
    mine, other = call(
        functools.partial(expert_kernel, experts),
        [(half, jnp.float32), (half, jnp.bfloat16)],
        (near, far, gate_turned, up_first, up_second, down_weight),
        flops=12 * half[0] * width * hidden_units * local_experts,
        moved=6 * width * hidden_units * local_experts,
        limit=16 * MIB,
    )
    received = to_inner(other)
    kept, *sent = call(
        split_kernel,
        [(block, jnp.float32)] + [(block, jnp.bfloat16)] * (outer - 1),
        (mine, received),
        flops=half[0] * width,
        moved=half[0] * width * 8,
        limit=4 * MIB,
    )
    returned = []
    for step, piece in enumerate(sent, 1):
        returned.append(to_outer(piece, step))
    slab = (sequences, width // tensor_ranks)
    total, *sent = call(
        functools.partial(return_kernel, len(returned)),
        [(slab, jnp.float32)] + [(slab, jnp.bfloat16)] * (tensor_ranks - 1),
        (residual, kept, *returned),
        flops=half[0] * width,
        moved=half[0] * width * 2,
        limit=2 * MIB,
    )
    for step, piece in enumerate(sent, 1):
        pairs = [(rank, rank ^ step) for rank in range(tensor_ranks)]
        total = total + lax.ppermute(piece, "tensor", pairs).astype(jnp.float32)
    return total.astype(jnp.bfloat16)


def solution(mesh):
    in_specs = (
        P(("groups", "expert"), None),
        P(("groups", "expert"), "tensor", None),
        P(("groups", "expert"), "tensor", None),
        P(("groups", "expert"), "tensor", None),
        P(("groups", "expert"), "tensor", None, None),
        P(("groups", "expert"), "tensor", None, None),
        P(("groups", "expert")),
        P("tensor", None),
        P(),
        P(("groups", "expert"), None),
        P(("groups", "expert"), None),
        P(("groups", "expert"), None),
        P("expert", None, "tensor"),
        P("expert", None, "tensor"),
        P("expert", "tensor", None),
    )
    out_specs = P(("groups", "expert"), "tensor")

    return jax.shard_map(
        per_device, mesh=mesh, in_specs=in_specs, out_specs=out_specs, check_vma=False
    )
```

```python
import functools

import jax
import jax.numpy as jnp
from jax import lax
from jax.experimental import pallas as pl
from jax.experimental.pallas import tpu as pltpu
from jax.sharding import PartitionSpec as P

EPSILON = 1e-05
GLU_SLOPE = 1.702
WINDOW_FLOPS = 50_000_000_000


def attend(queries, new_keys, new_values, cache_keys, cache_values, cache_lengths):
    sequence_count, head_count, head_dim = queries.shape
    kv_heads = new_keys.shape[1]
    group_size = head_count // kv_heads
    scaling = 1.0 / head_dim**0.5
    query_rows = queries.reshape(sequence_count, kv_heads, group_size, head_dim)
    scores = (
        jnp.einsum("sgqd,sgdc->sgqc", query_rows, cache_keys, preferred_element_type=jnp.float32)
        * scaling
    )
    own_score = (
        jnp.einsum("sgqd,sgd->sgq", query_rows, new_keys, preferred_element_type=jnp.float32)
        * scaling
    )
    positions = jnp.arange(cache_keys.shape[3], dtype=jnp.int32)
    visible = positions[None, :] < cache_lengths[:, None]
    scores = jnp.where(visible[:, None, None, :], scores, -1e30)
    highest = jnp.maximum(jnp.max(scores, axis=3), own_score)
    cache_exp = jnp.exp(scores - highest[..., None])
    own_exp = jnp.exp(own_score - highest)
    totals = jnp.sum(cache_exp, axis=3) + own_exp
    cache_prob = (cache_exp / totals[..., None]).astype(jnp.bfloat16)
    own_prob = (own_exp / totals).astype(jnp.bfloat16)
    attended = jnp.einsum(
        "sgqc,sgdc->sgqd", cache_prob, cache_values, preferred_element_type=jnp.float32
    )
    attended = (
        attended
        + own_prob.astype(jnp.float32)[..., None] * new_values.astype(jnp.float32)[:, :, None, :]
    )
    return attended.astype(jnp.bfloat16).reshape(sequence_count, head_count * head_dim)


VMEM = pl.BlockSpec(memory_space=pltpu.VMEM)
LAST_DIMS = (((1,), (1,)), ((), ()))
MIB = 1 << 20


def call(kernel, outs, args, flops, moved, limit):
    return pl.pallas_call(
        kernel,
        out_shape=[jax.ShapeDtypeStruct(shape, dtype) for shape, dtype in outs],
        in_specs=[VMEM] * len(args),
        out_specs=[VMEM] * len(outs),
        compiler_params=pltpu.CompilerParams(vmem_limit_bytes=limit),
        cost_estimate=pl.CostEstimate(flops=flops, bytes_accessed=moved, transcendentals=0),
    )(*args)


def mm(left, right, dims=(((1,), (0,)), ((), ()))):
    return lax.dot_general(left, right, dims, preferred_element_type=jnp.float32)


def iota(shape, dim):
    return lax.broadcasted_iota(jnp.int32, shape, dim)


def attend_kernel(
    pieces,
    lengths_hbm,
    queries_hbm,
    new_keys_hbm,
    new_values_hbm,
    keys_hbm,
    values_hbm,
    weight_hbm,
    mine_ref,
    sent_ref,
    lengths_ref,
    queries_ref,
    new_keys_ref,
    new_values_ref,
    keys_ref,
    values_ref,
    weight_ref,
    own_keys_ref,
    own_values_ref,
    attended_ref,
    arrived,
):
    sequences, heads, head_dim = queries_ref.shape
    kv_heads = new_keys_ref.shape[1]
    group = heads // kv_heads
    span = kv_heads * head_dim
    lanes = group * head_dim
    moves = (
        (lengths_hbm, lengths_ref),
        (queries_hbm, queries_ref),
        (new_keys_hbm, new_keys_ref),
        (new_values_hbm, new_values_ref),
        (keys_hbm, keys_ref),
        (values_hbm, values_ref),
        *((weight_hbm.at[pl.ds(*piece)], weight_ref.at[pl.ds(*piece)]) for piece in pieces),
    )
    copies = [
        pltpu.make_async_copy(source, target, arrived.at[number])
        for number, (source, target) in enumerate(moves)
    ]
    for copy in copies:
        copy.start()

    rows = sequences * heads
    scaling = 1.0 / head_dim**0.5
    for copy in copies[:4]:
        copy.wait()
    queries = queries_ref[...].reshape(rows, head_dim)
    for sequence in range(sequences):
        block = pl.ds(sequence * kv_heads, kv_heads)
        own_keys_ref[block] = new_keys_ref[sequence].astype(jnp.float32)
        own_values_ref[block] = new_values_ref[sequence].astype(jnp.float32)
    own_keys = own_keys_ref[...].astype(jnp.bfloat16)
    own_values = own_values_ref[...].astype(jnp.bfloat16)

    spread = (iota((head_dim, span), 0) == iota((head_dim, span), 1) % head_dim).astype(
        jnp.bfloat16
    )
    same_head = iota((rows, span), 1) // head_dim == iota((rows, span), 0) % heads // group
    wide = jnp.where(same_head, mm(queries, spread), 0.0).astype(jnp.bfloat16)
    pairs = (rows, sequences * kv_heads)
    own_pair = iota(pairs, 1) == iota(pairs, 0) // group
    own_score = (
        jnp.sum(jnp.where(own_pair, mm(queries, own_keys, LAST_DIMS), 0.0), axis=1, keepdims=True)
        * scaling
    )

    repeat = (iota((span, lanes), 0) % head_dim == iota((span, lanes), 1) % head_dim).astype(
        jnp.bfloat16
    )
    own_lanes = iota((rows, lanes), 1) // head_dim == iota((rows, lanes), 0) % group
    sums = (kv_heads * sequences, rows)
    chosen = (iota(sums, 0) % sequences == iota(sums, 1) // heads) & (
        iota(sums, 0) // sequences == iota(sums, 1) % heads // group
    )
    chosen = chosen.astype(jnp.bfloat16)
    own_wide = mm(own_values, spread).astype(jnp.bfloat16)

    copies[4].wait()
    slots = keys_ref.shape[2]
    scores = []
    for sequence in range(sequences):
        block = slice(sequence * heads, (sequence + 1) * heads)
        score = mm(wide[block], keys_ref[sequence]) * scaling
        visible = iota((heads, slots), 1) < lengths_ref[sequence]
        scores.append(jnp.where(visible, score, -1e30))
    scores = jnp.concatenate(scores, axis=0)
    highest = jnp.maximum(jnp.max(scores, axis=1, keepdims=True), own_score)
    cache_exp = jnp.exp(scores - highest)
    own_exp = jnp.exp(own_score - highest)
    totals = jnp.sum(cache_exp, axis=1, keepdims=True) + own_exp
    cache_prob = (cache_exp / totals).astype(jnp.bfloat16)
    own_prob = own_exp / totals
    own_prob = jnp.where(own_pair, own_prob, 0.0).astype(jnp.bfloat16)
    own_part = mm(own_prob, own_wide)

    copies[5].wait()
    attended = [
        mm(
            cache_prob[sequence * heads : (sequence + 1) * heads],
            values_ref[sequence],
            LAST_DIMS,
        )
        for sequence in range(sequences)
    ]
    attended = jnp.concatenate(attended, axis=0) + own_part
    attended = jnp.where(same_head, attended, 0.0).astype(jnp.bfloat16)
    placed = jnp.where(own_lanes, mm(attended, repeat), 0.0).astype(jnp.bfloat16)
    by_head = mm(chosen, placed)
    for head in range(kv_heads):
        attended_ref[:, head * lanes : (head + 1) * lanes] = by_head[
            head * sequences : (head + 1) * sequences
        ].astype(jnp.bfloat16)
    attended = attended_ref[...]

    for copy, (start, size) in zip(copies[6:], pieces):
        copy.wait()
        part = mm(attended, weight_ref[pl.ds(start, size)], LAST_DIMS)
        mine_ref[:, start : start + size] = part
        sent_ref[:, start : start + size] = part.astype(jnp.bfloat16)


def attend_and_project(
    queries, new_keys, new_values, cache_keys, cache_values, cache_lengths, out_weight
):
    sequences, heads, head_dim = queries.shape
    kv_heads, slots = cache_keys.shape[1], cache_keys.shape[3]
    depth, width = out_weight.shape
    span = kv_heads * head_dim
    caches = (sequences, span, slots)
    hbm = pl.BlockSpec(memory_space=pltpu.HBM)
    arrays = (
        cache_lengths,
        queries,
        new_keys,
        new_values,
        cache_keys.reshape(caches),
        cache_values.reshape(caches),
        out_weight.T,
    )
    first = -(-width // 512) * 256
    pieces = ((0, first), (first, width - first))
    return pl.pallas_call(
        functools.partial(attend_kernel, pieces),
        out_shape=[
            jax.ShapeDtypeStruct((sequences, width), jnp.float32),
            jax.ShapeDtypeStruct((sequences, width), jnp.bfloat16),
        ],
        in_specs=[hbm] * len(arrays),
        out_specs=[VMEM] * 2,
        scratch_shapes=[pltpu.SMEM(cache_lengths.shape, cache_lengths.dtype)]
        + [pltpu.VMEM(array.shape, array.dtype) for array in arrays[1:]]
        + [
            pltpu.VMEM((sequences * kv_heads, head_dim), jnp.float32),
            pltpu.VMEM((sequences * kv_heads, head_dim), jnp.float32),
            pltpu.VMEM((sequences, depth), jnp.bfloat16),
            pltpu.SemaphoreType.DMA((len(arrays) - 1 + len(pieces),)),
        ],
        compiler_params=pltpu.CompilerParams(vmem_limit_bytes=53 * MIB),
        cost_estimate=pl.CostEstimate(
            flops=2 * sequences * width * depth,
            bytes_accessed=2 * (width * depth + 2 * sequences * span * slots),
            transcendentals=sequences * heads * slots,
        ),
    )(*[pltpu.with_memory_space_constraint(array, pltpu.HBM) for array in arrays])


def route_weights(expert_ids, route_probs, route_order, experts):
    picked = jnp.zeros(expert_ids.shape, jnp.float32)
    for column in range(expert_ids.shape[1]):
        picked = picked + jnp.where(route_order == column, route_probs[:, column : column + 1], 0.0)
    weights = picked / jnp.sum(route_probs, axis=1, keepdims=True)
    named = expert_ids[:, :, None] == jnp.arange(experts, dtype=jnp.int32)[None, None, :]
    return jnp.sum(jnp.where(named, weights[:, :, None], 0.0), axis=1)


def exchange(values, sent, axis, ranks):
    step = 1
    while True:
        pairs = [(rank, rank ^ step) for rank in range(ranks)]
        received = lax.ppermute(sent, axis, pairs)
        step *= 2
        if step >= ranks:
            return values, received
        values = values + received.astype(jnp.float32)
        sent = values.astype(jnp.bfloat16)


def table_kernel(weights_ref, table_ref):
    experts = weights_ref.shape[1]
    weights = weights_ref[...]
    high = weights.astype(jnp.bfloat16)
    low = (weights - high.astype(jnp.float32)).astype(jnp.bfloat16)
    table_ref[...] = jnp.zeros_like(table_ref)
    table_ref[:, :experts] = high
    table_ref[:, experts : 2 * experts] = low


def norm_kernel(mine_ref, received_ref, hidden_ref, gain_ref, table_ref, residual_ref, rows_ref):
    width = hidden_ref.shape[1]
    residual = (
        hidden_ref[...].astype(jnp.float32) + mine_ref[...] + received_ref[...].astype(jnp.float32)
    )
    residual_ref[...] = residual
    mean_square = jnp.mean(residual * residual, axis=1, keepdims=True)
    normed = residual * lax.rsqrt(mean_square + EPSILON) * gain_ref[...]
    rows_ref[:, :width] = normed.astype(jnp.bfloat16)
    rows_ref[:, width:] = table_ref[...]


def pack_kernel(*refs):
    *piece_refs, packed_ref = refs
    size = piece_refs[0].shape[0]
    for number, piece_ref in enumerate(piece_refs):
        packed_ref[pl.ds(number * size, size)] = piece_ref[...]


def turn_kernel(pieces, *refs):
    for (start, size), source_ref, target_ref in zip(
        pieces, refs[: len(pieces)], refs[len(pieces) :]
    ):
        for local in range(source_ref.shape[0]):
            target_ref[local] = source_ref[local, pl.ds(start, size)].T


def turn(*sources):
    weights = [weight for weight, _, _ in sources]
    pieces = [(start, size) for _, start, size in sources]
    return call(
        functools.partial(turn_kernel, pieces),
        [(weight.shape[:2] + (size,), weight.dtype) for weight, _, size in sources],
        [weight.swapaxes(1, 2) for weight in weights],
        flops=1,
        moved=1,
        limit=6 * MIB,
    )


def expert_kernel(experts, *refs):
    *row_refs, gate_ref, first_ref, second_ref, down_ref, mine_ref, other_ref = refs
    local_experts, _, width = down_ref.shape
    rows = jnp.concatenate([ref[:, :width] for ref in row_refs], axis=0)
    table = jnp.concatenate([ref[:, width:] for ref in row_refs], axis=0).astype(jnp.float32)
    column = lax.broadcasted_iota(jnp.int32, table.shape, 1)
    total = None
    for local in range(local_experts):
        expert = lax.axis_index("expert") * local_experts + local
        chosen = (column == expert) | (column == expert + experts)
        weight = jnp.sum(jnp.where(chosen, table, 0.0), axis=1, keepdims=True)
        gate = mm(rows, gate_ref[local])
        up = [mm(rows, up_ref[local]) for up_ref in (first_ref, second_ref)]
        up = jnp.concatenate(up, axis=1)
        active = (gate * jax.nn.sigmoid(GLU_SLOPE * gate) * (up + 1.0)).astype(jnp.bfloat16)
        part = mm(active, down_ref[local])
        part = part * weight
        total = part if total is None else total + part
    half = mine_ref.shape[0]
    mine_ref[...] = total[:half]
    other_ref[...] = total[half:].astype(jnp.bfloat16)


def split_kernel(mine_ref, received_ref, kept_ref, *sent_refs):
    size = kept_ref.shape[0]
    kept_ref[...] = mine_ref[:size] + received_ref[:size].astype(jnp.float32)
    for number, sent_ref in enumerate(sent_refs, 1):
        block = pl.ds(number * size, size)
        total = mine_ref[block] + received_ref[block].astype(jnp.float32)
        sent_ref[...] = total.astype(jnp.bfloat16)


def return_kernel(received, residual_ref, *refs):
    kept_ref, *received_refs = refs[: 1 + received]
    base_ref, *sent_refs = refs[1 + received :]
    total = kept_ref[...]
    for received_ref in received_refs:
        total = total + received_ref[...].astype(jnp.float32)
    width = base_ref.shape[1]
    rank = lax.axis_index("tensor")

    def slab_of(values, owner):
        slab = values[:, :width]
        for number in range(1, values.shape[1] // width):
            piece = values[:, number * width : (number + 1) * width]
            slab = jnp.where(owner == number, piece, slab)
        return slab

    base_ref[...] = slab_of(total + residual_ref[...], rank)
    for step, sent_ref in enumerate(sent_refs, 1):
        sent_ref[...] = slab_of(total, rank ^ step).astype(jnp.bfloat16)


def per_device(
    hidden_in,
    queries,
    new_keys,
    new_values,
    cache_keys,
    cache_values,
    cache_lengths,
    out_weight,
    norm_gain,
    expert_ids,
    route_probs,
    route_order,
    gate_weight,
    up_weight,
    down_weight,
):
    sequences, width = hidden_in.shape
    expert_ranks = lax.axis_size("expert")
    tensor_ranks = lax.axis_size("tensor")
    local_experts, hidden_units = down_weight.shape[:2]
    experts = local_experts * expert_ranks
    inner = 2
    outer = expert_ranks // inner
    cut = 3 * hidden_units // 4 // 128 * 128
    row_width = -(-(width + 2 * experts) // 128) * 128

    def to_outer(values, step):
        pairs = [(rank, rank ^ (step * inner)) for rank in range(expert_ranks)]
        return lax.ppermute(values, "expert", pairs)

    def to_inner(values):
        return lax.ppermute(values, "expert", [(rank, rank ^ 1) for rank in range(expert_ranks)])

    operands = (queries, new_keys, new_values, cache_keys, cache_values, cache_lengths)
    if queries.shape[1] % 16 == 0:
        mine, sent = attend_and_project(*operands, out_weight)
    else:
        mine = jnp.dot(attend(*operands), out_weight, preferred_element_type=jnp.float32)
        sent = mine.astype(jnp.bfloat16)
    mine, received = exchange(mine, sent, "tensor", tensor_ranks)

    weights = route_weights(expert_ids, route_probs, route_order, experts)
    (table,) = call(
        table_kernel,
        [((sequences, row_width - width), jnp.bfloat16)],
        (weights,),
        flops=WINDOW_FLOPS,
        moved=sequences * row_width,
        limit=MIB,
    )

    block = (sequences, width)
    residual, rows = call(
        norm_kernel,
        [(block, jnp.float32), ((sequences, row_width), jnp.bfloat16)],
        (mine, received, hidden_in, norm_gain.reshape(1, width), table),
        flops=16 * sequences * width,
        moved=sequences * width * 16,
        limit=2 * MIB,
    )

    near = [rows]
    for step in range(1, outer):
        near.append(to_outer(rows, step))
    gate_turned, up_first = turn((gate_weight, 0, hidden_units), (up_weight, 0, cut))
    (near,) = call(
        pack_kernel,
        [((outer * sequences, row_width), jnp.bfloat16)],
        near,
        flops=sequences,
        moved=4 * outer * sequences * row_width,
        limit=2 * MIB,
    )
    far = to_inner(near)
    (up_second,) = turn((up_weight, cut, hidden_units - cut))
    half = (outer * sequences, width)
    mine, other = call(
        functools.partial(expert_kernel, experts),
        [(half, jnp.float32), (half, jnp.bfloat16)],
        (near, far, gate_turned, up_first, up_second, down_weight),
        flops=12 * half[0] * width * hidden_units * local_experts,
        moved=6 * width * hidden_units * local_experts,
        limit=16 * MIB,
    )
    received = to_inner(other)
    kept, *sent = call(
        split_kernel,
        [(block, jnp.float32)] + [(block, jnp.bfloat16)] * (outer - 1),
        (mine, received),
        flops=half[0] * width,
        moved=half[0] * width * 8,
        limit=4 * MIB,
    )
    returned = []
    for step, piece in enumerate(sent, 1):
        returned.append(to_outer(piece, step))
    slab = (sequences, width // tensor_ranks)
    total, *sent = call(
        functools.partial(return_kernel, len(returned)),
        [(slab, jnp.float32)] + [(slab, jnp.bfloat16)] * (tensor_ranks - 1),
        (residual, kept, *returned),
        flops=half[0] * width,
        moved=half[0] * width * 2,
        limit=2 * MIB,
    )
    for step, piece in enumerate(sent, 1):
        pairs = [(rank, rank ^ step) for rank in range(tensor_ranks)]
        total = total + lax.ppermute(piece, "tensor", pairs).astype(jnp.float32)
    return total.astype(jnp.bfloat16)


def solution(mesh):
    in_specs = (
        P(("groups", "expert"), None),
        P(("groups", "expert"), "tensor", None),
        P(("groups", "expert"), "tensor", None),
        P(("groups", "expert"), "tensor", None),
        P(("groups", "expert"), "tensor", None, None),
        P(("groups", "expert"), "tensor", None, None),
        P(("groups", "expert")),
        P("tensor", None),
        P(),
        P(("groups", "expert"), None),
        P(("groups", "expert"), None),
        P(("groups", "expert"), None),
        P("expert", None, "tensor"),
        P("expert", None, "tensor"),
        P("expert", "tensor", None),
    )
    out_specs = P(("groups", "expert"), "tensor")

    return jax.shard_map(
        per_device, mesh=mesh, in_specs=in_specs, out_specs=out_specs, check_vma=False
    )
```
